512 devices in a mesh: row: 16 (over x_hi, y, core), col: 32 (over z, x_lo).
Axes of the slice: x: 4 (x_hi: 2, x_lo: 2; x = x_hi * 2 + x_lo), y: 4, z: 16, core: 2. Of those that a mesh axis runs over, the one named last changes fastest.
Arguments:
- phase: float32 [512, 32, 512], P('col', 'row'), may hold values from -6 to 6
- velocity: float32 [3, 512, 32, 512], P(None, 'col', 'row'), may hold values from -12 to 12
Outputs:
- phase_next: float32 [512, 32, 512], P('col', 'row')
- velocity_next: float32 [3, 512, 32, 512], P(None, 'col', 'row')
The draws below stay inside these ranges and needn't reach their ends.
All inputs are finite; a program needn't handle non-finite values.
Results may differ from the reference program's by a relative error of at most 0.013.
Values may be sent and summed in bfloat16 or wider, within the bound.
No kernel may reach another device: no remote copies, remote signals or barrier semaphores. Data moves between devices by JAX's collectives and lax.ppermute only.
A program may use at most 64 MiB of HBM per device.

```python
import math
import jax
import jax.numpy as jnp
from jax import lax

NX = 512
NY = 512
NZ = 32
KC = 192
KY = 384
KZH = 12
KZ = 24


def block_scale(rng, shape, cuts, low, largest):
    def one(dim, parts):
        heights = jax.random.uniform(jax.random.fold_in(jax.random.fold_in(rng, 6), dim), (parts,), jnp.float32, low / len(cuts), largest / len(cuts))
        return jnp.repeat(jnp.exp(heights), shape[dim] // parts).reshape((-1,) + (1,) * (len(shape) - dim - 1))

    factor_of = one(*cuts[0])
    for cut in cuts[1:]:
        factor_of = factor_of * one(*cut)
    return factor_of


def gaussian(key, extent, scale, reach, split=(), kind=jnp.bfloat16):
    gain = block_scale(key, extent, split, -0.22, 0.18) if split else 1.0
    drawn = jax.random.normal(key, extent, jnp.float32) * scale * gain
    return jnp.minimum(jnp.maximum(drawn, -reach), reach).astype(kind)


def setup_inputs(seed: int = 0) -> dict:
    key_of = jax.random.split(jax.random.key(seed), 3)
    return {
        "phase": gaussian(key_of[0], (NY, NZ, NX), 1.0, 6.0, ((0, 32), (1, 16)), jnp.float32),
        "velocity": gaussian(key_of[1], (3, NY, NZ, NX), 2.0, 12.0, ((1, 32), (2, 16)), jnp.float32),
    }


time_step = 1e-3
epsilon = 0.01
mobility = 1.0
reynolds = 100.0
stabilizer = 2.0


def cos_sin(row_index, col_index, period):
    residue = (row_index[:, None] * col_index[None, :]) % period
    angles = residue.astype(jnp.float32) * (2.0 * math.pi / period)
    return jnp.stack([jnp.cos(angles), jnp.sin(angles)]).astype(jnp.bfloat16)


def pair_sum(pieces, direction, stack_axis):
    if direction < 0:
        real_part = pieces[0, 0] + pieces[1, 1]
        imag_part = pieces[1, 0] - pieces[0, 1]
    else:
        real_part = pieces[0, 0] - pieces[1, 1]
        imag_part = pieces[0, 1] + pieces[1, 0]
    return jnp.stack([real_part, imag_part], axis=stack_axis)


def rounded(values):
    return lax.optimization_barrier(values.astype(jnp.bfloat16))


def product(form, first_op, second_op):
    return jnp.einsum(form, first_op.astype(jnp.float32), second_op.astype(jnp.float32), precision=lax.Precision.HIGHEST)


def times_i(values):
    return jnp.stack([-values[1], values[0]])


def reference(phase, velocity):
    table_x = cos_sin(jnp.arange(NX, dtype=jnp.int32), jnp.arange(KC, dtype=jnp.int32), NX)
    table_y = cos_sin(jnp.arange(NY, dtype=jnp.int32), jnp.arange(KY, dtype=jnp.int32) - KC, NY)
    table_z = cos_sin(jnp.arange(NZ, dtype=jnp.int32), jnp.arange(KZ, dtype=jnp.int32) - KZH, NZ)
    scale_inv = 1.0 / (NX * NY * NZ)
    weight = jnp.where(jnp.arange(KC) == 0, 1.0, 2.0).astype(jnp.float32)[:, None, None]

    def forward(field):
        pieces = product('yzx,txa->tayz', rounded(field), table_x)
        x_lines = rounded(jnp.stack([pieces[0], -pieces[1]]))
        pieces = product('payz,tyb->ptabz', x_lines, table_y)
        y_planes = rounded(pair_sum(pieces, -1, 0))
        pieces = product('pabz,tzm->ptabm', y_planes, table_z)
        return pair_sum(pieces, -1, 0) * scale_inv

    def inverse(coeff):
        pieces = product('pabm,tzm->ptabz', rounded(coeff), table_z)
        z_planes = rounded(pair_sum(pieces, 1, 0))
        pieces = product('pabz,tyb->ptayz', z_planes, table_y)
        x_lines = rounded(pair_sum(pieces, 1, 0))
        scaled = jnp.stack([x_lines[0] * weight, -(x_lines[1] * weight)])
        return product('payz,pxa->yzx', scaled, table_x)

    wave_x = jnp.arange(KC).astype(jnp.float32)[None, :, None, None]
    wave_y = (jnp.arange(KY) - KC).astype(jnp.float32)[None, None, :, None]
    wave_z = ((jnp.arange(KZ) - KZH).astype(jnp.float32) * (NX / NZ))[None, None, None, :]
    squared = wave_x * wave_x + wave_y * wave_y + wave_z * wave_z

    coeff_phase = forward(phase)
    coeff_u = [forward(velocity[j]) for j in range(3)]
    gradient = [inverse(times_i(wave_x * coeff_phase)), inverse(times_i(wave_y * coeff_phase)), inverse(times_i(wave_z * coeff_phase))]
    lap_field = inverse(-squared * coeff_phase)
    vortex = [inverse(times_i(wave_y * coeff_u[2] - wave_z * coeff_u[1])),
              inverse(times_i(wave_z * coeff_u[0] - wave_x * coeff_u[2])),
              inverse(times_i(wave_x * coeff_u[1] - wave_y * coeff_u[0]))]
    advect = velocity[0] * gradient[0] + velocity[1] * gradient[1] + velocity[2] * gradient[2]
    bulk_term = phase * phase * phase - phase
    potential = bulk_term - epsilon * epsilon * lap_field
    forcing = [velocity[1] * vortex[2] - velocity[2] * vortex[1] + potential * gradient[0],
               velocity[2] * vortex[0] - velocity[0] * vortex[2] + potential * gradient[1],
               velocity[0] * vortex[1] - velocity[1] * vortex[0] + potential * gradient[2]]
    mean_mode = (wave_x == 0) & (wave_y == 0) & (wave_z == 0)
    advect_hat = jnp.where(mean_mode, 0.0, forward(advect))
    bulk_hat = forward(bulk_term)
    force_hat = [forward(forcing[j]) for j in range(3)]
    stable_part = 1.0 / time_step + mobility * stabilizer * squared
    new_phase = (stable_part * coeff_phase - advect_hat - mobility * squared * bulk_hat) / (stable_part + mobility * epsilon * epsilon * squared * squared)
    viscous = 1.0 / time_step + squared / reynolds
    unprojected = [(coeff_u[j] / time_step + force_hat[j]) / viscous for j in range(3)]
    normal_part = (wave_x * unprojected[0] + wave_y * unprojected[1] + wave_z * unprojected[2]) / jnp.maximum(squared, 1.0)
    waves = [wave_x, wave_y, wave_z]
    phase_next = inverse(new_phase)
    velocity_next = jnp.stack([inverse(unprojected[j] - waves[j] * normal_part) for j in range(3)])
    return phase_next, velocity_next
```

```python
import numpy as np

import jax
import jax.numpy as jnp
from jax import lax
from jax.experimental import pallas as pl
from jax.experimental.pallas import tpu as pltpu
from jax.sharding import Mesh
from jax.sharding import PartitionSpec as P

NX = 512
NY = 512
NZ = 32
KC = 192
KZ = 24
COLS = 32
GROUPS = 8
CORES = 2
PEERS = GROUPS * COLS
YL = NY // COLS
QS = 12
QP = 16
MODES = KZ * 32
CHUNK = 96

time_step = 0.001
epsilon = 0.01
mobility = 1.0
reynolds = 100.0
stabilizer = 2.0

PHYS = ("rg", "col")


def roots(numerator, period):
    angle = (numerator % period) * (2.0 * np.pi / period)
    return np.cos(angle), np.sin(angle)


def as_bf16(values):
    return jnp.asarray(np.asarray(values, np.float32)).astype(jnp.bfloat16)


def x_forward_table():
    c, s = roots(np.arange(KC)[:, None] * np.arange(NX)[None, :], NX)
    out = np.zeros((2, PEERS, NX))
    out[0, :KC] = c
    out[1, :KC] = -s
    return out.reshape(2 * PEERS, NX)


def x_inverse_table():
    c, s = roots(np.arange(KC)[:, None] * np.arange(NX)[None, :], NX)
    w = np.where(np.arange(KC) == 0, 1.0, 2.0)[:, None]
    return np.concatenate([w * c, -w * s])


def left_angle():
    q = np.arange(KZ) - KZ // 2
    k32 = np.arange(32)
    core = np.arange(CORES)
    rg = np.arange(GROUPS)
    c = np.arange(COLS)
    zpart = q[:, None] * (2 * core[:, None] + 4 * rg[None, :]).reshape(-1)[None, :]
    ypart = k32[:, None] * c[None, :]
    return (zpart[:, None, :, None] + ypart[None, :, None, :]).reshape(
        MODES, CORES * PEERS
    )


def left_forward_table():
    c, s = roots(left_angle(), 32)
    return np.block([[c, s], [-s, c]])


def left_inverse_table():
    c, s = roots(left_angle()[:, :PEERS].T, 32)
    return np.block([[c, -s], [s, c]])


def twiddles():
    core = np.arange(CORES)[:, None, None, None, None, None]
    q = (np.arange(KZ) - KZ // 2)[None, :, None, None, None, None]
    k32 = np.arange(32)[None, None, :, None, None, None]
    yl = np.arange(YL)[None, None, None, None, :, None]
    z2 = np.arange(2)[None, None, None, None, None, :]
    f = np.zeros((1, 1, 1, 4, 1, 1), np.int64)
    c, s = roots(yl * k32 + 16 * q * (2 * core + z2) + f, 512)
    return c.reshape(CORES * MODES, 128), s.reshape(CORES * MODES, 128)


def short_roots():
    q = np.arange(QS) - QS // 2
    return roots(q[:, None] * np.arange(YL)[None, :], 16)


def right_forward_table(sources, fields_in):
    c, s = short_roots()
    out = np.zeros((2, fields_in, YL, 2, len(sources), 2, QP))
    for slot, src in enumerate(sources):
        if src is None:
            continue
        f, times_i = src
        to_re = [c, s]
        to_im = [-s, c]
        if times_i:
            to_re, to_im = [s, -c], [c, s]
        for p in range(2):
            for z2 in range(2):
                out[p, f, :, z2, slot, 0, :QS] = to_re[p].T
                out[p, f, :, z2, slot, 1, :QS] = to_im[p].T
    scale_inv = 1.0 / (NX * NY * NZ)
    return out.reshape(2 * fields_in * 32, len(sources) * 32) * scale_inv


def right_inverse_table(slots):
    c, s = short_roots()
    out = np.zeros((slots, 2, QP, 2, slots, YL, 2))
    for f in range(slots):
        for z2 in range(2):
            out[f, 0, :QS, 0, f, :, z2] = c
            out[f, 1, :QS, 0, f, :, z2] = -s
            out[f, 0, :QS, 1, f, :, z2] = s
            out[f, 1, :QS, 1, f, :, z2] = c
    return out.reshape(slots * 32, 2 * slots * 32)


def dot(lhs, rhs):
    return lax.dot_general(
        lhs, rhs, (((1,), (0,)), ((), ())), preferred_element_type=jnp.float32
    )


def dot_nt(lhs, rhs):
    return lax.dot_general(
        lhs, rhs, (((1,), (1,)), ((), ())), preferred_element_type=jnp.float32
    )


def flat_rows(ref, *lead):
    return ref[lead].reshape(2 * YL, NX) if lead else ref[...].reshape(2 * YL, NX)


def mode_waves(row0, rows, slot_lanes):
    row = row0 + lax.broadcasted_iota(jnp.int32, (rows, slot_lanes), 0)
    lane = lax.broadcasted_iota(jnp.int32, (rows, slot_lanes), 1)
    ky = (lane % QP - QS // 2) * 32 + row % 32
    kz = (row // 32 - KZ // 2) * (NX // NZ)
    return ky.astype(jnp.float32), kz.astype(jnp.float32), lane // 32


def x_forward_kernel(phase_ref, vel_ref, table_ref, out_ref, scratch):
    x = jnp.concatenate(
        [flat_rows(phase_ref)] + [flat_rows(vel_ref, j) for j in range(3)], axis=0
    ).astype(jnp.bfloat16)
    lines = dot_nt(table_ref[...], x)
    for p in range(2):
        scratch[pl.ds(p, PEERS, stride=2), :] = lines[p * PEERS : (p + 1) * PEERS]
    out_ref[...] = scratch[...].astype(jnp.bfloat16)


def gather_rows(in_ref, wide, rhs, tiles):
    count = CORES * PEERS
    wide[...] = in_ref[...].astype(jnp.float32)
    for p in range(2):
        for t in range(tiles):
            rows = wide[pl.ds(2 * t + p, count, stride=2 * tiles), :]
            rhs[pl.ds(p * count, count), pl.ds(128 * t, 128)] = rows.astype(jnp.bfloat16)


def forward_yz(left_ref, rhs, sums):
    sums[...] = dot(left_ref[...], rhs[...])


def twiddled(sums, cos_ref, sin_ref, r0, tiles):
    c = cos_ref[pl.ds(r0, CHUNK), :]
    s = sin_ref[pl.ds(r0, CHUNK), :]
    res, ims = [], []
    for t in range(tiles):
        re = sums[pl.ds(r0, CHUNK), pl.ds(128 * t, 128)]
        im = sums[pl.ds(MODES + r0, CHUNK), pl.ds(128 * t, 128)]
        res.append((re * c + im * s).astype(jnp.bfloat16))
        ims.append((im * c - re * s).astype(jnp.bfloat16))
    return jnp.concatenate(res + ims, axis=1)


def untwiddled(core, values, cos_ref, sin_ref, r0, tiles, spec):
    base = pl.multiple_of(core * MODES + r0, 8)
    c = cos_ref[pl.ds(base, CHUNK), :]
    s = sin_ref[pl.ds(base, CHUNK), :]
    for t in range(tiles):
        re = values[:, 128 * t : 128 * (t + 1)]
        im = values[:, 128 * (tiles + t) : 128 * (tiles + t + 1)]
        spec[pl.ds(r0, CHUNK), pl.ds(128 * t, 128)] = (re * c - im * s).astype(jnp.bfloat16)
        spec[pl.ds(MODES + r0, CHUNK), pl.ds(128 * t, 128)] = (re * s + im * c).astype(
            jnp.bfloat16
        )


def inverse_rows(left_ref, spec, wide, out_ref, tiles):
    lines = dot(left_ref[...], spec[...])
    for p in range(2):
        for t in range(tiles):
            wide[pl.ds(2 * t + p, PEERS, stride=2 * tiles), :] = lines[
                p * PEERS : (p + 1) * PEERS, 128 * t : 128 * (t + 1)
            ]
    rows = 2 * tiles * PEERS
    out_ref[...] = wide[pl.ds(0, rows), :].astype(jnp.bfloat16)


def derive_kernel(
    where_ref, in_ref, left_ref, cos_ref, sin_ref, right_ref, back_ref, leftinv_ref,
    out_ref, spectra_ref, wide, rhs, sums, spec,
):
    core = where_ref[0]
    kx = where_ref[1].astype(jnp.float32)
    gather_rows(in_ref, wide, rhs, 1)
    forward_yz(left_ref, rhs, sums)

    @pl.loop(0, MODES // CHUNK)
    def _(j):
        r0 = pl.multiple_of(j * CHUNK, CHUNK)
        lines = twiddled(sums, cos_ref, sin_ref, r0, 1)
        modes = dot(lines, right_ref[...])
        spectra_ref[pl.ds(r0, CHUNK), :] = modes[:, 0:128]
        ky, kz, slot = mode_waves(r0, CHUNK, 128)
        k2 = kx * kx + ky * ky + kz * kz
        first = jnp.where(
            slot == 0, kx, jnp.where(slot == 1, ky, jnp.where(slot == 2, kz, -k2))
        )
        second = jnp.where(slot == 0, ky, jnp.where(slot == 1, kz, kx))
        third = jnp.where(slot == 0, kz, jnp.where(slot == 1, kx, ky))
        low = modes[:, 128:256] * first
        high = modes[:, 256:384] * second - modes[:, 384:512] * third
        coeff = jnp.concatenate([low, high], axis=1).astype(jnp.bfloat16)
        untwiddled(core, dot(coeff, back_ref[...]), cos_ref, sin_ref, r0, 2, spec)

    inverse_rows(leftinv_ref, spec, wide, out_ref, 2)


def solve_kernel(
    where_ref, in_ref, spectra_ref, left_ref, cos_ref, sin_ref, right_ref, back_ref,
    leftinv_ref, out_ref, wide, rhs, sums, spec,
):
    core = where_ref[0]
    kx = where_ref[1].astype(jnp.float32)
    gather_rows(in_ref, wide, rhs, 2)
    forward_yz(left_ref, rhs, sums)

    @pl.loop(0, MODES // CHUNK)
    def _(j):
        r0 = pl.multiple_of(j * CHUNK, CHUNK)
        lines = twiddled(sums, cos_ref, sin_ref, r0, 2)
        modes = dot(lines, right_ref[...])
        old = spectra_ref[pl.ds(r0, CHUNK), :]
        ky, kz, slot = mode_waves(r0, CHUNK, 128)
        k2 = kx * kx + ky * ky + kz * kz
        stable = 1.0 / time_step + mobility * stabilizer * k2
        scalar = slot == 0
        below = jnp.where(
            scalar,
            stable + mobility * epsilon * epsilon * k2 * k2,
            1.0 / time_step + k2 / reynolds,
        )
        keep = jnp.where(scalar, stable, 1.0 / time_step)
        mean = scalar & (k2 == 0.0)
        sign = jnp.where(scalar, -1.0, 1.0)
        update = jnp.where(mean, 0.0, modes[:, 0:128]) * sign
        bulk = jnp.where(scalar, mobility * k2, 0.0) * modes[:, 128:256]
        fresh = (keep * old + update - bulk) / below
        wave = jnp.where(
            scalar, 0.0, jnp.where(slot == 1, kx, jnp.where(slot == 2, ky, kz))
        )
        normal = wave * fresh
        normal = normal + pltpu.roll(normal, 32, 1)
        normal = normal + pltpu.roll(normal, 64, 1)
        fresh = fresh - wave * (normal / jnp.maximum(k2, 1.0))
        coeff = fresh.astype(jnp.bfloat16)
        untwiddled(core, dot(coeff, back_ref[...]), cos_ref, sin_ref, r0, 1, spec)

    inverse_rows(leftinv_ref, spec, wide, out_ref, 1)


def physical(wide, table_ref, tiles):
    fields = []
    for t in range(tiles):
        lines = jnp.concatenate(
            [
                wide[pl.ds(2 * t + p, KC, stride=2 * tiles), :]
                for p in range(2)
            ],
            axis=0,
        )
        values = dot(lines.T.astype(jnp.bfloat16), table_ref[...])
        fields += [values[32 * f : 32 * (f + 1)] for f in range(4)]
    return fields


def nonlinear_kernel(in_ref, phase_ref, vel_ref, back_ref, table_ref, out_ref, wide):
    wide[...] = in_ref[...].astype(jnp.float32)
    d = physical(wide, back_ref, 2)
    phase = flat_rows(phase_ref)
    v = [flat_rows(vel_ref, j) for j in range(3)]
    g, lap, w = d[0:3], d[3], d[4:7]
    advect = v[0] * g[0] + v[1] * g[1] + v[2] * g[2]
    bulk = phase * phase * phase - phase
    potential = bulk - epsilon * epsilon * lap
    terms = [
        advect,
        v[1] * w[2] - v[2] * w[1] + potential * g[0],
        v[2] * w[0] - v[0] * w[2] + potential * g[1],
        v[0] * w[1] - v[1] * w[0] + potential * g[2],
        bulk,
        jnp.zeros((96, NX), jnp.float32),
    ]
    x = jnp.concatenate([t.astype(jnp.bfloat16) for t in terms], axis=0)
    lines = dot_nt(table_ref[...], x)
    for p in range(2):
        for t in range(2):
            wide[pl.ds(2 * t + p, PEERS, stride=4), :] = lines[
                p * PEERS : (p + 1) * PEERS, 128 * t : 128 * (t + 1)
            ]
    out_ref[...] = wide[...].astype(jnp.bfloat16)


def x_inverse_kernel(in_ref, back_ref, phase_ref, vel_ref, wide):
    wide[...] = in_ref[...].astype(jnp.float32)
    d = physical(wide, back_ref, 1)
    phase_ref[...] = d[0].reshape(YL, 2, NX)
    for j in range(3):
        vel_ref[j] = d[1 + j].reshape(YL, 2, NX)


def vmem(count):
    return [pl.BlockSpec(memory_space=pltpu.VMEM)] * count


def call(kernel, outs, scratch, *args, scalars=0):
    specs = [pl.BlockSpec(memory_space=pltpu.SMEM)] * scalars + vmem(len(args) - scalars)
    out_specs = vmem(len(outs)) if len(outs) > 1 else vmem(1)[0]
    return pl.pallas_call(
        kernel,
        in_specs=specs,
        out_specs=out_specs,
        out_shape=outs if len(outs) > 1 else outs[0],
        scratch_shapes=scratch,
        compiler_params=pltpu.CompilerParams(vmem_limit_bytes=48 * 1024 * 1024),
    )(*args)


def shape(rows, lanes, dtype):
    return jax.ShapeDtypeStruct((rows, lanes), dtype)


def exchange(values):
    rows = values.shape[0]
    swapped = lax.all_to_all(
        values.reshape(rows // 2, 2, 128), PHYS, split_axis=0, concat_axis=0, tiled=True
    )
    return swapped.reshape(rows, 128)


def both_cores(values):
    rows = values.shape[0]
    joined = lax.all_gather(values.reshape(rows // 2, 2, 128), "core", axis=0, tiled=True)
    return joined.reshape(CORES * rows, 128)


def on_device(phase, velocity):
    bf, f32 = jnp.bfloat16, jnp.float32
    x_table = as_bf16(x_forward_table())
    x_back = as_bf16(x_inverse_table())
    left = as_bf16(left_forward_table())
    left_inv = as_bf16(left_inverse_table())
    cos_t, sin_t = (jnp.asarray(t, f32) for t in twiddles())
    plain = [(0, False), (1, False), (2, False), (3, False)]
    lows = [(0, True), (0, True), (0, True), (0, False)]
    highs = [(3, True), (1, True), (2, True), None]
    others = [(2, True), (3, True), (1, True), None]
    right_derive = as_bf16(right_forward_table(plain + lows + highs + others, 4))
    right_solve = as_bf16(
        right_forward_table(plain + [(4, False), None, None, None], 8)
    )
    back_derive = as_bf16(right_inverse_table(8))
    back_solve = as_bf16(right_inverse_table(4))
    wave = lax.axis_index("rg") * COLS + lax.axis_index("col")
    where = jnp.stack([lax.axis_index("core"), wave]).astype(jnp.int32)

    def middle(tiles_in, tiles_out):
        return [
            pltpu.VMEM((2 * CORES * PEERS * tiles_in, 128), f32),
            pltpu.VMEM((2 * CORES * PEERS, 128 * tiles_in), bf),
            pltpu.VMEM((2 * MODES, 128 * tiles_in), f32),
            pltpu.VMEM((2 * MODES, 128 * tiles_out), bf),
        ]

    lines = call(
        x_forward_kernel, [shape(2 * PEERS, 128, bf)],
        [pltpu.VMEM((2 * PEERS, 128), f32)], phase, velocity, x_table,
    )
    gathered = both_cores(exchange(lines))
    lines, spectra = call(
        derive_kernel, [shape(4 * PEERS, 128, bf), shape(MODES, 128, f32)], middle(1, 2),
        where, gathered, left, cos_t, sin_t, right_derive, back_derive, left_inv, scalars=1,
    )
    lines = call(
        nonlinear_kernel, [shape(4 * PEERS, 128, bf)],
        [pltpu.VMEM((4 * PEERS, 128), f32)], exchange(lines), phase, velocity, x_back, x_table,
    )
    gathered = both_cores(exchange(lines))
    lines = call(
        solve_kernel, [shape(2 * PEERS, 128, bf)], middle(2, 1),
        where, gathered, spectra, left, cos_t, sin_t, right_solve, back_solve, left_inv,
        scalars=1,
    )
    return call(
        x_inverse_kernel,
        [
            jax.ShapeDtypeStruct(phase.shape, f32),
            jax.ShapeDtypeStruct(velocity.shape, f32),
        ],
        [pltpu.VMEM((2 * PEERS, 128), f32)], exchange(lines), x_back,
    )


def solution(mesh):
    finer = Mesh(
        mesh.devices.reshape(GROUPS, CORES, mesh.shape["col"]), ("rg", "core", "col")
    )
    row = ("rg", "core")
    in_specs = (P("col", row, None), P(None, "col", row, None))
    out_specs = (P("col", row, None), P(None, "col", row, None))
    return jax.shard_map(
        on_device, mesh=finer, in_specs=in_specs, out_specs=out_specs, check_vma=False
    )
```

```python
import numpy as np

import jax
import jax.numpy as jnp
from jax import lax
from jax.experimental import pallas as pl
from jax.experimental.pallas import tpu as pltpu
from jax.sharding import PartitionSpec as P

NX = 512
NY = 512
NZ = 32
KC = 192
KZ = 24
COLS = 32
ROWS = 16
AS = KC // COLS
LO = 32 // ROWS
YL = NY // COLS
QS = 12
QP = 16
BATCH = AS * LO
MODES = KZ * BATCH
LINES = COLS * AS * 2

time_step = 0.001
epsilon = 0.01
mobility = 1.0
reynolds = 100.0
stabilizer = 2.0


def roots(numerator, period):
    angle = (numerator % period) * (2.0 * np.pi / period)
    return np.cos(angle), np.sin(angle)


def as_bf16(values):
    return jnp.asarray(np.asarray(values, np.float32)).astype(jnp.bfloat16)


def x_forward_table():
    c, s = roots(np.arange(KC)[:, None] * np.arange(NX)[None, :], NX)
    return np.stack([c, -s], axis=1).reshape(LINES, NX)


def x_inverse_table():
    c, s = roots(np.arange(KC)[:, None] * np.arange(NX)[None, :], NX)
    w = np.where(np.arange(KC) == 0, 1.0, 2.0)[:, None]
    return np.stack([w * c, -w * s], axis=1).reshape(LINES, NX)


def complex_rotation(c, s):
    return np.array([[c, -s], [s, c]])


def left_y_table(zr, direction):
    k32 = np.arange(32)
    c, s = roots(k32[:, None] * np.arange(COLS)[None, :], 32)
    same = np.einsum("ab,zy->abzy", np.eye(AS), np.eye(zr))
    rot = complex_rotation(c, direction * s).reshape(2, 2, ROWS, LO, COLS)
    n = 2 * 32 * AS * zr
    if direction < 0:
        return np.einsum("pqrlc,abzy->pralzcbqy", rot, same).reshape(n, n)
    return np.einsum("pqrlc,abzy->capzqrbly", rot, same).reshape(n, n)


def twiddles(zr):
    k32 = np.arange(32).reshape(ROWS, 1, LO, 1, 1)
    yl = lane_yl(zr).reshape(1, 1, 1, 1, 128)
    c, s = roots(np.broadcast_to(k32 * yl, (ROWS, AS, LO, zr, 128)), 512)
    return c.reshape(-1, 128), s.reshape(-1, 128)


def lane_yl(zr):
    if zr == 1:
        return np.broadcast_to(np.arange(YL)[None, :, None], (4, YL, 2)).reshape(-1)
    return np.broadcast_to(np.arange(YL)[None, :], (8, YL)).reshape(-1)


def right_y_table(zr, direction):
    q = np.arange(QS) - QS // 2
    c, s = np.zeros((2, QP, YL))
    c[:QS], s[:QS] = roots(q[:, None] * np.arange(YL)[None, :], 16)
    rot = complex_rotation(c, direction * s)
    eye = np.eye
    if zr == 1:
        if direction < 0:
            out = np.einsum("pkqy,fg,zw->kfyzpwgq", rot, eye(4), eye(2))
        else:
            out = np.einsum("pkqy,fg,zw->kzfqpgyw", rot, eye(4), eye(2))
    elif direction < 0:
        out = np.einsum("pkqy,fg->kfypgq", rot, eye(8))
    else:
        out = np.einsum("pkqy,fg->kfqpgy", rot, eye(8))
    return out.reshape(256, 256)


def left_z_table(direction, z_major):
    q = np.arange(KZ) - KZ // 2
    c, s = roots(q[:, None] * np.arange(NZ)[None, :], NZ)
    rot = complex_rotation(c, direction * s).reshape(2, 2, KZ, ROWS, 2)
    same = np.eye(BATCH)
    if direction < 0:
        form = "pkmsz,ab->pmazsbk" if z_major else "pkmsz,ab->pmasbzk"
        out = np.einsum(form, rot, same).reshape(2 * MODES, -1)
        return out / (NX * NY * NZ)
    form = "pkmsz,ab->zsapkmb" if z_major else "pkmsz,ab->sazpkmb"
    return np.einsum(form, rot, same).reshape(-1, 2 * MODES)


def spread_table():
    low = [0, 0, 0, 0]
    high = [3, 1, 2, None]
    plain = [0, 1, 2, 3]
    other = [2, 3, 1, None]
    out = np.zeros((2, 4, QP, 2, 16, QP))
    for slot, f in enumerate(low + high + plain + other):
        if f is not None:
            for z in range(2):
                out[z, f, :, z, slot, :] = np.eye(QP)
    return out.reshape(128, 512)


def wave_table():
    a = np.arange(AS).reshape(1, AS, 1, 1, 1)
    lo = np.arange(LO).reshape(1, 1, LO, 1, 1)
    m = np.arange(KZ).reshape(KZ, 1, 1, 1, 1)
    q = np.arange(QP).reshape(1, 1, 1, 1, QP)
    full = (KZ, AS, LO, 8, QP)
    return np.stack(
        [
            np.broadcast_to(a, full),
            np.broadcast_to(32 * (q - QS // 2) + lo, full),
            np.broadcast_to((m - KZ // 2) * (NX // NZ), full),
        ]
    ).reshape(3 * MODES, 128)


def dot(lhs, rhs):
    return lax.dot_general(
        lhs, rhs, (((1,), (0,)), ((), ())), preferred_element_type=jnp.float32
    )


def dot_nt(lhs, rhs):
    return lax.dot_general(
        lhs, rhs, (((1,), (1,)), ((), ())), preferred_element_type=jnp.float32
    )


def to_bf16(values):
    return values.astype(jnp.bfloat16)


def flat_rows(ref, *lead):
    return ref[lead].reshape(2 * YL, NX) if lead else ref[...].reshape(2 * YL, NX)


def x_forward_kernel(phase_ref, vel_ref, table_ref, out_ref):
    x = jnp.concatenate(
        [flat_rows(phase_ref)] + [flat_rows(vel_ref, j) for j in range(3)], axis=0
    )
    out_ref[...] = to_bf16(dot_nt(table_ref[...], to_bf16(x)))


def y_forward_kernel(in_ref, left_ref, cos_ref, sin_ref, right_ref, out_ref, wide):
    half = in_ref.shape[0] // 2
    sums = dot(left_ref[...], in_ref[...])
    re, im = sums[:half], sums[half:]
    c, s = cos_ref[...], sin_ref[...]
    lines = jnp.concatenate([to_bf16(re * c + im * s), to_bf16(im * c - re * s)], axis=1)
    modes = dot(lines, right_ref[...])
    for p in range(2):
        wide[pl.ds(p, half, stride=2), :] = modes[:, 128 * p : 128 * (p + 1)]
    out_ref[...] = to_bf16(wide[...])


def y_inverse_kernel(in_ref, left_ref, cos_ref, sin_ref, right_ref, out_ref, wide):
    half = in_ref.shape[0] // 2
    wide[...] = in_ref[...].astype(jnp.float32)
    modes = jnp.concatenate(
        [to_bf16(wide[pl.ds(p, half, stride=2), :]) for p in range(2)], axis=1
    )
    lines = dot(modes, right_ref[...])
    re, im = lines[:, :128], lines[:, 128:]
    c, s = cos_ref[...], sin_ref[...]
    spun = jnp.concatenate([to_bf16(re * c - im * s), to_bf16(re * s + im * c)], axis=0)
    out_ref[...] = to_bf16(dot(left_ref[...], spun))


def wave_numbers(where_ref, wave_ref):
    kx = wave_ref[0:MODES] + where_ref[0].astype(jnp.float32)
    ky = wave_ref[MODES : 2 * MODES] + where_ref[1].astype(jnp.float32)
    kz = wave_ref[2 * MODES : 3 * MODES]
    slot = lax.broadcasted_iota(jnp.int32, (MODES, 128), 1) // QP
    return kx, ky, kz, kx * kx + ky * ky + kz * kz, slot


def derive_kernel(
    where_ref, in_ref, spread_ref, left_ref, wave_ref, back_ref, out_ref, spectra_ref
):
    spread = to_bf16(dot(in_ref[...], spread_ref[...]))
    modes = dot(left_ref[...], jnp.concatenate([spread[:, :256], spread[:, 256:]], axis=0))
    spectra_ref[...] = modes[:, 128:]
    kx, ky, kz, k2, slot = wave_numbers(where_ref, wave_ref)
    one = jnp.where(
        (slot == 0) | (slot == 6),
        kx,
        jnp.where(
            (slot == 1) | (slot == 4),
            ky,
            jnp.where((slot == 2) | (slot == 5), kz, jnp.where(slot == 3, -k2, 0.0)),
        ),
    )
    two = jnp.where(
        slot == 4, kz, jnp.where(slot == 5, kx, jnp.where(slot == 6, ky, 0.0))
    )
    re = modes[:MODES, :128] * one - modes[:MODES, 128:] * two
    im = modes[MODES:, :128] * one - modes[MODES:, 128:] * two
    plain = slot == 3
    coeff = jnp.concatenate(
        [to_bf16(jnp.where(plain, re, -im)), to_bf16(jnp.where(plain, im, re))], axis=0
    )
    out_ref[...] = to_bf16(dot(back_ref[...], coeff))


def solve_kernel(where_ref, in_ref, spectra_ref, left_ref, wave_ref, back_ref, out_ref):
    modes = dot(left_ref[...], in_ref[...])
    kx, ky, kz, k2, slot = wave_numbers(where_ref, wave_ref)
    scalar = slot == 0
    stable = 1.0 / time_step + mobility * stabilizer * k2
    below = jnp.where(
        scalar,
        stable + mobility * epsilon * epsilon * k2 * k2,
        1.0 / time_step + k2 / reynolds,
    )
    used = slot < 4
    inv = jnp.where(used, 1.0 / below, 0.0)
    keep = jnp.where(scalar, stable, 1.0 / time_step)
    mean = scalar & (k2 == 0.0)
    sign = jnp.where(mean, 0.0, jnp.where(scalar, -1.0, 1.0))
    bulk = jnp.where(scalar, mobility * k2, 0.0)
    wave = jnp.where(
        slot == 1, kx, jnp.where(slot == 2, ky, jnp.where(slot == 3, kz, 0.0))
    )
    shared = wave / jnp.maximum(k2, 1.0)
    parts = []
    for p in range(2):
        now = modes[p * MODES : (p + 1) * MODES]
        old = spectra_ref[p * MODES : (p + 1) * MODES]
        fresh = (keep * old + sign * now - bulk * pltpu.roll(now, 64, 1)) * inv
        normal = wave * fresh
        for step in (16, 32, 64):
            normal = normal + pltpu.roll(normal, step, 1)
        parts.append(to_bf16(fresh - shared * normal))
    both = dot(back_ref[...], jnp.concatenate(parts, axis=0))
    half = both.shape[0] // 2
    out_ref[...] = to_bf16(both[:half] + pltpu.roll(both[half:], 64, 1))


def nonlinear_kernel(in_ref, phase_ref, vel_ref, back_ref, table_ref, out_ref, wide):
    wide[...] = in_ref[...].astype(jnp.float32)
    for z in range(2):
        lines = to_bf16(wide[pl.ds(z, LINES, stride=2), :].T)
        values = dot(lines, back_ref[...])
        d = [values[YL * f : YL * (f + 1)] for f in range(7)]
        phase = phase_ref[:, z, :]
        v = [vel_ref[j, :, z, :] for j in range(3)]
        g, lap, w = d[0:3], d[3], d[4:7]
        advect = v[0] * g[0] + v[1] * g[1] + v[2] * g[2]
        bulk = phase * phase * phase - phase
        potential = bulk - epsilon * epsilon * lap
        terms = [
            advect,
            v[1] * w[2] - v[2] * w[1] + potential * g[0],
            v[2] * w[0] - v[0] * w[2] + potential * g[1],
            v[0] * w[1] - v[1] * w[0] + potential * g[2],
            bulk,
            jnp.zeros((3 * YL, NX), jnp.float32),
        ]
        x = jnp.concatenate([to_bf16(t) for t in terms], axis=0)
        wide[pl.ds(z, LINES, stride=2), :] = dot_nt(table_ref[...], x)
    out_ref[...] = to_bf16(wide[...])


def x_inverse_kernel(in_ref, back_ref, phase_ref, vel_ref):
    lines = to_bf16(in_ref[...].astype(jnp.float32).T)
    values = dot(lines, back_ref[...])
    phase_ref[...] = values[0:32].reshape(YL, 2, NX)
    for j in range(3):
        vel_ref[j] = values[32 * (j + 1) : 32 * (j + 2)].reshape(YL, 2, NX)


def call(kernel, outs, scratch, *args, scalars=0):
    vmem = pl.BlockSpec(memory_space=pltpu.VMEM)
    specs = [pl.BlockSpec(memory_space=pltpu.SMEM)] * scalars + [vmem] * (
        len(args) - scalars
    )
    return pl.pallas_call(
        kernel,
        in_specs=specs,
        out_specs=[vmem] * len(outs),
        out_shape=outs,
        scratch_shapes=scratch,
        compiler_params=pltpu.CompilerParams(vmem_limit_bytes=16 * 1024 * 1024),
    )(*args)


def buffer(rows, dtype=jnp.bfloat16):
    return jax.ShapeDtypeStruct((rows, 128), dtype)


def exchange(values, axis):
    rows = values.shape[0]
    swapped = lax.all_to_all(
        values.reshape(rows // 2, 2, 128), axis, split_axis=0, concat_axis=0, tiled=True
    )
    return swapped.reshape(rows, 128)


def on_device(phase, velocity):
    f32 = jnp.float32
    x_table = as_bf16(x_forward_table())
    x_back = as_bf16(x_inverse_table())
    waves = jnp.asarray(wave_table(), f32)
    where = jnp.stack(
        [lax.axis_index("col") * AS, lax.axis_index("row") * LO]
    ).astype(jnp.int32)

    def y_tables(zr, direction):
        cos_t, sin_t = twiddles(zr)
        return (
            as_bf16(left_y_table(zr, direction)),
            jnp.asarray(cos_t, f32),
            jnp.asarray(sin_t, f32),
            as_bf16(right_y_table(zr, direction)),
        )

    def y_step(kernel, lines, zr, direction):
        rows = LINES * zr
        return call(
            kernel, [buffer(rows)], [pltpu.VMEM((rows, 128), f32)],
            lines, *y_tables(zr, direction),
        )[0]

    lines = call(x_forward_kernel, [buffer(LINES)], [], phase, velocity, x_table)[0]
    planes = y_step(y_forward_kernel, exchange(lines, "col"), 1, -1)
    planes, spectra = call(
        derive_kernel, [buffer(2 * LINES), buffer(2 * MODES, f32)], [],
        where, exchange(planes, "row"), as_bf16(spread_table()),
        as_bf16(left_z_table(-1, True)), waves, as_bf16(left_z_table(1, False)), scalars=1,
    )
    lines = y_step(y_inverse_kernel, exchange(planes, "row"), 2, 1)
    lines = call(
        nonlinear_kernel, [buffer(2 * LINES)], [pltpu.VMEM((2 * LINES, 128), f32)],
        exchange(lines, "col"), phase, velocity, x_back, x_table,
    )[0]
    planes = y_step(y_forward_kernel, exchange(lines, "col"), 2, -1)
    planes = call(
        solve_kernel, [buffer(LINES)], [],
        where, exchange(planes, "row"), spectra, as_bf16(left_z_table(-1, False)), waves,
        as_bf16(left_z_table(1, True)), scalars=1,
    )[0]
    lines = y_step(y_inverse_kernel, exchange(planes, "row"), 1, 1)
    return tuple(
        call(
            x_inverse_kernel,
            [
                jax.ShapeDtypeStruct(phase.shape, f32),
                jax.ShapeDtypeStruct(velocity.shape, f32),
            ],
            [], exchange(lines, "col"), x_back,
        )
    )


def solution(mesh):
    in_specs = (P("col", "row", None), P(None, "col", "row", None))
    out_specs = (P("col", "row", None), P(None, "col", "row", None))
    return jax.shard_map(
        on_device, mesh=mesh, in_specs=in_specs, out_specs=out_specs, check_vma=False
    )
```

```python
import numpy as np

import jax
import jax.numpy as jnp
from jax import lax
from jax.experimental import pallas as pl
from jax.experimental.pallas import tpu as pltpu
from jax.sharding import PartitionSpec as P

NX = 512
NY = 512
NZ = 32
KC = 192
KZ = 24
COLS = 32
ROWS = 16
AS = KC // COLS
LO = 32 // ROWS
YL = NY // COLS
QS = 12
QP = 16
BATCH = AS * LO
MODES = KZ * BATCH
LINES = COLS * AS * 2
COST = 10_000_000_000

time_step = 0.001
epsilon = 0.01
mobility = 1.0
reynolds = 100.0
stabilizer = 2.0


def roots(numerator, period):
    angle = (numerator % period) * (2.0 * np.pi / period)
    return np.cos(angle), np.sin(angle)


def as_bf16(values):
    return jnp.asarray(np.asarray(values, np.float32)).astype(jnp.bfloat16)


def x_forward_table():
    c, s = roots(np.arange(KC)[:, None] * np.arange(NX)[None, :], NX)
    return np.stack([c, -s], axis=1).reshape(LINES, NX)


def x_inverse_table():
    c, s = roots(np.arange(KC)[:, None] * np.arange(NX)[None, :], NX)
    w = np.where(np.arange(KC) == 0, 1.0, 2.0)[:, None]
    return np.stack([w * c, -w * s], axis=1).reshape(LINES, NX)


def complex_rotation(c, s):
    return np.array([[c, -s], [s, c]])


def left_y_table(zr, direction):
    k32 = np.arange(32)
    c, s = roots(k32[:, None] * np.arange(COLS)[None, :], 32)
    same = np.einsum("ab,zy->abzy", np.eye(AS), np.eye(zr))
    rot = complex_rotation(c, direction * s).reshape(2, 2, ROWS, LO, COLS)
    n = 2 * 32 * AS * zr
    if direction < 0:
        return np.einsum("pqrlc,abzy->pralzcbqy", rot, same).reshape(n, n)
    return np.einsum("pqrlc,abzy->capzqrbly", rot, same).reshape(n, n)


def twiddles(zr):
    k32 = np.arange(32).reshape(ROWS, 1, LO, 1, 1)
    yl = lane_yl(zr).reshape(1, 1, 1, 1, 128)
    c, s = roots(np.broadcast_to(k32 * yl, (ROWS, AS, LO, zr, 128)), 512)
    return c.reshape(-1, 128), s.reshape(-1, 128)


def lane_yl(zr):
    if zr == 1:
        return np.broadcast_to(np.arange(YL)[None, :, None], (4, YL, 2)).reshape(-1)
    return np.broadcast_to(np.arange(YL)[None, :], (8, YL)).reshape(-1)


def right_y_table(zr, direction):
    q = np.arange(QS) - QS // 2
    c, s = np.zeros((2, QP, YL))
    c[:QS], s[:QS] = roots(q[:, None] * np.arange(YL)[None, :], 16)
    rot = complex_rotation(c, direction * s)
    eye = np.eye
    if zr == 1:
        if direction < 0:
            out = np.einsum("pkqy,fg,zw->kfyzpwgq", rot, eye(4), eye(2))
        else:
            out = np.einsum("pkqy,fg,zw->kzfqpgyw", rot, eye(4), eye(2))
    elif direction < 0:
        out = np.einsum("pkqy,fg->kfypgq", rot, eye(8))
    else:
        out = np.einsum("pkqy,fg->kfqpgy", rot, eye(8))
    return out.reshape(256, 256)


def left_z_table(direction, z_major):
    q = np.arange(KZ) - KZ // 2
    c, s = roots(q[:, None] * np.arange(NZ)[None, :], NZ)
    rot = complex_rotation(c, direction * s).reshape(2, 2, KZ, ROWS, 2)
    same = np.eye(BATCH)
    if direction < 0:
        form = "pkmsz,ab->pmazsbk" if z_major else "pkmsz,ab->pmasbzk"
        out = np.einsum(form, rot, same).reshape(2 * MODES, -1)
        return out / (NX * NY * NZ)
    form = "pkmsz,ab->zsapkmb" if z_major else "pkmsz,ab->sazpkmb"
    return np.einsum(form, rot, same).reshape(-1, 2 * MODES)


def spread_table():
    low = [0, 0, 0, 0]
    high = [3, 1, 2, None]
    plain = [0, 1, 2, 3]
    other = [2, 3, 1, None]
    out = np.zeros((2, 4, QP, 2, 16, QP))
    for slot, f in enumerate(low + high + plain + other):
        if f is not None:
            for z in range(2):
                out[z, f, :, z, slot, :] = np.eye(QP)
    return out.reshape(128, 512)


def wave_table():
    a = np.arange(AS).reshape(1, AS, 1, 1, 1)
    lo = np.arange(LO).reshape(1, 1, LO, 1, 1)
    m = np.arange(KZ).reshape(KZ, 1, 1, 1, 1)
    q = np.arange(QP).reshape(1, 1, 1, 1, QP)
    full = (KZ, AS, LO, 8, QP)
    return np.stack(
        [
            np.broadcast_to(a, full),
            np.broadcast_to(32 * (q - QS // 2) + lo, full),
            np.broadcast_to((m - KZ // 2) * (NX // NZ), full),
        ]
    ).reshape(3 * MODES, 128)


def dot(lhs, rhs):
    return lax.dot_general(
        lhs, rhs, (((1,), (0,)), ((), ())), preferred_element_type=jnp.float32
    )


def dot_nt(lhs, rhs):
    return lax.dot_general(
        lhs, rhs, (((1,), (1,)), ((), ())), preferred_element_type=jnp.float32
    )


def to_bf16(values):
    return values.astype(jnp.bfloat16)


def flat_rows(ref, *lead):
    return ref[lead].reshape(2 * YL, NX) if lead else ref[...].reshape(2 * YL, NX)


def x_forward_kernel(
    phase_hbm, vel_hbm, table_hbm, out_ref, phase_ref, vel_ref, table_ref, sems
):
    copies = [
        pltpu.make_async_copy(src, dst, sems.at[i])
        for i, (src, dst) in enumerate(
            [(phase_hbm, phase_ref), (vel_hbm, vel_ref), (table_hbm, table_ref)]
        )
    ]
    for c in copies:
        c.start()
    for c in copies:
        c.wait()
    x = jnp.concatenate(
        [flat_rows(phase_ref)] + [flat_rows(vel_ref, j) for j in range(3)], axis=0
    )
    out_ref[...] = to_bf16(dot_nt(table_ref[...], to_bf16(x)))


def y_forward_kernel(in_ref, left_ref, cos_ref, sin_ref, right_ref, out_ref, wide):
    half = in_ref.shape[0] // 2
    sums = dot(left_ref[...], in_ref[...])
    re, im = sums[:half], sums[half:]
    c, s = cos_ref[...], sin_ref[...]
    lines = jnp.concatenate([to_bf16(re * c + im * s), to_bf16(im * c - re * s)], axis=1)
    modes = dot(lines, right_ref[...])
    for p in range(2):
        wide[pl.ds(p, half, stride=2), :] = modes[:, 128 * p : 128 * (p + 1)]
    out_ref[...] = to_bf16(wide[...])


def y_inverse_kernel(in_ref, left_ref, cos_ref, sin_ref, right_ref, out_ref, wide):
    half = in_ref.shape[0] // 2
    wide[...] = in_ref[...].astype(jnp.float32)
    modes = jnp.concatenate(
        [to_bf16(wide[pl.ds(p, half, stride=2), :]) for p in range(2)], axis=1
    )
    lines = dot(modes, right_ref[...])
    re, im = lines[:, :128], lines[:, 128:]
    c, s = cos_ref[...], sin_ref[...]
    spun = jnp.concatenate([to_bf16(re * c - im * s), to_bf16(re * s + im * c)], axis=0)
    out_ref[...] = to_bf16(dot(left_ref[...], spun))


def wave_numbers(wave_ref):
    kx = wave_ref[0:MODES] + (lax.axis_index("col") * AS).astype(jnp.float32)
    ky = wave_ref[MODES : 2 * MODES] + (lax.axis_index("row") * LO).astype(jnp.float32)
    kz = wave_ref[2 * MODES : 3 * MODES]
    slot = lax.broadcasted_iota(jnp.int32, (MODES, 128), 1) // QP
    return kx, ky, kz, kx * kx + ky * ky + kz * kz, slot


def derive_kernel(
    in_ref, spread_ref, left_ref, wave_ref, back_ref, out_ref, spectra_ref
):
    spread = to_bf16(dot(in_ref[...], spread_ref[...]))
    modes = dot(left_ref[...], jnp.concatenate([spread[:, :256], spread[:, 256:]], axis=0))
    spectra_ref[...] = modes[:, 128:]
    kx, ky, kz, k2, slot = wave_numbers(wave_ref)
    one = jnp.where(
        (slot == 0) | (slot == 6),
        kx,
        jnp.where(
            (slot == 1) | (slot == 4),
            ky,
            jnp.where((slot == 2) | (slot == 5), kz, jnp.where(slot == 3, -k2, 0.0)),
        ),
    )
    two = jnp.where(
        slot == 4, kz, jnp.where(slot == 5, kx, jnp.where(slot == 6, ky, 0.0))
    )
    re = modes[:MODES, :128] * one - modes[:MODES, 128:] * two
    im = modes[MODES:, :128] * one - modes[MODES:, 128:] * two
    plain = slot == 3
    coeff = jnp.concatenate(
        [to_bf16(jnp.where(plain, re, -im)), to_bf16(jnp.where(plain, im, re))], axis=0
    )
    out_ref[...] = to_bf16(dot(back_ref[...], coeff))


def solve_kernel(in_ref, spectra_ref, left_ref, wave_ref, back_ref, out_ref):
    modes = dot(left_ref[...], in_ref[...])
    kx, ky, kz, k2, slot = wave_numbers(wave_ref)
    scalar = slot == 0
    stable = 1.0 / time_step + mobility * stabilizer * k2
    below = jnp.where(
        scalar,
        stable + mobility * epsilon * epsilon * k2 * k2,
        1.0 / time_step + k2 / reynolds,
    )
    used = slot < 4
    inv = jnp.where(used, 1.0 / below, 0.0)
    keep = jnp.where(scalar, stable, 1.0 / time_step)
    mean = scalar & (k2 == 0.0)
    sign = jnp.where(mean, 0.0, jnp.where(scalar, -1.0, 1.0))
    bulk = jnp.where(scalar, mobility * k2, 0.0)
    wave = jnp.where(
        slot == 1, kx, jnp.where(slot == 2, ky, jnp.where(slot == 3, kz, 0.0))
    )
    shared = wave / jnp.maximum(k2, 1.0)
    parts = []
    for p in range(2):
        now = modes[p * MODES : (p + 1) * MODES]
        old = spectra_ref[p * MODES : (p + 1) * MODES]
        fresh = (keep * old + sign * now - bulk * pltpu.roll(now, 64, 1)) * inv
        normal = wave * fresh
        for step in (16, 32, 64):
            normal = normal + pltpu.roll(normal, step, 1)
        parts.append(to_bf16(fresh - shared * normal))
    both = dot(back_ref[...], jnp.concatenate(parts, axis=0))
    half = both.shape[0] // 2
    out_ref[...] = to_bf16(both[:half] + pltpu.roll(both[half:], 64, 1))


def nonlinear_kernel(in_ref, phase_ref, vel_ref, back_ref, table_ref, out_ref, wide):
    wide[...] = in_ref[...].astype(jnp.float32)
    for z in range(2):
        lines = to_bf16(wide[pl.ds(z, LINES, stride=2), :].T)
        values = dot(lines, back_ref[...])
        d = [values[YL * f : YL * (f + 1)] for f in range(7)]
        phase = phase_ref[:, z, :]
        v = [vel_ref[j, :, z, :] for j in range(3)]
        g, lap, w = d[0:3], d[3], d[4:7]
        advect = v[0] * g[0] + v[1] * g[1] + v[2] * g[2]
        bulk = phase * phase * phase - phase
        potential = bulk - epsilon * epsilon * lap
        terms = [
            advect,
            v[1] * w[2] - v[2] * w[1] + potential * g[0],
            v[2] * w[0] - v[0] * w[2] + potential * g[1],
            v[0] * w[1] - v[1] * w[0] + potential * g[2],
            bulk,
            jnp.zeros((3 * YL, NX), jnp.float32),
        ]
        x = jnp.concatenate([to_bf16(t) for t in terms], axis=0)
        wide[pl.ds(z, LINES, stride=2), :] = dot_nt(table_ref[...], x)
    out_ref[...] = to_bf16(wide[...])


def x_inverse_kernel(in_ref, back_ref, phase_ref, vel_ref):
    lines = to_bf16(in_ref[...].astype(jnp.float32).T)
    values = dot(lines, back_ref[...])
    phase_ref[...] = values[0:32].reshape(YL, 2, NX)
    for j in range(3):
        vel_ref[j] = values[32 * (j + 1) : 32 * (j + 2)].reshape(YL, 2, NX)


def call(kernel, outs, scratch, *args, space=pltpu.VMEM, traffic=COST // 400):
    vmem = pl.BlockSpec(memory_space=pltpu.VMEM)
    specs = [pl.BlockSpec(memory_space=space)] * len(args)
    return pl.pallas_call(
        kernel,
        in_specs=specs,
        out_specs=[vmem] * len(outs),
        out_shape=outs,
        scratch_shapes=scratch,
        compiler_params=pltpu.CompilerParams(vmem_limit_bytes=16 * 1024 * 1024),
        cost_estimate=pl.CostEstimate(
            flops=COST, bytes_accessed=traffic, transcendentals=0
        ),
    )(*args)


def buffer(rows, dtype=jnp.bfloat16):
    return jax.ShapeDtypeStruct((rows, 128), dtype)


def exchange(values, axis):
    rows = values.shape[0]
    swapped = lax.all_to_all(
        values.reshape(rows // 2, 2, 128), axis, split_axis=0, concat_axis=0, tiled=True
    )
    return swapped.reshape(rows, 128)


def on_device(phase, velocity):
    f32 = jnp.float32
    x_table = as_bf16(x_forward_table())
    x_back = as_bf16(x_inverse_table())
    waves = jnp.asarray(wave_table(), f32)

    def y_tables(zr, direction):
        cos_t, sin_t = twiddles(zr)
        return (
            as_bf16(left_y_table(zr, direction)),
            jnp.asarray(cos_t, f32),
            jnp.asarray(sin_t, f32),
            as_bf16(right_y_table(zr, direction)),
        )

    def y_step(kernel, lines, zr, direction):
        rows = LINES * zr
        return call(
            kernel, [buffer(rows)], [pltpu.VMEM((rows, 128), f32)],
            lines, *y_tables(zr, direction),
        )[0]

    lines = call(
        x_forward_kernel, [buffer(LINES)],
        [
            pltpu.VMEM(phase.shape, f32),
            pltpu.VMEM(velocity.shape, f32),
            pltpu.VMEM(x_table.shape, x_table.dtype),
            pltpu.SemaphoreType.DMA((3,)),
        ],
        *(
            pltpu.with_memory_space_constraint(v, pltpu.HBM)
            for v in (phase, velocity, x_table)
        ),
        space=pltpu.HBM,
    )[0]
    planes = y_step(y_forward_kernel, exchange(lines, "col"), 1, -1)
    planes, spectra = call(
        derive_kernel, [buffer(2 * LINES), buffer(2 * MODES, f32)], [],
        exchange(planes, "row"), as_bf16(spread_table()),
        as_bf16(left_z_table(-1, True)), waves, as_bf16(left_z_table(1, False)),
    )
    lines = y_step(y_inverse_kernel, exchange(planes, "row"), 2, 1)
    lines = call(
        nonlinear_kernel, [buffer(2 * LINES)], [pltpu.VMEM((2 * LINES, 128), f32)],
        exchange(lines, "col"), phase, velocity, x_back, x_table,
    )[0]
    planes = y_step(y_forward_kernel, exchange(lines, "col"), 2, -1)
    planes = call(
        solve_kernel, [buffer(LINES)], [],
        exchange(planes, "row"), spectra, as_bf16(left_z_table(-1, False)), waves,
        as_bf16(left_z_table(1, True)),
    )[0]
    lines = y_step(y_inverse_kernel, exchange(planes, "row"), 1, 1)
    return tuple(
        call(
            x_inverse_kernel,
            [
                jax.ShapeDtypeStruct(phase.shape, f32),
                jax.ShapeDtypeStruct(velocity.shape, f32),
            ],
            [], exchange(lines, "col"), x_back,
        )
    )


def solution(mesh):
    in_specs = (P("col", "row", None), P(None, "col", "row", None))
    out_specs = (P("col", "row", None), P(None, "col", "row", None))
    return jax.shard_map(
        on_device, mesh=mesh, in_specs=in_specs, out_specs=out_specs, check_vma=False
    )
```

```python
import numpy as np

import jax
import jax.numpy as jnp
from jax import lax
from jax.experimental import pallas as pl
from jax.experimental.pallas import tpu as pltpu
from jax.sharding import Mesh
from jax.sharding import PartitionSpec as P

NX = 512
NY = 512
NZ = 32
KC = 192
KZ = 24
COLS = 32
FAR = 2
NEAR = 8
AS = KC // (FAR * COLS)
LO = 32 // NEAR
YL = NY // COLS
QS = 12
QP = 16
BATCH = AS * LO
MODES = KZ * BATCH
LINES = 2 * KC
COST = 10_000_000_000

BIG = ("far", "col")

time_step = 0.001
epsilon = 0.01
mobility = 1.0
reynolds = 100.0
stabilizer = 2.0


def roots(numerator, period):
    angle = (numerator % period) * (2.0 * np.pi / period)
    return np.cos(angle), np.sin(angle)


def as_bf16(values):
    return jnp.asarray(np.asarray(values, np.float32)).astype(jnp.bfloat16)


def x_forward_table():
    c, s = roots(np.arange(KC)[:, None] * np.arange(NX)[None, :], NX)
    return np.stack([c, -s], axis=1).reshape(LINES, NX)


def x_inverse_table():
    c, s = roots(np.arange(KC)[:, None] * np.arange(NX)[None, :], NX)
    w = np.where(np.arange(KC) == 0, 1.0, 2.0)[:, None]
    return np.stack([w * c, -w * s], axis=1).reshape(LINES, NX)


def complex_rotation(c, s):
    return np.array([[c, -s], [s, c]])


def left_y_table(zr, direction):
    k32 = np.arange(32)
    c, s = roots(k32[:, None] * np.arange(COLS)[None, :], 32)
    same = np.einsum("ab,xw,zy->abxwzy", np.eye(AS), np.eye(FAR), np.eye(zr))
    rot = complex_rotation(c, direction * s).reshape(2, 2, NEAR, LO, COLS)
    n = LINES * zr
    if direction < 0:
        return np.einsum("pqrlc,abxwzy->pralxzwcbqy", rot, same).reshape(n, n)
    return np.einsum("pqrlc,abxwzy->xcapzqrblwy", rot, same).reshape(n, n)


def twiddles(zr, lanes):
    k32 = np.arange(32).reshape(NEAR, 1, LO, 1, 1)
    full = (NEAR, AS, LO, FAR * zr, 128)
    c, s = roots(np.broadcast_to(k32 * lanes.reshape(1, 1, 1, 1, 128), full), 512)
    return c.reshape(-1, 128), s.reshape(-1, 128)


def lanes_yz():
    return np.broadcast_to(np.arange(YL)[None, :, None], (4, YL, 2)).reshape(-1)


def lanes_y():
    return np.broadcast_to(np.arange(YL)[None, :], (8, YL)).reshape(-1)


def short_rotation(direction):
    q = np.arange(QS) - QS // 2
    c, s = np.zeros((2, QP, YL))
    c[:QS], s[:QS] = roots(q[:, None] * np.arange(YL)[None, :], 16)
    return complex_rotation(c, direction * s)


def right_y_table(zr, direction):
    rot = short_rotation(direction)
    eye = np.eye
    if zr == 1:
        if direction < 0:
            out = np.einsum("pkqy,fg,zw->kfyzpwgq", rot, eye(4), eye(2))
        else:
            out = np.einsum("pkqy,fg,zw->kzfqpgyw", rot, eye(4), eye(2))
    else:
        out = np.einsum("pkqy,fg->kfqpgy", rot, eye(8))
    return out.reshape(256, 256)


def right_merge_table():
    rot = short_rotation(-1)
    out = np.zeros((2, 16, YL, 2, 2, 8, QP))
    for z in range(2):
        for f in range(4):
            out[:, 4 * z + f, :, z, :, f, :] = np.einsum("pkqy->kypq", rot)
        out[:, 15 - z, :, z, :, 4, :] = np.einsum("pkqy->kypq", rot)
    return out.reshape(512, 512)


def left_z_table(direction, z_major):
    q = np.arange(KZ) - KZ // 2
    c, s = roots(q[:, None] * np.arange(NZ)[None, :], NZ)
    rot = complex_rotation(c, direction * s).reshape(2, 2, KZ, FAR, NEAR, 2)
    same = np.eye(BATCH)
    if direction < 0:
        form = "pkmxsz,ab->pmazsbxk" if z_major else "pkmxsz,ab->pmasbxzk"
        out = np.einsum(form, rot, same).reshape(2 * MODES, -1)
        return out / (NX * NY * NZ)
    form = "pkmxsz,ab->zsaxpkmb" if z_major else "pkmxsz,ab->saxzpkmb"
    return np.einsum(form, rot, same).reshape(-1, 2 * MODES)


def spread_table():
    low = [0, 0, 0, 0]
    high = [3, 1, 2, None]
    plain = [0, 1, 2, 3]
    other = [2, 3, 1, None]
    out = np.zeros((2, 4, QP, 2, 16, QP))
    for slot, f in enumerate(low + high + plain + other):
        if f is not None:
            for z in range(2):
                out[z, f, :, z, slot, :] = np.eye(QP)
    return out.reshape(128, 512)


def wave_table():
    a = np.arange(AS).reshape(1, AS, 1, 1, 1)
    lo = np.arange(LO).reshape(1, 1, LO, 1, 1)
    m = np.arange(KZ).reshape(KZ, 1, 1, 1, 1)
    q = np.arange(QP).reshape(1, 1, 1, 1, QP)
    full = (KZ, AS, LO, 8, QP)
    return np.stack(
        [
            np.broadcast_to(a, full),
            np.broadcast_to(32 * (q - QS // 2) + lo, full),
            np.broadcast_to((m - KZ // 2) * (NX // NZ), full),
        ]
    ).reshape(3 * MODES, 128)


def dot(lhs, rhs):
    return lax.dot_general(
        lhs, rhs, (((1,), (0,)), ((), ())), preferred_element_type=jnp.float32
    )


def dot_nt(lhs, rhs):
    return lax.dot_general(
        lhs, rhs, (((1,), (1,)), ((), ())), preferred_element_type=jnp.float32
    )


def to_bf16(values):
    return values.astype(jnp.bfloat16)


def flat_rows(ref, *lead):
    return ref[lead].reshape(2 * YL, NX) if lead else ref[...].reshape(2 * YL, NX)


def x_forward_kernel(
    phase_hbm, vel_hbm, table_hbm, out_ref, bulk_ref, phase_ref, vel_ref, table_ref,
    sems, wide,
):
    copies = [
        pltpu.make_async_copy(src, dst, sems.at[i])
        for i, (src, dst) in enumerate(
            [(phase_hbm, phase_ref), (vel_hbm, vel_ref), (table_hbm, table_ref)]
        )
    ]
    for c in copies:
        c.start()
    for c in copies:
        c.wait()
    x = jnp.concatenate(
        [flat_rows(phase_ref)] + [flat_rows(vel_ref, j) for j in range(3)], axis=0
    )
    table = table_ref[...]
    out_ref[...] = to_bf16(dot_nt(table, to_bf16(x)))
    for z in range(2):
        phase = phase_ref[:, z, :]
        bulk = to_bf16(phase * phase * phase - phase)
        padded = jnp.concatenate([jnp.zeros((7 * YL, NX), jnp.bfloat16), bulk], axis=0)
        wide[pl.ds(z, LINES, stride=2), :] = dot_nt(table, padded)
    bulk_ref[...] = to_bf16(wide[...])


def y_forward_kernel(in_ref, left_ref, cos_ref, sin_ref, right_ref, out_ref, wide):
    half = in_ref.shape[0] // 2
    sums = dot(left_ref[...], in_ref[...])
    re, im = sums[:half], sums[half:]
    c, s = cos_ref[...], sin_ref[...]
    lines = jnp.concatenate([to_bf16(re * c + im * s), to_bf16(im * c - re * s)], axis=1)
    modes = dot(lines, right_ref[...])
    for p in range(2):
        wide[pl.ds(p, half, stride=2), :] = modes[:, 128 * p : 128 * (p + 1)]
    out_ref[...] = to_bf16(wide[...])


def y_merge_kernel(in_ref, bulk_ref, left_ref, cos_ref, sin_ref, right_ref, out_ref, wide):
    half = in_ref.shape[0] // 2
    sums = dot(left_ref[...], jnp.concatenate([in_ref[...], bulk_ref[...]], axis=1))
    c, s = cos_ref[...], sin_ref[...]
    res, ims = [], []
    for t in range(2):
        re, im = (sums[p * half : (p + 1) * half, 128 * t : 128 * (t + 1)] for p in range(2))
        res.append(to_bf16(re * c + im * s))
        ims.append(to_bf16(im * c - re * s))
    modes = dot(jnp.concatenate(res + ims, axis=1), right_ref[...])
    for t in range(4):
        wide[pl.ds(t, half, stride=4), :] = modes[:, 128 * t : 128 * (t + 1)]
    out_ref[...] = to_bf16(wide[...])


def y_inverse(in_ref, left_ref, cos_ref, sin_ref, right_ref, wide):
    half = in_ref.shape[0] // 2
    wide[...] = in_ref[...].astype(jnp.float32)
    modes = jnp.concatenate(
        [to_bf16(wide[pl.ds(p, half, stride=2), :]) for p in range(2)], axis=1
    )
    lines = dot(modes, right_ref[...])
    re, im = lines[:, :128], lines[:, 128:]
    c, s = cos_ref[...], sin_ref[...]
    spun = jnp.concatenate([to_bf16(re * c - im * s), to_bf16(re * s + im * c)], axis=0)
    return dot(left_ref[...], spun)


def y_inverse_kernel(in_ref, left_ref, cos_ref, sin_ref, right_ref, out_ref, wide):
    out_ref[...] = to_bf16(y_inverse(in_ref, left_ref, cos_ref, sin_ref, right_ref, wide))


def y_inverse_rider_kernel(
    in_ref, rider_ref, left_ref, cos_ref, sin_ref, right_ref, out_ref, wide
):
    lines = y_inverse(in_ref, left_ref, cos_ref, sin_ref, right_ref, wide)
    lane = lax.broadcasted_iota(jnp.int32, lines.shape, 1)
    out_ref[...] = to_bf16(
        jnp.where(lane < 7 * YL, lines, rider_ref[...].astype(jnp.float32))
    )


def wave_numbers(wave_ref):
    kx = wave_ref[0:MODES] + (
        (lax.axis_index("far") * COLS + lax.axis_index("col")) * AS
    ).astype(jnp.float32)
    ky = wave_ref[MODES : 2 * MODES] + (lax.axis_index("near") * LO).astype(jnp.float32)
    kz = wave_ref[2 * MODES : 3 * MODES]
    slot = lax.broadcasted_iota(jnp.int32, (MODES, 128), 1) // QP
    return kx, ky, kz, kx * kx + ky * ky + kz * kz, slot


def derive_kernel(
    in_ref, spread_ref, left_ref, wave_ref, back_ref, out_ref, spectra_ref
):
    spread = to_bf16(dot(in_ref[...], spread_ref[...]))
    modes = dot(left_ref[...], jnp.concatenate([spread[:, :256], spread[:, 256:]], axis=0))
    spectra_ref[...] = modes[:, 128:]
    kx, ky, kz, k2, slot = wave_numbers(wave_ref)
    one = jnp.where(
        (slot == 0) | (slot == 6),
        kx,
        jnp.where(
            (slot == 1) | (slot == 4),
            ky,
            jnp.where((slot == 2) | (slot == 5), kz, jnp.where(slot == 3, -k2, 0.0)),
        ),
    )
    two = jnp.where(
        slot == 4, kz, jnp.where(slot == 5, kx, jnp.where(slot == 6, ky, 0.0))
    )
    re = modes[:MODES, :128] * one - modes[:MODES, 128:] * two
    im = modes[MODES:, :128] * one - modes[MODES:, 128:] * two
    plain = slot == 3
    coeff = jnp.concatenate(
        [to_bf16(jnp.where(plain, re, -im)), to_bf16(jnp.where(plain, im, re))], axis=0
    )
    out_ref[...] = to_bf16(dot(back_ref[...], coeff))


def solve_kernel(in_ref, spectra_ref, left_ref, wave_ref, back_ref, out_ref):
    modes = dot(left_ref[...], in_ref[...])
    kx, ky, kz, k2, slot = wave_numbers(wave_ref)
    scalar = slot == 0
    stable = 1.0 / time_step + mobility * stabilizer * k2
    below = jnp.where(
        scalar,
        stable + mobility * epsilon * epsilon * k2 * k2,
        1.0 / time_step + k2 / reynolds,
    )
    used = slot < 4
    inv = jnp.where(used, 1.0 / below, 0.0)
    keep = jnp.where(scalar, stable, 1.0 / time_step)
    mean = scalar & (k2 == 0.0)
    sign = jnp.where(mean, 0.0, jnp.where(scalar, -1.0, 1.0))
    bulk = jnp.where(scalar, mobility * k2, 0.0)
    wave = jnp.where(
        slot == 1, kx, jnp.where(slot == 2, ky, jnp.where(slot == 3, kz, 0.0))
    )
    shared = wave / jnp.maximum(k2, 1.0)
    parts = []
    for p in range(2):
        now = modes[p * MODES : (p + 1) * MODES]
        old = spectra_ref[p * MODES : (p + 1) * MODES]
        fresh = (keep * old + sign * now - bulk * pltpu.roll(now, 64, 1)) * inv
        normal = wave * fresh
        for step in (16, 32, 64):
            normal = normal + pltpu.roll(normal, step, 1)
        parts.append(to_bf16(fresh - shared * normal))
    both = dot(back_ref[...], jnp.concatenate(parts, axis=0))
    half = both.shape[0] // 2
    out_ref[...] = to_bf16(both[:half] + pltpu.roll(both[half:], 64, 1))


def nonlinear_kernel(
    in_ref, phase_ref, vel_ref, back_ref, table_ref, out_ref, bulk_ref, wide
):
    wide[...] = in_ref[...].astype(jnp.float32)
    sides = [wide[pl.ds(z, LINES, stride=2), :] for z in range(2)]
    lane = lax.broadcasted_iota(jnp.int32, (LINES, 128), 1)
    bulk_ref[...] = to_bf16(
        jnp.where(lane < 7 * YL, pltpu.roll(sides[1], 7 * YL, 1), sides[0])
    )
    terms = []
    for z in range(2):
        values = dot(to_bf16(sides[z].T), back_ref[...])
        d = [values[YL * f : YL * (f + 1)] for f in range(7)]
        phase = phase_ref[:, z, :]
        v = [vel_ref[j, :, z, :] for j in range(3)]
        g, lap, w = d[0:3], d[3], d[4:7]
        potential = phase * phase * phase - phase - epsilon * epsilon * lap
        terms += [
            v[0] * g[0] + v[1] * g[1] + v[2] * g[2],
            v[1] * w[2] - v[2] * w[1] + potential * g[0],
            v[2] * w[0] - v[0] * w[2] + potential * g[1],
            v[0] * w[1] - v[1] * w[0] + potential * g[2],
        ]
    x = jnp.concatenate([to_bf16(t) for t in terms], axis=0)
    out_ref[...] = to_bf16(dot_nt(table_ref[...], x))


def x_inverse_kernel(in_ref, back_ref, phase_ref, vel_ref):
    lines = to_bf16(in_ref[...].astype(jnp.float32).T)
    values = dot(lines, back_ref[...])
    phase_ref[...] = values[0:32].reshape(YL, 2, NX)
    for j in range(3):
        vel_ref[j] = values[32 * (j + 1) : 32 * (j + 2)].reshape(YL, 2, NX)


def call(kernel, outs, scratch, *args, space=pltpu.VMEM):
    vmem = pl.BlockSpec(memory_space=pltpu.VMEM)
    specs = [pl.BlockSpec(memory_space=space)] * len(args)
    return pl.pallas_call(
        kernel,
        in_specs=specs,
        out_specs=[vmem] * len(outs),
        out_shape=outs,
        scratch_shapes=scratch,
        compiler_params=pltpu.CompilerParams(vmem_limit_bytes=16 * 1024 * 1024),
        cost_estimate=pl.CostEstimate(
            flops=COST, bytes_accessed=COST // 400, transcendentals=0
        ),
    )(*args)


def buffer(rows, dtype=jnp.bfloat16):
    return jax.ShapeDtypeStruct((rows, 128), dtype)


def exchange(values, axis):
    rows = values.shape[0]
    swapped = lax.all_to_all(
        values.reshape(rows // 2, 2, 128), axis, split_axis=0, concat_axis=0, tiled=True
    )
    return swapped.reshape(rows, 128)


def on_device(phase, velocity):
    f32 = jnp.float32
    x_table = as_bf16(x_forward_table())
    x_back = as_bf16(x_inverse_table())
    waves = jnp.asarray(wave_table(), f32)

    def spin(zr, lanes):
        return tuple(jnp.asarray(t, f32) for t in twiddles(zr, lanes))

    def scratch(rows):
        return pltpu.VMEM((rows, 128), f32)

    lines, rider = call(
        x_forward_kernel, [buffer(LINES), buffer(2 * LINES)],
        [
            pltpu.VMEM(phase.shape, f32),
            pltpu.VMEM(velocity.shape, f32),
            pltpu.VMEM(x_table.shape, x_table.dtype),
            pltpu.SemaphoreType.DMA((3,)),
            scratch(2 * LINES),
        ],
        *(
            pltpu.with_memory_space_constraint(v, pltpu.HBM)
            for v in (phase, velocity, x_table)
        ),
        space=pltpu.HBM,
    )
    planes = call(
        y_forward_kernel, [buffer(LINES)], [scratch(LINES)],
        exchange(lines, BIG), as_bf16(left_y_table(1, -1)), *spin(1, lanes_yz()),
        as_bf16(right_y_table(1, -1)),
    )[0]
    planes, spectra = call(
        derive_kernel, [buffer(2 * LINES), buffer(2 * MODES, f32)], [],
        exchange(planes, "near"), as_bf16(spread_table()),
        as_bf16(left_z_table(-1, True)), waves, as_bf16(left_z_table(1, False)),
    )
    lines = call(
        y_inverse_rider_kernel, [buffer(2 * LINES)], [scratch(2 * LINES)],
        exchange(planes, "near"), rider, as_bf16(left_y_table(2, 1)), *spin(2, lanes_y()),
        as_bf16(right_y_table(2, 1)),
    )[0]
    lines, bulk = call(
        nonlinear_kernel, [buffer(LINES), buffer(LINES)], [scratch(2 * LINES)],
        exchange(lines, BIG), phase, velocity, x_back, x_table,
    )
    planes = call(
        y_merge_kernel, [buffer(2 * LINES)], [scratch(2 * LINES)],
        exchange(lines, BIG), bulk, as_bf16(left_y_table(1, -1)), *spin(1, lanes_y()),
        as_bf16(right_merge_table()),
    )[0]
    planes = call(
        solve_kernel, [buffer(LINES)], [],
        exchange(planes, "near"), spectra, as_bf16(left_z_table(-1, False)), waves,
        as_bf16(left_z_table(1, True)),
    )[0]
    lines = call(
        y_inverse_kernel, [buffer(LINES)], [scratch(LINES)],
        exchange(planes, "near"), as_bf16(left_y_table(1, 1)), *spin(1, lanes_yz()),
        as_bf16(right_y_table(1, 1)),
    )[0]
    return tuple(
        call(
            x_inverse_kernel,
            [
                jax.ShapeDtypeStruct(phase.shape, f32),
                jax.ShapeDtypeStruct(velocity.shape, f32),
            ],
            [], exchange(lines, BIG), x_back,
        )
    )


def solution(mesh):
    finer = Mesh(
        mesh.devices.reshape(FAR, NEAR, mesh.shape["col"]), ("far", "near", "col")
    )
    row = ("far", "near")
    in_specs = (P("col", row, None), P(None, "col", row, None))
    out_specs = (P("col", row, None), P(None, "col", row, None))
    return jax.shard_map(
        on_device, mesh=finer, in_specs=in_specs, out_specs=out_specs, check_vma=False
    )
```

```python
import numpy as np

import jax
import jax.numpy as jnp
from jax import lax
from jax.experimental import pallas as pl
from jax.experimental.pallas import tpu as pltpu
from jax.sharding import Mesh
from jax.sharding import PartitionSpec as P

NX = 512
NY = 512
NZ = 32
KC = 192
KZ = 24
COLS = 32
FAR = 2
NEAR = 8
AS = KC // (FAR * COLS)
LO = 32 // NEAR
YL = NY // COLS
QS = 12
QP = 16
MODES = KZ * LO
LINES = 2 * KC
COST = 10_000_000_000

BIG = ("xl", "far", "z")

time_step = 0.001
epsilon = 0.01
mobility = 1.0
reynolds = 100.0
stabilizer = 2.0


def roots(numerator, period):
    angle = (numerator % period) * (2.0 * np.pi / period)
    return np.cos(angle), np.sin(angle)


def as_bf16(values):
    return jnp.asarray(np.asarray(values, np.float32)).astype(jnp.bfloat16)


def x_forward_table():
    c, s = roots(np.arange(KC)[:, None] * np.arange(NX)[None, :], NX)
    return np.stack([c, -s], axis=1).reshape(LINES, NX)


def x_inverse_table():
    c, s = roots(np.arange(KC)[:, None] * np.arange(NX)[None, :], NX)
    w = np.where(np.arange(KC) == 0, 1.0, 2.0)[:, None]
    return np.stack([w * c, -w * s], axis=1).reshape(LINES, NX)


def complex_rotation(c, s):
    return np.array([[c, -s], [s, c]])


def left_y_table(zr, direction):
    k32 = np.arange(32)
    c, s = roots(k32[:, None] * np.arange(COLS)[None, :], 32)
    same = np.einsum("ab,xw,zy->abxwzy", np.eye(AS), np.eye(FAR), np.eye(zr))
    rot = complex_rotation(c, direction * s).reshape(2, 2, NEAR, LO, COLS // 2, 2)
    n = LINES * zr
    if direction < 0:
        return np.einsum("pqrlcd,abxwzy->pralxzdwcbqy", rot, same).reshape(n, n)
    return np.einsum("pqrlcd,abxwzy->dxcapzqrblwy", rot, same).reshape(n, n)


def twiddles(zr, lanes):
    k32 = np.arange(32).reshape(NEAR, 1, LO, 1, 1)
    full = (NEAR, AS, LO, FAR * zr, 128)
    c, s = roots(np.broadcast_to(k32 * lanes.reshape(1, 1, 1, 1, 128), full), 512)
    return c.reshape(-1, 128), s.reshape(-1, 128)


def lanes_yz():
    return np.broadcast_to(np.arange(YL)[None, :, None], (4, YL, 2)).reshape(-1)


def lanes_y():
    return np.broadcast_to(np.arange(YL)[None, :], (8, YL)).reshape(-1)


def short_rotation(direction):
    q = np.arange(QS) - QS // 2
    c, s = np.zeros((2, QP, YL))
    c[:QS], s[:QS] = roots(q[:, None] * np.arange(YL)[None, :], 16)
    return complex_rotation(c, direction * s)


def right_y_table(zr, direction):
    rot = short_rotation(direction)
    eye = np.eye
    if zr == 1:
        if direction < 0:
            out = np.einsum("pkqy,fg,zw->kfyzpwgq", rot, eye(4), eye(2))
        else:
            out = np.einsum("pkqy,fg,zw->kzfqpgyw", rot, eye(4), eye(2))
    else:
        out = np.einsum("pkqy,fg->kfqpgy", rot, eye(8))
    return out.reshape(256, 256)


def right_merge_table():
    rot = short_rotation(-1)
    out = np.zeros((2, 16, YL, 2, 2, 8, QP))
    for z in range(2):
        for f in range(4):
            out[:, 4 * z + f, :, z, :, f, :] = np.einsum("pkqy->kypq", rot)
        out[:, 15 - z, :, z, :, 4, :] = np.einsum("pkqy->kypq", rot)
    return out.reshape(512, 512)


def left_z_table(direction, z_major):
    q = np.arange(KZ) - KZ // 2
    c, s = roots(q[:, None] * np.arange(NZ)[None, :], NZ)
    rot = complex_rotation(c, direction * s).reshape(2, 2, KZ, FAR, NEAR, 2)
    same = np.eye(LO)
    if direction < 0:
        form = "pkmxsz,ab->pmazsbxk" if z_major else "pkmxsz,ab->pmasbxzk"
        out = np.einsum(form, rot, same).reshape(2 * MODES, -1)
        return out / (NX * NY * NZ)
    form = "pkmxsz,ab->zsaxpkmb" if z_major else "pkmxsz,ab->saxzpkmb"
    return np.einsum(form, rot, same).reshape(-1, 2 * MODES)


def spread_table():
    low = [0, 0, 0, 0]
    high = [3, 1, 2, None]
    plain = [0, 1, 2, 3]
    other = [2, 3, 1, None]
    out = np.zeros((2, 4, QP, 2, 16, QP))
    for slot, f in enumerate(low + high + plain + other):
        if f is not None:
            for z in range(2):
                out[z, f, :, z, slot, :] = np.eye(QP)
    return out.reshape(128, 512)


def wave_table():
    lo = np.arange(LO).reshape(1, LO, 1, 1)
    m = np.arange(KZ).reshape(KZ, 1, 1, 1)
    q = np.arange(QP).reshape(1, 1, 1, QP)
    full = (KZ, LO, 8, QP)
    return np.stack(
        [
            np.broadcast_to(32 * (q - QS // 2) + lo, full),
            np.broadcast_to((m - KZ // 2) * (NX // NZ), full),
        ]
    ).reshape(2 * MODES, 128)


def dot(lhs, rhs):
    return lax.dot_general(
        lhs, rhs, (((1,), (0,)), ((), ())), preferred_element_type=jnp.float32
    )


def dot_nt(lhs, rhs):
    return lax.dot_general(
        lhs, rhs, (((1,), (1,)), ((), ())), preferred_element_type=jnp.float32
    )


def to_bf16(values):
    return values.astype(jnp.bfloat16)


def flat_rows(ref, *lead):
    return ref[lead].reshape(2 * YL, NX) if lead else ref[...].reshape(2 * YL, NX)


def x_forward_kernel(
    phase_hbm, vel_hbm, table_hbm, out_ref, bulk_ref, phase_ref, vel_ref, table_ref,
    sems, wide,
):
    copies = [
        pltpu.make_async_copy(src, dst, sems.at[i])
        for i, (src, dst) in enumerate(
            [(phase_hbm, phase_ref), (vel_hbm, vel_ref), (table_hbm, table_ref)]
        )
    ]
    for c in copies:
        c.start()
    for c in copies:
        c.wait()
    x = jnp.concatenate(
        [flat_rows(phase_ref)] + [flat_rows(vel_ref, j) for j in range(3)], axis=0
    )
    phases = [phase_ref[:, z, :] for z in range(2)]
    bulk = [to_bf16(p * p * p - p) for p in phases]
    x = jnp.concatenate(
        [to_bf16(x), jnp.zeros((6 * YL, NX), jnp.bfloat16), bulk[1], bulk[0]], axis=0
    )
    lines = dot_nt(table_ref[...], x)
    out_ref[...] = to_bf16(lines[:, :128])
    wide[pl.ds(0, LINES, stride=2), :] = lines[:, 128:]
    wide[pl.ds(1, LINES, stride=2), :] = pltpu.roll(lines[:, 128:], YL, 1)
    bulk_ref[...] = to_bf16(wide[...])


def y_forward_kernel(in_ref, left_ref, cos_ref, sin_ref, right_ref, out_ref, wide):
    half = in_ref.shape[0] // 2
    sums = dot(left_ref[...], in_ref[...])
    re, im = sums[:half], sums[half:]
    c, s = cos_ref[...], sin_ref[...]
    lines = jnp.concatenate([to_bf16(re * c + im * s), to_bf16(im * c - re * s)], axis=1)
    modes = dot(lines, right_ref[...])
    for p in range(2):
        wide[pl.ds(p, half, stride=2), :] = modes[:, 128 * p : 128 * (p + 1)]
    out_ref[...] = to_bf16(wide[...])


def y_merge_kernel(in_ref, bulk_ref, left_ref, cos_ref, sin_ref, right_ref, out_ref, wide):
    half = in_ref.shape[0] // 2
    sums = dot(left_ref[...], jnp.concatenate([in_ref[...], bulk_ref[...]], axis=1))
    c, s = cos_ref[...], sin_ref[...]
    res, ims = [], []
    for t in range(2):
        re, im = (sums[p * half : (p + 1) * half, 128 * t : 128 * (t + 1)] for p in range(2))
        res.append(to_bf16(re * c + im * s))
        ims.append(to_bf16(im * c - re * s))
    modes = dot(jnp.concatenate(res + ims, axis=1), right_ref[...])
    for t in range(4):
        wide[pl.ds(t, half, stride=4), :] = modes[:, 128 * t : 128 * (t + 1)]
    out_ref[...] = to_bf16(wide[...])


def y_inverse(in_ref, left_ref, cos_ref, sin_ref, right_ref, wide):
    half = in_ref.shape[0] // 2
    wide[...] = in_ref[...].astype(jnp.float32)
    modes = jnp.concatenate(
        [to_bf16(wide[pl.ds(p, half, stride=2), :]) for p in range(2)], axis=1
    )
    lines = dot(modes, right_ref[...])
    re, im = lines[:, :128], lines[:, 128:]
    c, s = cos_ref[...], sin_ref[...]
    spun = jnp.concatenate([to_bf16(re * c - im * s), to_bf16(re * s + im * c)], axis=0)
    return dot(left_ref[...], spun)


def y_inverse_kernel(in_ref, left_ref, cos_ref, sin_ref, right_ref, out_ref, wide):
    out_ref[...] = to_bf16(y_inverse(in_ref, left_ref, cos_ref, sin_ref, right_ref, wide))


def y_inverse_rider_kernel(
    in_ref, rider_ref, left_ref, cos_ref, sin_ref, right_ref, out_ref, wide
):
    lines = y_inverse(in_ref, left_ref, cos_ref, sin_ref, right_ref, wide)
    lane = lax.broadcasted_iota(jnp.int32, lines.shape, 1)
    out_ref[...] = to_bf16(
        jnp.where(lane < 7 * YL, lines, rider_ref[...].astype(jnp.float32))
    )


def first_wave():
    owner = (lax.axis_index("xl") * FAR + lax.axis_index("far")) * (COLS // 2)
    return ((owner + lax.axis_index("z")) * AS).astype(jnp.float32)


def cross_waves(wave_ref):
    ky = wave_ref[0:MODES] + (lax.axis_index("near") * LO).astype(jnp.float32)
    kz = wave_ref[MODES : 2 * MODES]
    slot = lax.broadcasted_iota(jnp.int32, (MODES, 128), 1) // QP
    return ky, kz, slot


def rows_of(ref, a):
    block = ref.shape[0] // NEAR
    part = block // AS
    return jnp.concatenate(
        [ref[pl.ds(r * block + a * part, part), :] for r in range(NEAR)], axis=0
    )


def put_rows(ref, a, values):
    block = ref.shape[0] // NEAR
    part = block // AS
    for r in range(NEAR):
        ref[pl.ds(r * block + a * part, part), :] = values[r * part : (r + 1) * part]


def derive_kernel(
    in_ref, spread_ref, left_ref, wave_ref, back_ref, out_ref, spectra_ref
):
    ky, kz, slot = cross_waves(wave_ref)
    across = ky * ky + kz * kz
    plain = slot == 3
    for a in range(AS):
        spread = to_bf16(dot(rows_of(in_ref, a), spread_ref[...]))
        modes = dot(
            left_ref[...], jnp.concatenate([spread[:, :256], spread[:, 256:]], axis=0)
        )
        spectra_ref[pl.ds(2 * MODES * a, 2 * MODES), :] = modes[:, 128:]
        kx = first_wave() + float(a)
        one = jnp.where(
            (slot == 0) | (slot == 6),
            kx,
            jnp.where(
                (slot == 1) | (slot == 4),
                ky,
                jnp.where(
                    (slot == 2) | (slot == 5),
                    kz,
                    jnp.where(plain, -(across + kx * kx), 0.0),
                ),
            ),
        )
        two = jnp.where(
            slot == 4, kz, jnp.where(slot == 5, kx, jnp.where(slot == 6, ky, 0.0))
        )
        re = modes[:MODES, :128] * one - modes[:MODES, 128:] * two
        im = modes[MODES:, :128] * one - modes[MODES:, 128:] * two
        coeff = jnp.concatenate(
            [to_bf16(jnp.where(plain, re, -im)), to_bf16(jnp.where(plain, im, re))],
            axis=0,
        )
        put_rows(out_ref, a, to_bf16(dot(back_ref[...], coeff)))


def solve_kernel(in_ref, spectra_ref, left_ref, wave_ref, back_ref, out_ref):
    ky, kz, slot = cross_waves(wave_ref)
    across = ky * ky + kz * kz
    scalar = slot == 0
    used = slot < 4
    for a in range(AS):
        modes = dot(left_ref[...], rows_of(in_ref, a))
        kx = first_wave() + float(a)
        k2 = across + kx * kx
        stable = 1.0 / time_step + mobility * stabilizer * k2
        below = jnp.where(
            scalar,
            stable + mobility * epsilon * epsilon * k2 * k2,
            1.0 / time_step + k2 / reynolds,
        )
        inv = jnp.where(used, 1.0 / below, 0.0)
        keep = jnp.where(scalar, stable, 1.0 / time_step)
        mean = scalar & (k2 == 0.0)
        sign = jnp.where(mean, 0.0, jnp.where(scalar, -1.0, 1.0))
        bulk = jnp.where(scalar, mobility * k2, 0.0)
        wave = jnp.where(
            slot == 1, kx, jnp.where(slot == 2, ky, jnp.where(slot == 3, kz, 0.0))
        )
        shared = wave / jnp.maximum(k2, 1.0)
        parts = []
        for p in range(2):
            now = modes[p * MODES : (p + 1) * MODES]
            old = spectra_ref[pl.ds((2 * a + p) * MODES, MODES), :]
            fresh = (keep * old + sign * now - bulk * pltpu.roll(now, 64, 1)) * inv
            normal = wave * fresh
            for step in (16, 32, 64):
                normal = normal + pltpu.roll(normal, step, 1)
            parts.append(to_bf16(fresh - shared * normal))
        both = dot(back_ref[...], jnp.concatenate(parts, axis=0))
        half = both.shape[0] // 2
        put_rows(out_ref, a, to_bf16(both[:half] + pltpu.roll(both[half:], 64, 1)))


def nonlinear_kernel(
    in_ref, phase_ref, vel_ref, back_ref, table_ref, out_ref, bulk_ref, wide
):
    wide[...] = in_ref[...].astype(jnp.float32)
    sides = [wide[pl.ds(z, LINES, stride=2), :] for z in range(2)]
    lane = lax.broadcasted_iota(jnp.int32, (LINES, 128), 1)
    bulk_ref[...] = to_bf16(
        jnp.where(lane < 7 * YL, pltpu.roll(sides[1], 7 * YL, 1), sides[0])
    )
    terms = []
    for z in range(2):
        values = dot(to_bf16(sides[z].T), back_ref[...])
        d = [values[YL * f : YL * (f + 1)] for f in range(7)]
        phase = phase_ref[:, z, :]
        v = [vel_ref[j, :, z, :] for j in range(3)]
        g, lap, w = d[0:3], d[3], d[4:7]
        potential = phase * phase * phase - phase - epsilon * epsilon * lap
        terms += [
            v[0] * g[0] + v[1] * g[1] + v[2] * g[2],
            v[1] * w[2] - v[2] * w[1] + potential * g[0],
            v[2] * w[0] - v[0] * w[2] + potential * g[1],
            v[0] * w[1] - v[1] * w[0] + potential * g[2],
        ]
    x = jnp.concatenate([to_bf16(t) for t in terms], axis=0)
    out_ref[...] = to_bf16(dot_nt(table_ref[...], x))


def x_inverse_kernel(in_ref, back_ref, phase_ref, vel_ref):
    lines = to_bf16(in_ref[...].astype(jnp.float32).T)
    values = dot(lines, back_ref[...])
    phase_ref[...] = values[0:32].reshape(YL, 2, NX)
    for j in range(3):
        vel_ref[j] = values[32 * (j + 1) : 32 * (j + 2)].reshape(YL, 2, NX)


def call(kernel, outs, scratch, *args, space=pltpu.VMEM):
    vmem = pl.BlockSpec(memory_space=pltpu.VMEM)
    specs = [pl.BlockSpec(memory_space=space)] * len(args)
    return pl.pallas_call(
        kernel,
        in_specs=specs,
        out_specs=[vmem] * len(outs),
        out_shape=outs,
        scratch_shapes=scratch,
        compiler_params=pltpu.CompilerParams(vmem_limit_bytes=16 * 1024 * 1024),
        cost_estimate=pl.CostEstimate(
            flops=COST, bytes_accessed=COST // 400, transcendentals=0
        ),
    )(*args)


def buffer(rows, dtype=jnp.bfloat16):
    return jax.ShapeDtypeStruct((rows, 128), dtype)


def exchange(values, axis):
    rows = values.shape[0]
    swapped = lax.all_to_all(
        values.reshape(rows // 2, 2, 128), axis, split_axis=0, concat_axis=0, tiled=True
    )
    return swapped.reshape(rows, 128)


def on_device(phase, velocity):
    f32 = jnp.float32
    x_table = as_bf16(x_forward_table())
    x_back = as_bf16(x_inverse_table())
    waves = jnp.asarray(wave_table(), f32)

    def spin(zr, lanes):
        return tuple(jnp.asarray(t, f32) for t in twiddles(zr, lanes))

    def scratch(rows):
        return pltpu.VMEM((rows, 128), f32)

    lines, rider = call(
        x_forward_kernel, [buffer(LINES), buffer(2 * LINES)],
        [
            pltpu.VMEM(phase.shape, f32),
            pltpu.VMEM(velocity.shape, f32),
            pltpu.VMEM(x_table.shape, x_table.dtype),
            pltpu.SemaphoreType.DMA((3,)),
            scratch(2 * LINES),
        ],
        *(
            pltpu.with_memory_space_constraint(v, pltpu.HBM)
            for v in (phase, velocity, x_table)
        ),
        space=pltpu.HBM,
    )
    planes = call(
        y_forward_kernel, [buffer(LINES)], [scratch(LINES)],
        exchange(lines, BIG), as_bf16(left_y_table(1, -1)), *spin(1, lanes_yz()),
        as_bf16(right_y_table(1, -1)),
    )[0]
    planes, spectra = call(
        derive_kernel, [buffer(2 * LINES), buffer(2 * MODES * AS, f32)], [],
        exchange(planes, "near"), as_bf16(spread_table()),
        as_bf16(left_z_table(-1, True)), waves, as_bf16(left_z_table(1, False)),
    )
    lines = call(
        y_inverse_rider_kernel, [buffer(2 * LINES)], [scratch(2 * LINES)],
        exchange(planes, "near"), rider, as_bf16(left_y_table(2, 1)), *spin(2, lanes_y()),
        as_bf16(right_y_table(2, 1)),
    )[0]
    lines, bulk = call(
        nonlinear_kernel, [buffer(LINES), buffer(LINES)], [scratch(2 * LINES)],
        exchange(lines, BIG), phase, velocity, x_back, x_table,
    )
    planes = call(
        y_merge_kernel, [buffer(2 * LINES)], [scratch(2 * LINES)],
        exchange(lines, BIG), bulk, as_bf16(left_y_table(1, -1)), *spin(1, lanes_y()),
        as_bf16(right_merge_table()),
    )[0]
    planes = call(
        solve_kernel, [buffer(LINES)], [],
        exchange(planes, "near"), spectra, as_bf16(left_z_table(-1, False)), waves,
        as_bf16(left_z_table(1, True)),
    )[0]
    lines = call(
        y_inverse_kernel, [buffer(LINES)], [scratch(LINES)],
        exchange(planes, "near"), as_bf16(left_y_table(1, 1)), *spin(1, lanes_yz()),
        as_bf16(right_y_table(1, 1)),
    )[0]
    return tuple(
        call(
            x_inverse_kernel,
            [
                jax.ShapeDtypeStruct(phase.shape, f32),
                jax.ShapeDtypeStruct(velocity.shape, f32),
            ],
            [], exchange(lines, BIG), x_back,
        )
    )


def solution(mesh):
    finer = Mesh(
        mesh.devices.reshape(FAR, NEAR, COLS // 2, 2), ("far", "near", "z", "xl")
    )
    row, col = ("far", "near"), ("z", "xl")
    in_specs = (P(col, row, None), P(None, col, row, None))
    out_specs = (P(col, row, None), P(None, col, row, None))
    return jax.shard_map(
        on_device, mesh=finer, in_specs=in_specs, out_specs=out_specs, check_vma=False
    )
```

```python
import numpy as np

import jax
import jax.numpy as jnp
from jax import lax
from jax.experimental import pallas as pl
from jax.experimental.pallas import tpu as pltpu
from jax.sharding import Mesh
from jax.sharding import PartitionSpec as P

NX = 512
NY = 512
NZ = 32
KC = 192
KZ = 24
COLS = 32
FAR = 2
NEAR = 8
AS = KC // (FAR * COLS)
LO = 32 // NEAR
YL = NY // COLS
QS = 12
QP = 16
MODES = KZ * LO
LINES = 2 * KC
COST = 10_000_000_000

BIG = ("xl", "far", "z")

time_step = 0.001
epsilon = 0.01
mobility = 1.0
reynolds = 100.0
stabilizer = 2.0


def roots(numerator, period):
    angle = (numerator % period) * (2.0 * np.pi / period)
    return np.cos(angle), np.sin(angle)


def as_bf16(values):
    return jnp.asarray(np.asarray(values, np.float32)).astype(jnp.bfloat16)


def x_forward_table():
    c, s = roots(np.arange(KC)[:, None] * np.arange(NX)[None, :], NX)
    return np.stack([c, -s], axis=1).reshape(LINES, NX)


def x_inverse_table():
    c, s = roots(np.arange(KC)[:, None] * np.arange(NX)[None, :], NX)
    w = np.where(np.arange(KC) == 0, 1.0, 2.0)[:, None]
    return np.stack([w * c, -w * s], axis=1).reshape(LINES, NX)


def complex_rotation(c, s):
    return np.array([[c, -s], [s, c]])


def left_y_table(zr, direction):
    k32 = np.arange(32)
    c, s = roots(k32[:, None] * np.arange(COLS)[None, :], 32)
    same = np.einsum("ab,xw,zy->abxwzy", np.eye(AS), np.eye(FAR), np.eye(zr))
    rot = complex_rotation(c, direction * s).reshape(2, 2, NEAR, LO, COLS // 2, 2)
    n = LINES * zr
    if direction < 0:
        return np.einsum("pqrlcd,abxwzy->pralxzdwcbqy", rot, same).reshape(n, n)
    return np.einsum("pqrlcd,abxwzy->dxcapzqrblwy", rot, same).reshape(n, n)


def left_y_single_table():
    k32 = np.arange(32)
    c, s = roots(k32[:, None] * np.arange(COLS)[None, :], 32)
    same = np.einsum("xw,zy->xwzy", np.eye(FAR), np.eye(2))
    rot = complex_rotation(c, s).reshape(2, 2, NEAR, LO, COLS // 2, 2)
    return np.einsum("pqrlcd,xwzy->pzdxcqrlwy", rot, same).reshape(256, 256)


def twiddles(count, inner, lanes):
    k32 = np.arange(32).reshape(NEAR, 1, LO, 1, 1)
    full = (NEAR, count, LO, inner, 128)
    c, s = roots(np.broadcast_to(k32 * lanes.reshape(1, 1, 1, 1, 128), full), 512)
    return c.reshape(-1, 128), s.reshape(-1, 128)


def lanes_y():
    return np.broadcast_to(np.arange(YL)[None, :], (8, YL)).reshape(-1)


def short_rotation(direction):
    q = np.arange(QS) - QS // 2
    c, s = np.zeros((2, QP, YL))
    c[:QS], s[:QS] = roots(q[:, None] * np.arange(YL)[None, :], 16)
    return complex_rotation(c, direction * s)


def right_y_table(direction):
    form = "pkqy,fg->kfypgq" if direction < 0 else "pkqy,fg->kfqpgy"
    return np.einsum(form, short_rotation(direction), np.eye(8)).reshape(256, 256)


def right_merge_table():
    rot = short_rotation(-1)
    out = np.zeros((2, 16, YL, 2, 2, 8, QP))
    for z in range(2):
        for f in range(4):
            out[:, 4 * z + f, :, z, :, f, :] = np.einsum("pkqy->kypq", rot)
        out[:, 15 - z, :, z, :, 4, :] = np.einsum("pkqy->kypq", rot)
    return out.reshape(512, 512)


def left_z_table(direction, z_major):
    q = np.arange(KZ) - KZ // 2
    c, s = roots(q[:, None] * np.arange(NZ)[None, :], NZ)
    rot = complex_rotation(c, direction * s).reshape(2, 2, KZ, FAR, NEAR, 2)
    same = np.eye(LO)
    if direction < 0:
        form = "pkmxsz,ab->pmazsbxk" if z_major else "pkmxsz,ab->pmasbxzk"
        out = np.einsum(form, rot, same).reshape(2 * MODES, -1)
        return out / (NX * NY * NZ)
    form = "pkmxsz,ab->zsaxpkmb" if z_major else "pkmxsz,ab->saxzpkmb"
    return np.einsum(form, rot, same).reshape(-1, 2 * MODES)


def spread_table():
    low = [0, 0, 0, 0]
    high = [3, 1, 2, None]
    plain = [0, 1, 2, 3]
    other = [2, 3, 1, None]
    out = np.zeros((2, 4, QP, 2, 16, QP))
    for slot, f in enumerate(low + high + plain + other):
        if f is not None:
            for z in range(2):
                out[z, f, :, z, slot, :] = np.eye(QP)
    return out.reshape(128, 512)


def wave_table():
    lo = np.arange(LO).reshape(1, LO, 1, 1)
    m = np.arange(KZ).reshape(KZ, 1, 1, 1)
    q = np.arange(QP).reshape(1, 1, 1, QP)
    full = (KZ, LO, 8, QP)
    return np.stack(
        [
            np.broadcast_to(32 * (q - QS // 2) + lo, full),
            np.broadcast_to((m - KZ // 2) * (NX // NZ), full),
        ]
    ).reshape(2 * MODES, 128)


def dot(lhs, rhs):
    return lax.dot_general(
        lhs, rhs, (((1,), (0,)), ((), ())), preferred_element_type=jnp.float32
    )


def dot_nt(lhs, rhs):
    return lax.dot_general(
        lhs, rhs, (((1,), (1,)), ((), ())), preferred_element_type=jnp.float32
    )


def to_bf16(values):
    return values.astype(jnp.bfloat16)


TILES = NX // 128


def tiled(values):
    lead = values.shape[:-3]
    split = values.reshape(*lead, YL, 2, TILES, 128)
    return jnp.swapaxes(split, -3, -2).reshape(*lead, YL * TILES * 2, 128)


def untiled(values):
    lead = values.shape[:-2]
    split = values.reshape(*lead, YL, TILES, 2, 128)
    return jnp.swapaxes(split, -3, -2).reshape(*lead, YL, 2, NX)


def plane(ref, z, *lead):
    return jnp.concatenate(
        [ref[(*lead, pl.ds(2 * t + z, YL, stride=2 * TILES))] for t in range(TILES)], axis=1
    )


def put_plane(ref, z, values, *lead):
    for t in range(TILES):
        ref[(*lead, pl.ds(2 * t + z, YL, stride=2 * TILES))] = values[
            :, 128 * t : 128 * (t + 1)
        ]


def x_forward_kernel(
    phase_hbm, vel_hbm, table_hbm, out_ref, bulk_ref, phase_ref, vel_ref, table_ref,
    sems, wide,
):
    copies = [
        pltpu.make_async_copy(src, dst, sems.at[i])
        for i, (src, dst) in enumerate(
            [(phase_hbm, phase_ref), (vel_hbm, vel_ref), (table_hbm, table_ref)]
        )
    ]
    for c in copies:
        c.start()
    for c in copies[:2]:
        c.wait()
    phases = [plane(phase_ref, z) for z in range(2)]
    rows = []
    for z in range(2):
        rows += [phases[z]] + [plane(vel_ref, z, j) for j in range(3)]
    bulk = [p * p * p - p for p in phases]
    rows += [jnp.zeros((6 * YL, NX), jnp.float32), bulk[1], bulk[0]]
    x = jnp.concatenate([to_bf16(r) for r in rows], axis=0)
    copies[2].wait()
    lines = dot_nt(table_ref[...], x)
    out_ref[...] = to_bf16(lines[:, :128])
    wide[pl.ds(0, LINES, stride=2), :] = lines[:, 128:]
    wide[pl.ds(1, LINES, stride=2), :] = pltpu.roll(lines[:, 128:], YL, 1)
    bulk_ref[...] = to_bf16(wide[...])


def y_forward_kernel(in_ref, left_ref, cos_ref, sin_ref, right_ref, out_ref, wide):
    half = in_ref.shape[0] // 2
    sums = dot(left_ref[...], in_ref[...])
    re, im = sums[:half], sums[half:]
    c, s = cos_ref[...], sin_ref[...]
    lines = jnp.concatenate([to_bf16(re * c + im * s), to_bf16(im * c - re * s)], axis=1)
    modes = dot(lines, right_ref[...])
    for p in range(2):
        wide[pl.ds(p, half, stride=2), :] = modes[:, 128 * p : 128 * (p + 1)]
    out_ref[...] = to_bf16(wide[...])


def y_merge_kernel(in_ref, bulk_ref, left_ref, cos_ref, sin_ref, right_ref, out_ref, wide):
    half = in_ref.shape[0] // 2
    sums = dot(left_ref[...], jnp.concatenate([in_ref[...], bulk_ref[...]], axis=1))
    c, s = cos_ref[...], sin_ref[...]
    res, ims = [], []
    for t in range(2):
        re, im = (sums[p * half : (p + 1) * half, 128 * t : 128 * (t + 1)] for p in range(2))
        res.append(to_bf16(re * c + im * s))
        ims.append(to_bf16(im * c - re * s))
    modes = dot(jnp.concatenate(res + ims, axis=1), right_ref[...])
    for t in range(4):
        wide[pl.ds(t, half, stride=4), :] = modes[:, 128 * t : 128 * (t + 1)]
    out_ref[...] = to_bf16(wide[...])


def y_inverse_kernel(in_ref, left_ref, cos_ref, sin_ref, right_ref, out_ref, wide):
    half = in_ref.shape[0] // 2
    wide[...] = in_ref[...].astype(jnp.float32)
    modes = jnp.concatenate(
        [to_bf16(wide[pl.ds(p, half, stride=2), :]) for p in range(2)], axis=1
    )
    spun = unspun(dot(modes, right_ref[...]), cos_ref[...], sin_ref[...])
    out_ref[...] = to_bf16(dot(left_ref[...], spun))


def unspun(lines, c, s):
    re, im = lines[:, :128], lines[:, 128:]
    return jnp.concatenate([to_bf16(re * c - im * s), to_bf16(re * s + im * c)], axis=0)


def y_inverse_rider_kernel(
    in_ref, rider_ref, left_ref, cos_ref, sin_ref, right_ref, out_ref, wide, lines
):
    block = 2 * LINES // AS
    half = block // 2
    for a in range(AS):
        wide[pl.ds(a * block, block), :] = rows_of(in_ref, a).astype(jnp.float32)
    modes = jnp.concatenate(
        [to_bf16(wide[pl.ds(p, AS * half, stride=2), :]) for p in range(2)], axis=1
    )
    turned = dot(modes, right_ref[...])
    c, s = cos_ref[...], sin_ref[...]
    spun = [unspun(turned[a * half : (a + 1) * half], c, s) for a in range(AS)]
    every = dot(left_ref[...], jnp.concatenate(spun, axis=1))
    for a in range(AS):
        for j in range(4):
            lines[pl.ds(4 * a + j, 64, stride=4 * AS), :] = every[
                64 * j : 64 * (j + 1), 128 * a : 128 * (a + 1)
            ]
    lane = lax.broadcasted_iota(jnp.int32, (2 * LINES, 128), 1)
    out_ref[...] = to_bf16(
        jnp.where(lane < 7 * YL, lines[...], rider_ref[...].astype(jnp.float32))
    )


def first_wave():
    owner = (lax.axis_index("xl") * FAR + lax.axis_index("far")) * (COLS // 2)
    return ((owner + lax.axis_index("z")) * AS).astype(jnp.float32)


def cross_waves(wave_ref):
    ky = wave_ref[0:MODES] + (lax.axis_index("near") * LO).astype(jnp.float32)
    kz = wave_ref[MODES : 2 * MODES]
    slot = lax.broadcasted_iota(jnp.int32, (MODES, 128), 1) // QP
    return ky, kz, slot


def rows_of(ref, a):
    block = ref.shape[0] // NEAR
    part = block // AS
    return jnp.concatenate(
        [ref[pl.ds(r * block + a * part, part), :] for r in range(NEAR)], axis=0
    )


def put_rows(ref, a, values):
    block = ref.shape[0] // NEAR
    part = block // AS
    for r in range(NEAR):
        ref[pl.ds(r * block + a * part, part), :] = values[r * part : (r + 1) * part]


def derive_kernel(
    in_ref, spread_ref, left_ref, wave_ref, back_ref, out_ref, spectra_ref
):
    ky, kz, slot = cross_waves(wave_ref)
    across = ky * ky + kz * kz
    plain = slot == 3
    rows = jnp.concatenate([rows_of(in_ref, a) for a in range(AS)], axis=0)
    spreads = to_bf16(dot(rows, spread_ref[...]))
    part = rows.shape[0] // AS
    stacks = [
        jnp.concatenate([w[:, :256], w[:, 256:]], axis=0)
        for w in (spreads[part * a : part * (a + 1)] for a in range(AS))
    ]
    left = left_ref[...]
    many = [dot(left, stack) for stack in stacks]
    coeffs = []
    for a, modes in enumerate(many):
        spectra_ref[pl.ds(2 * MODES * a, 2 * MODES), :] = modes[:, 128:]
        kx = first_wave() + float(a)
        one = jnp.where(
            (slot == 0) | (slot == 6),
            kx,
            jnp.where(
                (slot == 1) | (slot == 4),
                ky,
                jnp.where(
                    (slot == 2) | (slot == 5),
                    kz,
                    jnp.where(plain, -(across + kx * kx), 0.0),
                ),
            ),
        )
        two = jnp.where(
            slot == 4, kz, jnp.where(slot == 5, kx, jnp.where(slot == 6, ky, 0.0))
        )
        re = modes[:MODES, :128] * one - modes[:MODES, 128:] * two
        im = modes[MODES:, :128] * one - modes[MODES:, 128:] * two
        coeffs.append(
            jnp.concatenate(
                [to_bf16(jnp.where(plain, re, -im)), to_bf16(jnp.where(plain, im, re))],
                axis=0,
            )
        )
    back = dot(back_ref[...], jnp.concatenate(coeffs, axis=1))
    for a in range(AS):
        put_rows(out_ref, a, to_bf16(back[:, 128 * a : 128 * (a + 1)]))


def solve_kernel(in_ref, spectra_ref, left_ref, wave_ref, back_ref, out_ref):
    ky, kz, slot = cross_waves(wave_ref)
    across = ky * ky + kz * kz
    scalar = slot == 0
    used = slot < 4
    many = dot(
        left_ref[...], jnp.concatenate([rows_of(in_ref, a) for a in range(AS)], axis=1)
    )
    coeffs = []
    for a in range(AS):
        modes = many[:, 128 * a : 128 * (a + 1)]
        kx = first_wave() + float(a)
        k2 = across + kx * kx
        stable = 1.0 / time_step + mobility * stabilizer * k2
        below = jnp.where(
            scalar,
            stable + mobility * epsilon * epsilon * k2 * k2,
            1.0 / time_step + k2 / reynolds,
        )
        inv = jnp.where(used, 1.0 / below, 0.0)
        keep = jnp.where(scalar, stable, 1.0 / time_step)
        mean = scalar & (k2 == 0.0)
        sign = jnp.where(mean, 0.0, jnp.where(scalar, -1.0, 1.0))
        bulk = jnp.where(scalar, mobility * k2, 0.0)
        wave = jnp.where(
            slot == 1, kx, jnp.where(slot == 2, ky, jnp.where(slot == 3, kz, 0.0))
        )
        shared = wave / jnp.maximum(k2, 1.0)
        parts = []
        for p in range(2):
            now = modes[p * MODES : (p + 1) * MODES]
            old = spectra_ref[pl.ds((2 * a + p) * MODES, MODES), :]
            fresh = (keep * old + sign * now - bulk * pltpu.roll(now, 64, 1)) * inv
            normal = wave * fresh
            for step in (16, 32, 64):
                normal = normal + pltpu.roll(normal, step, 1)
            parts.append(to_bf16(fresh - shared * normal))
        coeffs.append(jnp.concatenate(parts, axis=0))
    back = dot(back_ref[...], jnp.concatenate(coeffs, axis=1))
    half = back.shape[0] // 2
    for a in range(AS):
        both = back[:, 128 * a : 128 * (a + 1)]
        put_rows(out_ref, a, to_bf16(both[:half] + pltpu.roll(both[half:], 64, 1)))


def nonlinear_kernel(
    in_ref, phase_ref, vel_ref, back_ref, table_ref, out_ref, bulk_ref, wide
):
    wide[...] = in_ref[...].astype(jnp.float32)
    sides = [wide[pl.ds(z, LINES, stride=2), :] for z in range(2)]
    lane = lax.broadcasted_iota(jnp.int32, (LINES, 128), 1)
    bulk_ref[...] = to_bf16(
        jnp.where(lane < 7 * YL, pltpu.roll(sides[1], 7 * YL, 1), sides[0])
    )
    terms = []
    for z in range(2):
        values = dot(to_bf16(sides[z].T), back_ref[...])
        d = [values[YL * f : YL * (f + 1)] for f in range(7)]
        phase = plane(phase_ref, z)
        v = [plane(vel_ref, z, j) for j in range(3)]
        g, lap, w = d[0:3], d[3], d[4:7]
        potential = phase * phase * phase - phase - epsilon * epsilon * lap
        terms += [
            v[0] * g[0] + v[1] * g[1] + v[2] * g[2],
            v[1] * w[2] - v[2] * w[1] + potential * g[0],
            v[2] * w[0] - v[0] * w[2] + potential * g[1],
            v[0] * w[1] - v[1] * w[0] + potential * g[2],
        ]
    x = jnp.concatenate([to_bf16(t) for t in terms], axis=0)
    out_ref[...] = to_bf16(dot_nt(table_ref[...], x))


def x_inverse_kernel(in_ref, back_ref, phase_hbm, vel_hbm, fields, sems):
    lines = to_bf16(in_ref[...].astype(jnp.float32).T)
    values = dot(lines, back_ref[...])
    copies = []
    for f in range(4):
        for z in range(2):
            row = YL * (4 * z + f)
            put_plane(fields, z, values[row : row + YL], f)
        target = phase_hbm if f == 0 else vel_hbm.at[f - 1]
        copies.append(pltpu.make_async_copy(fields.at[f], target, sems.at[f]))
        copies[-1].start()
    for c in copies:
        c.wait()


def call(kernel, outs, scratch, *args, space=pltpu.VMEM, out_space=pltpu.VMEM):
    specs = [pl.BlockSpec(memory_space=space)] * len(args)
    return pl.pallas_call(
        kernel,
        in_specs=specs,
        out_specs=[pl.BlockSpec(memory_space=out_space)] * len(outs),
        out_shape=outs,
        scratch_shapes=scratch,
        compiler_params=pltpu.CompilerParams(vmem_limit_bytes=16 * 1024 * 1024),
        cost_estimate=pl.CostEstimate(
            flops=COST, bytes_accessed=COST // 400, transcendentals=0
        ),
    )(*args)


def buffer(rows, dtype=jnp.bfloat16):
    return jax.ShapeDtypeStruct((rows, 128), dtype)


def exchange(values, axis):
    rows = values.shape[0]
    swapped = lax.all_to_all(
        values.reshape(rows // 2, 2, 128), axis, split_axis=0, concat_axis=0, tiled=True
    )
    return swapped.reshape(rows, 128)


def on_device(phase, velocity):
    phase, velocity = tiled(phase), tiled(velocity)
    f32 = jnp.float32
    x_table = as_bf16(x_forward_table())
    x_back = as_bf16(x_inverse_table())
    waves = jnp.asarray(wave_table(), f32)

    def spin(count, inner):
        return tuple(jnp.asarray(t, f32) for t in twiddles(count, inner, lanes_y()))

    def scratch(rows):
        return pltpu.VMEM((rows, 128), f32)

    lines, rider = call(
        x_forward_kernel, [buffer(LINES), buffer(2 * LINES)],
        [
            pltpu.VMEM(phase.shape, f32),
            pltpu.VMEM(velocity.shape, f32),
            pltpu.VMEM(x_table.shape, x_table.dtype),
            pltpu.SemaphoreType.DMA((3,)),
            scratch(2 * LINES),
        ],
        *(
            pltpu.with_memory_space_constraint(v, pltpu.HBM)
            for v in (phase, velocity, x_table)
        ),
        space=pltpu.HBM,
    )
    planes = call(
        y_forward_kernel, [buffer(LINES)], [scratch(LINES)],
        exchange(lines, BIG), as_bf16(left_y_table(1, -1)), *spin(AS, FAR),
        as_bf16(right_y_table(-1)),
    )[0]
    planes, spectra = call(
        derive_kernel, [buffer(2 * LINES), buffer(2 * MODES * AS, f32)], [],
        exchange(planes, "near"), as_bf16(spread_table()),
        as_bf16(left_z_table(-1, True)), waves, as_bf16(left_z_table(1, False)),
    )
    lines = call(
        y_inverse_rider_kernel, [buffer(2 * LINES)], [scratch(2 * LINES), scratch(2 * LINES)],
        exchange(planes, "near"), rider, as_bf16(left_y_single_table()), *spin(1, 2 * FAR),
        as_bf16(right_y_table(1)),
    )[0]
    lines, bulk = call(
        nonlinear_kernel, [buffer(LINES), buffer(LINES)], [scratch(2 * LINES)],
        exchange(lines, BIG), phase, velocity, x_back, x_table,
    )
    planes = call(
        y_merge_kernel, [buffer(2 * LINES)], [scratch(2 * LINES)],
        exchange(lines, BIG), bulk, as_bf16(left_y_table(1, -1)), *spin(AS, FAR),
        as_bf16(right_merge_table()),
    )[0]
    planes = call(
        solve_kernel, [buffer(LINES)], [],
        exchange(planes, "near"), spectra, as_bf16(left_z_table(-1, False)), waves,
        as_bf16(left_z_table(1, True)),
    )[0]
    lines = call(
        y_inverse_kernel, [buffer(LINES)], [scratch(LINES)],
        exchange(planes, "near"), as_bf16(left_y_table(1, 1)), *spin(AS, FAR),
        as_bf16(right_y_table(1)),
    )[0]
    done = tuple(
        call(
            x_inverse_kernel,
            [
                jax.ShapeDtypeStruct(phase.shape, f32),
                jax.ShapeDtypeStruct(velocity.shape, f32),
            ],
            [pltpu.VMEM((4, *phase.shape), f32), pltpu.SemaphoreType.DMA((4,))],
            exchange(lines, BIG), x_back, out_space=pltpu.HBM,
        )
    )
    return tuple(untiled(v) for v in done)


def solution(mesh):
    finer = Mesh(
        mesh.devices.reshape(FAR, NEAR, COLS // 2, 2), ("far", "near", "z", "xl")
    )
    row, col = ("far", "near"), ("z", "xl")
    in_specs = (P(col, row, None), P(None, col, row, None))
    out_specs = (P(col, row, None), P(None, col, row, None))
    return jax.shard_map(
        on_device, mesh=finer, in_specs=in_specs, out_specs=out_specs, check_vma=False
    )
```

```python
import numpy as np

import jax
import jax.numpy as jnp
from jax import lax
from jax.experimental import pallas as pl
from jax.experimental.pallas import tpu as pltpu
from jax.sharding import Mesh
from jax.sharding import PartitionSpec as P

NX = 512
NY = 512
NZ = 32
KC = 192
KZ = 24
COLS = 32
FAR = 2
NEAR = 8
AS = KC // (FAR * COLS)
LO = 32 // NEAR
YL = NY // COLS
QS = 12
QP = 16
MODES = KZ * LO
LINES = 2 * KC
COST = 10_000_000_000

BIG = ("xl", "far", "z")

time_step = 0.001
epsilon = 0.01
mobility = 1.0
reynolds = 100.0
stabilizer = 2.0


def roots(numerator, period):
    angle = (numerator % period) * (2.0 * np.pi / period)
    return np.cos(angle), np.sin(angle)


def as_bf16(values):
    return jnp.asarray(np.asarray(values, np.float32)).astype(jnp.bfloat16)


def x_forward_table():
    c, s = roots(np.arange(KC)[:, None] * np.arange(NX)[None, :], NX)
    return np.stack([c, -s], axis=1).reshape(LINES, NX)


def x_inverse_table():
    c, s = roots(np.arange(KC)[:, None] * np.arange(NX)[None, :], NX)
    w = np.where(np.arange(KC) == 0, 1.0, 2.0)[:, None]
    return np.stack([w * c, -w * s], axis=1).reshape(LINES, NX)


def complex_rotation(c, s):
    return np.array([[c, -s], [s, c]])


def left_y_table(zr, direction):
    k32 = np.arange(32)
    c, s = roots(k32[:, None] * np.arange(COLS)[None, :], 32)
    same = np.einsum("ab,xw,zy->abxwzy", np.eye(AS), np.eye(FAR), np.eye(zr))
    rot = complex_rotation(c, direction * s).reshape(2, 2, NEAR, LO, COLS // 2, 2)
    n = LINES * zr
    if direction < 0:
        return np.einsum("pqrlcd,abxwzy->pralxzdwcbqy", rot, same).reshape(n, n)
    return np.einsum("pqrlcd,abxwzy->dxcapzqrblwy", rot, same).reshape(n, n)


def left_y_single_table():
    k32 = np.arange(32)
    c, s = roots(k32[:, None] * np.arange(COLS)[None, :], 32)
    same = np.einsum("xw,zy->xwzy", np.eye(FAR), np.eye(2))
    rot = complex_rotation(c, s).reshape(2, 2, NEAR, LO, COLS // 2, 2)
    return np.einsum("pqrlcd,xwzy->pzdxcqrlwy", rot, same).reshape(256, 256)


def twiddles(count, inner, lanes):
    k32 = np.arange(32).reshape(NEAR, 1, LO, 1, 1)
    full = (NEAR, count, LO, inner, 128)
    c, s = roots(np.broadcast_to(k32 * lanes.reshape(1, 1, 1, 1, 128), full), 512)
    return c.reshape(-1, 128), s.reshape(-1, 128)


def lanes_y():
    return np.broadcast_to(np.arange(YL)[None, :], (8, YL)).reshape(-1)


def short_rotation(direction):
    q = np.arange(QS) - QS // 2
    c, s = np.zeros((2, QP, YL))
    c[:QS], s[:QS] = roots(q[:, None] * np.arange(YL)[None, :], 16)
    return complex_rotation(c, direction * s)


def right_y_table(direction):
    form = "pkqy,fg->kfypgq" if direction < 0 else "pkqy,fg->kfqpgy"
    return np.einsum(form, short_rotation(direction), np.eye(8)).reshape(256, 256)


def right_merge_table():
    rot = short_rotation(-1)
    out = np.zeros((2, 16, YL, 2, 2, 8, QP))
    for z in range(2):
        for f in range(4):
            out[:, 4 * z + f, :, z, :, f, :] = np.einsum("pkqy->kypq", rot)
        out[:, 15 - z, :, z, :, 4, :] = np.einsum("pkqy->kypq", rot)
    return out.reshape(512, 512)


def left_z_table(direction, z_major):
    q = np.arange(KZ) - KZ // 2
    c, s = roots(q[:, None] * np.arange(NZ)[None, :], NZ)
    rot = complex_rotation(c, direction * s).reshape(2, 2, KZ, FAR, NEAR, 2)
    same = np.eye(LO)
    if direction < 0:
        form = "pkmxsz,ab->pmazsbxk" if z_major else "pkmxsz,ab->pmasbxzk"
        out = np.einsum(form, rot, same).reshape(2 * MODES, -1)
        return out / (NX * NY * NZ)
    form = "pkmxsz,ab->zsaxpkmb" if z_major else "pkmxsz,ab->saxzpkmb"
    return np.einsum(form, rot, same).reshape(-1, 2 * MODES)


def spread_table():
    low = [0, 0, 0, 0]
    high = [3, 1, 2, None]
    plain = [0, 1, 2, 3]
    other = [2, 3, 1, None]
    out = np.zeros((2, 4, QP, 2, 16, QP))
    for slot, f in enumerate(low + high + plain + other):
        if f is not None:
            for z in range(2):
                out[z, f, :, z, slot, :] = np.eye(QP)
    return out.reshape(128, 512)


def wave_table():
    lo = np.arange(LO).reshape(1, LO, 1, 1)
    m = np.arange(KZ).reshape(KZ, 1, 1, 1)
    q = np.arange(QP).reshape(1, 1, 1, QP)
    full = (KZ, LO, 8, QP)
    return np.stack(
        [
            np.broadcast_to(32 * (q - QS // 2) + lo, full),
            np.broadcast_to((m - KZ // 2) * (NX // NZ), full),
        ]
    ).reshape(2 * MODES, 128)


def dot(lhs, rhs):
    return lax.dot_general(
        lhs, rhs, (((1,), (0,)), ((), ())), preferred_element_type=jnp.float32
    )


def dot_nt(lhs, rhs):
    return lax.dot_general(
        lhs, rhs, (((1,), (1,)), ((), ())), preferred_element_type=jnp.float32
    )


def to_bf16(values):
    return values.astype(jnp.bfloat16)


def two_parts(values):
    high = to_bf16(values)
    return high, to_bf16(values - high.astype(jnp.float32))


TILES = NX // 128


def tiled(values):
    lead = values.shape[:-3]
    split = values.reshape(*lead, YL, 2, TILES, 128)
    return jnp.swapaxes(split, -3, -2).reshape(*lead, YL * TILES * 2, 128)


def untiled(values):
    lead = values.shape[:-2]
    split = values.reshape(*lead, YL, TILES, 2, 128)
    return jnp.swapaxes(split, -3, -2).reshape(*lead, YL, 2, NX)


def plane(ref, z, *lead):
    return jnp.concatenate(
        [ref[(*lead, pl.ds(2 * t + z, YL, stride=2 * TILES))] for t in range(TILES)], axis=1
    )


def put_plane(ref, z, values, *lead):
    for t in range(TILES):
        ref[(*lead, pl.ds(2 * t + z, YL, stride=2 * TILES))] = values[
            :, 128 * t : 128 * (t + 1)
        ]


def x_forward_kernel(
    phase_hbm, vel_hbm, table_hbm, out_ref, bulk_ref, phase_ref, vel_ref, table_ref,
    sems, wide,
):
    copies = [
        pltpu.make_async_copy(src, dst, sems.at[i])
        for i, (src, dst) in enumerate(
            [(phase_hbm, phase_ref), (vel_hbm, vel_ref), (table_hbm, table_ref)]
        )
    ]
    for c in copies:
        c.start()
    for c in copies[:2]:
        c.wait()
    phases = [plane(phase_ref, z) for z in range(2)]
    rows = []
    for z in range(2):
        rows += [phases[z]] + [plane(vel_ref, z, j) for j in range(3)]
    bulk = [p * p * p - p for p in phases]
    rows += [jnp.zeros((6 * YL, NX), jnp.float32), bulk[1], bulk[0]]
    x = jnp.concatenate([to_bf16(r) for r in rows], axis=0)
    copies[2].wait()
    lines = dot_nt(table_ref[...], x)
    out_ref[...] = to_bf16(lines[:, :128])
    wide[pl.ds(0, LINES, stride=2), :] = lines[:, 128:]
    wide[pl.ds(1, LINES, stride=2), :] = pltpu.roll(lines[:, 128:], YL, 1)
    bulk_ref[...] = to_bf16(wide[...])


def y_forward_kernel(in_ref, left_ref, cos_ref, sin_ref, right_ref, out_ref, wide):
    half = in_ref.shape[0] // 2
    sums = dot(left_ref[...], in_ref[...])
    re, im = sums[:half], sums[half:]
    c, s = cos_ref[...], sin_ref[...]
    lines = two_parts(jnp.concatenate([re * c + im * s, im * c - re * s], axis=1))
    modes = dot(lines[0], right_ref[...]) + dot(lines[1], right_ref[...])
    for p in range(2):
        wide[pl.ds(p, half, stride=2), :] = modes[:, 128 * p : 128 * (p + 1)]
    out_ref[...] = to_bf16(wide[...])


def y_merge_kernel(in_ref, bulk_ref, left_ref, cos_ref, sin_ref, right_ref, out_ref, wide):
    half = in_ref.shape[0] // 2
    sums = dot(left_ref[...], jnp.concatenate([in_ref[...], bulk_ref[...]], axis=1))
    c, s = cos_ref[...], sin_ref[...]
    res, ims = [], []
    for t in range(2):
        re, im = (sums[p * half : (p + 1) * half, 128 * t : 128 * (t + 1)] for p in range(2))
        res.append(re * c + im * s)
        ims.append(im * c - re * s)
    lines = two_parts(jnp.concatenate(res + ims, axis=1))
    modes = dot(lines[0], right_ref[...]) + dot(lines[1], right_ref[...])
    for t in range(4):
        wide[pl.ds(t, half, stride=4), :] = modes[:, 128 * t : 128 * (t + 1)]
    out_ref[...] = to_bf16(wide[...])


def y_inverse_kernel(in_ref, left_ref, cos_ref, sin_ref, right_ref, out_ref, wide):
    half = in_ref.shape[0] // 2
    wide[...] = in_ref[...].astype(jnp.float32)
    modes = jnp.concatenate(
        [to_bf16(wide[pl.ds(p, half, stride=2), :]) for p in range(2)], axis=1
    )
    spun = two_parts(unspun(dot(modes, right_ref[...]), cos_ref[...], sin_ref[...]))
    out_ref[...] = to_bf16(dot(left_ref[...], spun[0]) + dot(left_ref[...], spun[1]))


def unspun(lines, c, s):
    re, im = lines[:, :128], lines[:, 128:]
    return jnp.concatenate([re * c - im * s, re * s + im * c], axis=0)


def y_inverse_rider_kernel(
    in_ref, rider_ref, left_ref, cos_ref, sin_ref, right_ref, out_ref, wide, lines
):
    block = 2 * LINES // AS
    half = block // 2
    for a in range(AS):
        wide[pl.ds(a * block, block), :] = rows_of(in_ref, a).astype(jnp.float32)
    modes = jnp.concatenate(
        [to_bf16(wide[pl.ds(p, AS * half, stride=2), :]) for p in range(2)], axis=1
    )
    turned = dot(modes, right_ref[...])
    c, s = cos_ref[...], sin_ref[...]
    spun = [unspun(turned[a * half : (a + 1) * half], c, s) for a in range(AS)]
    spun = two_parts(jnp.concatenate(spun, axis=1))
    every = dot(left_ref[...], spun[0]) + dot(left_ref[...], spun[1])
    for a in range(AS):
        for j in range(4):
            lines[pl.ds(4 * a + j, 64, stride=4 * AS), :] = every[
                64 * j : 64 * (j + 1), 128 * a : 128 * (a + 1)
            ]
    lane = lax.broadcasted_iota(jnp.int32, (2 * LINES, 128), 1)
    out_ref[...] = to_bf16(
        jnp.where(lane < 7 * YL, lines[...], rider_ref[...].astype(jnp.float32))
    )


def first_wave():
    owner = (lax.axis_index("xl") * FAR + lax.axis_index("far")) * (COLS // 2)
    return ((owner + lax.axis_index("z")) * AS).astype(jnp.float32)


def cross_waves(wave_ref):
    ky = wave_ref[0:MODES] + (lax.axis_index("near") * LO).astype(jnp.float32)
    kz = wave_ref[MODES : 2 * MODES]
    slot = lax.broadcasted_iota(jnp.int32, (MODES, 128), 1) // QP
    return ky, kz, slot


def rows_of(ref, a):
    block = ref.shape[0] // NEAR
    part = block // AS
    return jnp.concatenate(
        [ref[pl.ds(r * block + a * part, part), :] for r in range(NEAR)], axis=0
    )


def put_rows(ref, a, values):
    block = ref.shape[0] // NEAR
    part = block // AS
    for r in range(NEAR):
        ref[pl.ds(r * block + a * part, part), :] = values[r * part : (r + 1) * part]


def derive_kernel(
    in_ref, spread_ref, left_ref, wave_ref, back_ref, out_ref, spectra_ref
):
    ky, kz, slot = cross_waves(wave_ref)
    across = ky * ky + kz * kz
    plain = slot == 3
    rows = jnp.concatenate([rows_of(in_ref, a) for a in range(AS)], axis=0)
    spreads = to_bf16(dot(rows, spread_ref[...]))
    part = rows.shape[0] // AS
    stacks = [
        jnp.concatenate([w[:, :256], w[:, 256:]], axis=0)
        for w in (spreads[part * a : part * (a + 1)] for a in range(AS))
    ]
    left = left_ref[...]
    many = [dot(left, stack) for stack in stacks]
    coeffs = []
    for a, modes in enumerate(many):
        spectra_ref[pl.ds(2 * MODES * a, 2 * MODES), :] = modes[:, 128:]
        kx = first_wave() + float(a)
        one = jnp.where(
            (slot == 0) | (slot == 6),
            kx,
            jnp.where(
                (slot == 1) | (slot == 4),
                ky,
                jnp.where(
                    (slot == 2) | (slot == 5),
                    kz,
                    jnp.where(plain, -(across + kx * kx), 0.0),
                ),
            ),
        )
        two = jnp.where(
            slot == 4, kz, jnp.where(slot == 5, kx, jnp.where(slot == 6, ky, 0.0))
        )
        re = modes[:MODES, :128] * one - modes[:MODES, 128:] * two
        im = modes[MODES:, :128] * one - modes[MODES:, 128:] * two
        coeffs.append(
            jnp.concatenate(
                [to_bf16(jnp.where(plain, re, -im)), to_bf16(jnp.where(plain, im, re))],
                axis=0,
            )
        )
    back = dot(back_ref[...], jnp.concatenate(coeffs, axis=1))
    for a in range(AS):
        put_rows(out_ref, a, to_bf16(back[:, 128 * a : 128 * (a + 1)]))


def solve_kernel(in_ref, spectra_ref, left_ref, wave_ref, back_ref, out_ref):
    ky, kz, slot = cross_waves(wave_ref)
    across = ky * ky + kz * kz
    scalar = slot == 0
    used = slot < 4
    many = dot(
        left_ref[...], jnp.concatenate([rows_of(in_ref, a) for a in range(AS)], axis=1)
    )
    coeffs = []
    for a in range(AS):
        modes = many[:, 128 * a : 128 * (a + 1)]
        kx = first_wave() + float(a)
        k2 = across + kx * kx
        stable = 1.0 / time_step + mobility * stabilizer * k2
        below = jnp.where(
            scalar,
            stable + mobility * epsilon * epsilon * k2 * k2,
            1.0 / time_step + k2 / reynolds,
        )
        inv = jnp.where(used, 1.0 / below, 0.0)
        keep = jnp.where(scalar, stable, 1.0 / time_step)
        mean = scalar & (k2 == 0.0)
        sign = jnp.where(mean, 0.0, jnp.where(scalar, -1.0, 1.0))
        bulk = jnp.where(scalar, mobility * k2, 0.0)
        wave = jnp.where(
            slot == 1, kx, jnp.where(slot == 2, ky, jnp.where(slot == 3, kz, 0.0))
        )
        shared = wave / jnp.maximum(k2, 1.0)
        parts = []
        for p in range(2):
            now = modes[p * MODES : (p + 1) * MODES]
            old = spectra_ref[pl.ds((2 * a + p) * MODES, MODES), :]
            fresh = (keep * old + sign * now - bulk * pltpu.roll(now, 64, 1)) * inv
            normal = wave * fresh
            for step in (16, 32, 64):
                normal = normal + pltpu.roll(normal, step, 1)
            parts.append(to_bf16(fresh - shared * normal))
        coeffs.append(jnp.concatenate(parts, axis=0))
    back = dot(back_ref[...], jnp.concatenate(coeffs, axis=1))
    half = back.shape[0] // 2
    for a in range(AS):
        both = back[:, 128 * a : 128 * (a + 1)]
        put_rows(out_ref, a, to_bf16(both[:half] + pltpu.roll(both[half:], 64, 1)))


def nonlinear_kernel(
    in_ref, phase_ref, vel_ref, back_ref, table_ref, out_ref, bulk_ref, wide
):
    wide[...] = in_ref[...].astype(jnp.float32)
    sides = [wide[pl.ds(z, LINES, stride=2), :] for z in range(2)]
    lane = lax.broadcasted_iota(jnp.int32, (LINES, 128), 1)
    bulk_ref[...] = to_bf16(
        jnp.where(lane < 7 * YL, pltpu.roll(sides[1], 7 * YL, 1), sides[0])
    )
    terms = []
    for z in range(2):
        values = dot(to_bf16(sides[z].T), back_ref[...])
        d = [values[YL * f : YL * (f + 1)] for f in range(7)]
        phase = plane(phase_ref, z)
        v = [plane(vel_ref, z, j) for j in range(3)]
        g, lap, w = d[0:3], d[3], d[4:7]
        potential = phase * phase * phase - phase - epsilon * epsilon * lap
        terms += [
            v[0] * g[0] + v[1] * g[1] + v[2] * g[2],
            v[1] * w[2] - v[2] * w[1] + potential * g[0],
            v[2] * w[0] - v[0] * w[2] + potential * g[1],
            v[0] * w[1] - v[1] * w[0] + potential * g[2],
        ]
    x = jnp.concatenate([to_bf16(t) for t in terms], axis=0)
    out_ref[...] = to_bf16(dot_nt(table_ref[...], x))


def x_inverse_kernel(in_ref, back_ref, phase_hbm, vel_hbm, fields, sems):
    lines = to_bf16(in_ref[...].astype(jnp.float32).T)
    values = dot(lines, back_ref[...])
    copies = []
    for f in range(4):
        for z in range(2):
            row = YL * (4 * z + f)
            put_plane(fields, z, values[row : row + YL], f)
        target = phase_hbm if f == 0 else vel_hbm.at[f - 1]
        copies.append(pltpu.make_async_copy(fields.at[f], target, sems.at[f]))
        copies[-1].start()
    for c in copies:
        c.wait()


def call(kernel, outs, scratch, *args, space=pltpu.VMEM, out_space=pltpu.VMEM):
    specs = [pl.BlockSpec(memory_space=space)] * len(args)
    return pl.pallas_call(
        kernel,
        in_specs=specs,
        out_specs=[pl.BlockSpec(memory_space=out_space)] * len(outs),
        out_shape=outs,
        scratch_shapes=scratch,
        compiler_params=pltpu.CompilerParams(vmem_limit_bytes=16 * 1024 * 1024),
        cost_estimate=pl.CostEstimate(
            flops=COST, bytes_accessed=COST // 400, transcendentals=0
        ),
    )(*args)


def buffer(rows, dtype=jnp.bfloat16):
    return jax.ShapeDtypeStruct((rows, 128), dtype)


def exchange(values, axis):
    rows = values.shape[0]
    swapped = lax.all_to_all(
        values.reshape(rows // 2, 2, 128), axis, split_axis=0, concat_axis=0, tiled=True
    )
    return swapped.reshape(rows, 128)


def on_device(phase, velocity):
    phase, velocity = tiled(phase), tiled(velocity)
    f32 = jnp.float32
    x_table = as_bf16(x_forward_table())
    x_back = as_bf16(x_inverse_table())
    waves = jnp.asarray(wave_table(), f32)

    def spin(count, inner):
        return tuple(jnp.asarray(t, f32) for t in twiddles(count, inner, lanes_y()))

    def scratch(rows):
        return pltpu.VMEM((rows, 128), f32)

    lines, rider = call(
        x_forward_kernel, [buffer(LINES), buffer(2 * LINES)],
        [
            pltpu.VMEM(phase.shape, f32),
            pltpu.VMEM(velocity.shape, f32),
            pltpu.VMEM(x_table.shape, x_table.dtype),
            pltpu.SemaphoreType.DMA((3,)),
            scratch(2 * LINES),
        ],
        *(
            pltpu.with_memory_space_constraint(v, pltpu.HBM)
            for v in (phase, velocity, x_table)
        ),
        space=pltpu.HBM,
    )
    planes = call(
        y_forward_kernel, [buffer(LINES)], [scratch(LINES)],
        exchange(lines, BIG), as_bf16(left_y_table(1, -1)), *spin(AS, FAR),
        as_bf16(right_y_table(-1)),
    )[0]
    planes, spectra = call(
        derive_kernel, [buffer(2 * LINES), buffer(2 * MODES * AS, f32)], [],
        exchange(planes, "near"), as_bf16(spread_table()),
        as_bf16(left_z_table(-1, True)), waves, as_bf16(left_z_table(1, False)),
    )
    lines = call(
        y_inverse_rider_kernel, [buffer(2 * LINES)], [scratch(2 * LINES), scratch(2 * LINES)],
        exchange(planes, "near"), rider, as_bf16(left_y_single_table()), *spin(1, 2 * FAR),
        as_bf16(right_y_table(1)),
    )[0]
    lines, bulk = call(
        nonlinear_kernel, [buffer(LINES), buffer(LINES)], [scratch(2 * LINES)],
        exchange(lines, BIG), phase, velocity, x_back, x_table,
    )
    planes = call(
        y_merge_kernel, [buffer(2 * LINES)], [scratch(2 * LINES)],
        exchange(lines, BIG), bulk, as_bf16(left_y_table(1, -1)), *spin(AS, FAR),
        as_bf16(right_merge_table()),
    )[0]
    planes = call(
        solve_kernel, [buffer(LINES)], [],
        exchange(planes, "near"), spectra, as_bf16(left_z_table(-1, False)), waves,
        as_bf16(left_z_table(1, True)),
    )[0]
    lines = call(
        y_inverse_kernel, [buffer(LINES)], [scratch(LINES)],
        exchange(planes, "near"), as_bf16(left_y_table(1, 1)), *spin(AS, FAR),
        as_bf16(right_y_table(1)),
    )[0]
    done = tuple(
        call(
            x_inverse_kernel,
            [
                jax.ShapeDtypeStruct(phase.shape, f32),
                jax.ShapeDtypeStruct(velocity.shape, f32),
            ],
            [pltpu.VMEM((4, *phase.shape), f32), pltpu.SemaphoreType.DMA((4,))],
            exchange(lines, BIG), x_back, out_space=pltpu.HBM,
        )
    )
    return tuple(untiled(v) for v in done)


def solution(mesh):
    finer = Mesh(
        mesh.devices.reshape(FAR, NEAR, COLS // 2, 2), ("far", "near", "z", "xl")
    )
    row, col = ("far", "near"), ("z", "xl")
    in_specs = (P(col, row, None), P(None, col, row, None))
    out_specs = (P(col, row, None), P(None, col, row, None))
    return jax.shard_map(
        on_device, mesh=finer, in_specs=in_specs, out_specs=out_specs, check_vma=False
    )
```

```python
import numpy as np

import jax
import jax.numpy as jnp
from jax import lax
from jax.experimental import pallas as pl
from jax.experimental.pallas import tpu as pltpu
from jax.sharding import Mesh
from jax.sharding import PartitionSpec as P

NX = 512
NY = 512
NZ = 32
KC = 192
KZ = 24
COLS = 32
FAR = 2
NEAR = 8
AS = KC // (FAR * COLS)
LO = 32 // NEAR
YL = NY // COLS
QS = 12
QP = 16
MODES = KZ * LO
LINES = 2 * KC
COST = 10_000_000_000

BIG = ("xl", "far", "z")

time_step = 0.001
epsilon = 0.01
mobility = 1.0
reynolds = 100.0
stabilizer = 2.0


def roots(numerator, period):
    angle = (numerator % period) * (2.0 * np.pi / period)
    return np.cos(angle), np.sin(angle)


def as_bf16(values):
    return jnp.asarray(np.asarray(values, np.float32)).astype(jnp.bfloat16)


def x_forward_table():
    c, s = roots(np.arange(KC)[:, None] * np.arange(NX)[None, :], NX)
    return np.stack([c, -s], axis=1).reshape(LINES, NX)


def x_inverse_table():
    c, s = roots(np.arange(KC)[:, None] * np.arange(NX)[None, :], NX)
    w = np.where(np.arange(KC) == 0, 1.0, 2.0)[:, None]
    return np.stack([w * c, -w * s], axis=1).reshape(LINES, NX)


def complex_rotation(c, s):
    return np.array([[c, -s], [s, c]])


def left_y_table(zr, direction):
    k32 = np.arange(32)
    c, s = roots(k32[:, None] * np.arange(COLS)[None, :], 32)
    same = np.einsum("ab,xw,zy->abxwzy", np.eye(AS), np.eye(FAR), np.eye(zr))
    rot = complex_rotation(c, direction * s).reshape(2, 2, NEAR, LO, COLS // 2, 2)
    n = LINES * zr
    if direction < 0:
        return np.einsum("pqrlcd,abxwzy->pralxzdwcbqy", rot, same).reshape(n, n)
    return np.einsum("pqrlcd,abxwzy->dxcapzqrblwy", rot, same).reshape(n, n)


def left_y_single_table():
    k32 = np.arange(32)
    c, s = roots(k32[:, None] * np.arange(COLS)[None, :], 32)
    same = np.einsum("xw,zy->xwzy", np.eye(FAR), np.eye(2))
    rot = complex_rotation(c, s).reshape(2, 2, NEAR, LO, COLS // 2, 2)
    return np.einsum("pqrlcd,xwzy->pzdxcqrlwy", rot, same).reshape(256, 256)


def twiddles(count, inner, lanes):
    k32 = np.arange(32).reshape(NEAR, 1, LO, 1, 1)
    full = (NEAR, count, LO, inner, 128)
    c, s = roots(np.broadcast_to(k32 * lanes.reshape(1, 1, 1, 1, 128), full), 512)
    return c.reshape(-1, 128), s.reshape(-1, 128)


def lanes_y():
    return np.broadcast_to(np.arange(YL)[None, :], (8, YL)).reshape(-1)


def short_rotation(direction):
    q = np.arange(QS) - QS // 2
    c, s = np.zeros((2, QP, YL))
    c[:QS], s[:QS] = roots(q[:, None] * np.arange(YL)[None, :], 16)
    return complex_rotation(c, direction * s)


def right_y_table(direction):
    form = "pkqy,fg->kfypgq" if direction < 0 else "pkqy,fg->kfqpgy"
    return np.einsum(form, short_rotation(direction), np.eye(8)).reshape(256, 256)


def right_merge_table():
    rot = short_rotation(-1)
    out = np.zeros((2, 16, YL, 2, 2, 8, QP))
    for z in range(2):
        for f in range(4):
            out[:, 4 * z + f, :, z, :, f, :] = np.einsum("pkqy->kypq", rot)
        out[:, 15 - z, :, z, :, 4, :] = np.einsum("pkqy->kypq", rot)
    return out.reshape(512, 512)


def left_z_table(direction, z_major):
    q = np.arange(KZ) - KZ // 2
    c, s = roots(q[:, None] * np.arange(NZ)[None, :], NZ)
    rot = complex_rotation(c, direction * s).reshape(2, 2, KZ, FAR, NEAR, 2)
    same = np.eye(LO)
    if direction < 0:
        form = "pkmxsz,ab->pmazsbxk" if z_major else "pkmxsz,ab->pmasbxzk"
        out = np.einsum(form, rot, same).reshape(2 * MODES, -1)
        return out / (NX * NY * NZ)
    form = "pkmxsz,ab->zsaxpkmb" if z_major else "pkmxsz,ab->saxzpkmb"
    return np.einsum(form, rot, same).reshape(-1, 2 * MODES)


def spread_table():
    low = [0, 0, 0, 0]
    high = [3, 1, 2, None]
    plain = [0, 1, 2, 3]
    other = [2, 3, 1, None]
    out = np.zeros((2, 4, QP, 2, 16, QP))
    for slot, f in enumerate(low + high + plain + other):
        if f is not None:
            for z in range(2):
                out[z, f, :, z, slot, :] = np.eye(QP)
    return out.reshape(128, 512)


def wave_table():
    lo = np.arange(LO).reshape(1, LO, 1, 1)
    m = np.arange(KZ).reshape(KZ, 1, 1, 1)
    q = np.arange(QP).reshape(1, 1, 1, QP)
    full = (KZ, LO, 8, QP)
    return np.stack(
        [
            np.broadcast_to(32 * (q - QS // 2) + lo, full),
            np.broadcast_to((m - KZ // 2) * (NX // NZ), full),
        ]
    ).reshape(2 * MODES, 128)


def dot(lhs, rhs):
    return lax.dot_general(
        lhs, rhs, (((1,), (0,)), ((), ())), preferred_element_type=jnp.float32
    )


def dot_tn(lhs, rhs):
    return lax.dot_general(
        lhs, rhs, (((0,), (0,)), ((), ())), preferred_element_type=jnp.float32
    )


def dot_nt(lhs, rhs):
    return lax.dot_general(
        lhs, rhs, (((1,), (1,)), ((), ())), preferred_element_type=jnp.float32
    )


def to_bf16(values):
    return values.astype(jnp.bfloat16)


TILES = NX // 128


def tiled(values):
    lead = values.shape[:-3]
    split = values.reshape(*lead, YL, 2, TILES, 128)
    return jnp.swapaxes(split, -3, -2).reshape(*lead, YL * TILES * 2, 128)


def untiled(values):
    lead = values.shape[:-2]
    split = values.reshape(*lead, YL, TILES, 2, 128)
    return jnp.swapaxes(split, -3, -2).reshape(*lead, YL, 2, NX)


def plane(ref, z, *lead):
    return jnp.concatenate(
        [ref[(*lead, pl.ds(2 * t + z, YL, stride=2 * TILES))] for t in range(TILES)], axis=1
    )


def put_plane(ref, z, values, *lead):
    for t in range(TILES):
        ref[(*lead, pl.ds(2 * t + z, YL, stride=2 * TILES))] = values[
            :, 128 * t : 128 * (t + 1)
        ]


def x_forward_kernel(
    phase_hbm, vel_hbm, table_hbm, out_ref, bulk_ref, phase_ref, vel_ref, table_ref,
    sems, wide,
):
    copies = [
        pltpu.make_async_copy(src, dst, sems.at[i])
        for i, (src, dst) in enumerate(
            [(phase_hbm, phase_ref), (vel_hbm, vel_ref), (table_hbm, table_ref)]
        )
    ]
    for c in copies:
        c.start()
    for c in copies[:2]:
        c.wait()
    phases = [plane(phase_ref, z) for z in range(2)]
    rows = []
    for z in range(2):
        rows += [phases[z]] + [plane(vel_ref, z, j) for j in range(3)]
    bulk = [p * p * p - p for p in phases]
    rows += [jnp.zeros((6 * YL, NX), jnp.float32), bulk[1], bulk[0]]
    x = jnp.concatenate([to_bf16(r) for r in rows], axis=0)
    copies[2].wait()
    lines = dot_nt(table_ref[...], x)
    out_ref[...] = to_bf16(lines[:, :128])
    wide[pl.ds(0, LINES, stride=2), :] = lines[:, 128:]
    wide[pl.ds(1, LINES, stride=2), :] = pltpu.roll(lines[:, 128:], YL, 1)
    bulk_ref[...] = to_bf16(wide[...])


def y_forward_kernel(in_ref, left_ref, cos_ref, sin_ref, right_ref, out_ref, wide):
    half = in_ref.shape[0] // 2
    sums = dot(left_ref[...], in_ref[...])
    re, im = sums[:half], sums[half:]
    c, s = cos_ref[...], sin_ref[...]
    lines = jnp.concatenate([to_bf16(re * c + im * s), to_bf16(im * c - re * s)], axis=1)
    modes = dot(lines, right_ref[...])
    for p in range(2):
        wide[pl.ds(p, half, stride=2), :] = modes[:, 128 * p : 128 * (p + 1)]
    out_ref[...] = to_bf16(wide[...])


def y_merge_kernel(in_ref, bulk_ref, left_ref, cos_ref, sin_ref, right_ref, out_ref, wide):
    half = in_ref.shape[0] // 2
    sums = dot(left_ref[...], jnp.concatenate([in_ref[...], bulk_ref[...]], axis=1))
    c, s = cos_ref[...], sin_ref[...]
    res, ims = [], []
    for t in range(2):
        re, im = (sums[p * half : (p + 1) * half, 128 * t : 128 * (t + 1)] for p in range(2))
        res.append(to_bf16(re * c + im * s))
        ims.append(to_bf16(im * c - re * s))
    modes = dot(jnp.concatenate(res + ims, axis=1), right_ref[...])
    for t in range(4):
        wide[pl.ds(t, half, stride=4), :] = modes[:, 128 * t : 128 * (t + 1)]
    out_ref[...] = to_bf16(wide[...])


def y_inverse_kernel(in_ref, left_ref, cos_ref, sin_ref, right_ref, out_ref, wide):
    half = in_ref.shape[0] // 2
    wide[...] = in_ref[...].astype(jnp.float32)
    modes = jnp.concatenate(
        [to_bf16(wide[pl.ds(p, half, stride=2), :]) for p in range(2)], axis=1
    )
    spun = unspun(dot(modes, right_ref[...]), cos_ref[...], sin_ref[...])
    out_ref[...] = to_bf16(dot(left_ref[...], spun))


def unspun(lines, c, s):
    re, im = lines[:, :128], lines[:, 128:]
    return jnp.concatenate([to_bf16(re * c - im * s), to_bf16(re * s + im * c)], axis=0)


def y_inverse_rider_kernel(
    in_ref, rider_ref, left_ref, cos_ref, sin_ref, right_ref, out_ref, wide, lines
):
    block = 2 * LINES // AS
    half = block // 2
    for a in range(AS):
        wide[pl.ds(a * block, block), :] = rows_of(in_ref, a).astype(jnp.float32)
    modes = jnp.concatenate(
        [to_bf16(wide[pl.ds(p, AS * half, stride=2), :]) for p in range(2)], axis=1
    )
    turned = dot(modes, right_ref[...])
    c, s = cos_ref[...], sin_ref[...]
    spun = [unspun(turned[a * half : (a + 1) * half], c, s) for a in range(AS)]
    every = dot(left_ref[...], jnp.concatenate(spun, axis=1))
    for a in range(AS):
        for j in range(4):
            lines[pl.ds(4 * a + j, 64, stride=4 * AS), :] = every[
                64 * j : 64 * (j + 1), 128 * a : 128 * (a + 1)
            ]
    lane = lax.broadcasted_iota(jnp.int32, (2 * LINES, 128), 1)
    out_ref[...] = to_bf16(
        jnp.where(lane < 7 * YL, lines[...], rider_ref[...].astype(jnp.float32))
    )


def first_wave():
    owner = (lax.axis_index("xl") * FAR + lax.axis_index("far")) * (COLS // 2)
    return ((owner + lax.axis_index("z")) * AS).astype(jnp.float32)


def cross_waves(wave_ref):
    ky = wave_ref[0:MODES] + (lax.axis_index("near") * LO).astype(jnp.float32)
    kz = wave_ref[MODES : 2 * MODES]
    slot = lax.broadcasted_iota(jnp.int32, (MODES, 128), 1) // QP
    return ky, kz, slot


def rows_of(ref, a):
    block = ref.shape[0] // NEAR
    part = block // AS
    return jnp.concatenate(
        [ref[pl.ds(r * block + a * part, part), :] for r in range(NEAR)], axis=0
    )


def put_rows(ref, a, values):
    block = ref.shape[0] // NEAR
    part = block // AS
    for r in range(NEAR):
        ref[pl.ds(r * block + a * part, part), :] = values[r * part : (r + 1) * part]


def derive_kernel(
    in_ref, spread_ref, left_ref, wave_ref, back_ref, out_ref, spectra_ref
):
    ky, kz, slot = cross_waves(wave_ref)
    across = ky * ky + kz * kz
    plain = slot == 3
    rows = jnp.concatenate([rows_of(in_ref, a) for a in range(AS)], axis=0)
    spreads = to_bf16(dot(rows, spread_ref[...]))
    part = rows.shape[0] // AS
    stacks = [
        jnp.concatenate([w[:, :256], w[:, 256:]], axis=0)
        for w in (spreads[part * a : part * (a + 1)] for a in range(AS))
    ]
    left = left_ref[...]
    many = [dot(left, stack) for stack in stacks]
    coeffs = []
    for a, modes in enumerate(many):
        spectra_ref[pl.ds(2 * MODES * a, 2 * MODES), :] = modes[:, 128:]
        kx = first_wave() + float(a)
        one = jnp.where(
            (slot == 0) | (slot == 6),
            kx,
            jnp.where(
                (slot == 1) | (slot == 4),
                ky,
                jnp.where(
                    (slot == 2) | (slot == 5),
                    kz,
                    jnp.where(plain, -(across + kx * kx), 0.0),
                ),
            ),
        )
        two = jnp.where(
            slot == 4, kz, jnp.where(slot == 5, kx, jnp.where(slot == 6, ky, 0.0))
        )
        re = modes[:MODES, :128] * one - modes[:MODES, 128:] * two
        im = modes[MODES:, :128] * one - modes[MODES:, 128:] * two
        coeffs.append(
            jnp.concatenate(
                [to_bf16(jnp.where(plain, re, -im)), to_bf16(jnp.where(plain, im, re))],
                axis=0,
            )
        )
    back = dot(back_ref[...], jnp.concatenate(coeffs, axis=1))
    for a in range(AS):
        put_rows(out_ref, a, to_bf16(back[:, 128 * a : 128 * (a + 1)]))


def solve_kernel(in_ref, spectra_ref, left_ref, wave_ref, back_ref, out_ref):
    ky, kz, slot = cross_waves(wave_ref)
    across = ky * ky + kz * kz
    scalar = slot == 0
    used = slot < 4
    many = dot(
        left_ref[...], jnp.concatenate([rows_of(in_ref, a) for a in range(AS)], axis=1)
    )
    coeffs = []
    for a in range(AS):
        modes = many[:, 128 * a : 128 * (a + 1)]
        kx = first_wave() + float(a)
        k2 = across + kx * kx
        stable = 1.0 / time_step + mobility * stabilizer * k2
        below = jnp.where(
            scalar,
            stable + mobility * epsilon * epsilon * k2 * k2,
            1.0 / time_step + k2 / reynolds,
        )
        inv = jnp.where(used, 1.0 / below, 0.0)
        keep = jnp.where(scalar, stable, 1.0 / time_step)
        mean = scalar & (k2 == 0.0)
        sign = jnp.where(mean, 0.0, jnp.where(scalar, -1.0, 1.0))
        bulk = jnp.where(scalar, mobility * k2, 0.0)
        wave = jnp.where(
            slot == 1, kx, jnp.where(slot == 2, ky, jnp.where(slot == 3, kz, 0.0))
        )
        shared = wave / jnp.maximum(k2, 1.0)
        parts = []
        for p in range(2):
            now = modes[p * MODES : (p + 1) * MODES]
            old = spectra_ref[pl.ds((2 * a + p) * MODES, MODES), :]
            fresh = (keep * old + sign * now - bulk * pltpu.roll(now, 64, 1)) * inv
            normal = wave * fresh
            for step in (16, 32, 64):
                normal = normal + pltpu.roll(normal, step, 1)
            parts.append(to_bf16(fresh - shared * normal))
        coeffs.append(jnp.concatenate(parts, axis=0))
    back = dot(back_ref[...], jnp.concatenate(coeffs, axis=1))
    half = back.shape[0] // 2
    for a in range(AS):
        both = back[:, 128 * a : 128 * (a + 1)]
        put_rows(out_ref, a, to_bf16(both[:half] + pltpu.roll(both[half:], 64, 1)))


def nonlinear_kernel(
    in_ref, phase_ref, vel_ref, back_ref, table_ref, out_ref, bulk_ref, wide
):
    wide[...] = in_ref[...].astype(jnp.float32)
    sides = [wide[pl.ds(z, LINES, stride=2), :] for z in range(2)]
    lane = lax.broadcasted_iota(jnp.int32, (LINES, 128), 1)
    bulk_ref[...] = to_bf16(
        jnp.where(lane < 7 * YL, pltpu.roll(sides[1], 7 * YL, 1), sides[0])
    )
    terms = []
    for z in range(2):
        values = dot_tn(to_bf16(sides[z]), back_ref[...])
        d = [values[YL * f : YL * (f + 1)] for f in range(7)]
        phase = plane(phase_ref, z)
        v = [plane(vel_ref, z, j) for j in range(3)]
        g, lap, w = d[0:3], d[3], d[4:7]
        potential = phase * phase * phase - phase - epsilon * epsilon * lap
        terms += [
            v[0] * g[0] + v[1] * g[1] + v[2] * g[2],
            v[1] * w[2] - v[2] * w[1] + potential * g[0],
            v[2] * w[0] - v[0] * w[2] + potential * g[1],
            v[0] * w[1] - v[1] * w[0] + potential * g[2],
        ]
    x = jnp.concatenate([to_bf16(t) for t in terms], axis=0)
    out_ref[...] = to_bf16(dot_nt(table_ref[...], x))


def x_inverse_kernel(in_ref, back_ref, phase_hbm, vel_hbm, fields, sems):
    values = dot_tn(in_ref[...], back_ref[...])
    copies = []
    for f in range(4):
        for z in range(2):
            row = YL * (4 * z + f)
            put_plane(fields, z, values[row : row + YL], f)
        target = phase_hbm if f == 0 else vel_hbm.at[f - 1]
        copies.append(pltpu.make_async_copy(fields.at[f], target, sems.at[f]))
        copies[-1].start()
    for c in copies:
        c.wait()


def call(kernel, outs, scratch, *args, space=pltpu.VMEM, out_space=pltpu.VMEM):
    specs = [pl.BlockSpec(memory_space=space)] * len(args)
    return pl.pallas_call(
        kernel,
        in_specs=specs,
        out_specs=[pl.BlockSpec(memory_space=out_space)] * len(outs),
        out_shape=outs,
        scratch_shapes=scratch,
        compiler_params=pltpu.CompilerParams(vmem_limit_bytes=16 * 1024 * 1024),
        cost_estimate=pl.CostEstimate(
            flops=COST, bytes_accessed=COST // 400, transcendentals=0
        ),
    )(*args)


def buffer(rows, dtype=jnp.bfloat16):
    return jax.ShapeDtypeStruct((rows, 128), dtype)


def exchange(values, axis):
    rows = values.shape[0]
    swapped = lax.all_to_all(
        values.reshape(rows // 2, 2, 128), axis, split_axis=0, concat_axis=0, tiled=True
    )
    return swapped.reshape(rows, 128)


def on_device(phase, velocity):
    phase, velocity = tiled(phase), tiled(velocity)
    f32 = jnp.float32
    x_table = as_bf16(x_forward_table())
    x_back = as_bf16(x_inverse_table())
    waves = jnp.asarray(wave_table(), f32)

    def spin(count, inner):
        return tuple(jnp.asarray(t, f32) for t in twiddles(count, inner, lanes_y()))

    def scratch(rows):
        return pltpu.VMEM((rows, 128), f32)

    lines, rider = call(
        x_forward_kernel, [buffer(LINES), buffer(2 * LINES)],
        [
            pltpu.VMEM(phase.shape, f32),
            pltpu.VMEM(velocity.shape, f32),
            pltpu.VMEM(x_table.shape, x_table.dtype),
            pltpu.SemaphoreType.DMA((3,)),
            scratch(2 * LINES),
        ],
        *(
            pltpu.with_memory_space_constraint(v, pltpu.HBM)
            for v in (phase, velocity, x_table)
        ),
        space=pltpu.HBM,
    )
    planes = call(
        y_forward_kernel, [buffer(LINES)], [scratch(LINES)],
        exchange(lines, BIG), as_bf16(left_y_table(1, -1)), *spin(AS, FAR),
        as_bf16(right_y_table(-1)),
    )[0]
    planes, spectra = call(
        derive_kernel, [buffer(2 * LINES), buffer(2 * MODES * AS, f32)], [],
        exchange(planes, "near"), as_bf16(spread_table()),
        as_bf16(left_z_table(-1, True)), waves, as_bf16(left_z_table(1, False)),
    )
    lines = call(
        y_inverse_rider_kernel, [buffer(2 * LINES)], [scratch(2 * LINES), scratch(2 * LINES)],
        exchange(planes, "near"), rider, as_bf16(left_y_single_table()), *spin(1, 2 * FAR),
        as_bf16(right_y_table(1)),
    )[0]
    lines, bulk = call(
        nonlinear_kernel, [buffer(LINES), buffer(LINES)], [scratch(2 * LINES)],
        exchange(lines, BIG), phase, velocity, x_back, x_table,
    )
    planes = call(
        y_merge_kernel, [buffer(2 * LINES)], [scratch(2 * LINES)],
        exchange(lines, BIG), bulk, as_bf16(left_y_table(1, -1)), *spin(AS, FAR),
        as_bf16(right_merge_table()),
    )[0]
    planes = call(
        solve_kernel, [buffer(LINES)], [],
        exchange(planes, "near"), spectra, as_bf16(left_z_table(-1, False)), waves,
        as_bf16(left_z_table(1, True)),
    )[0]
    lines = call(
        y_inverse_kernel, [buffer(LINES)], [scratch(LINES)],
        exchange(planes, "near"), as_bf16(left_y_table(1, 1)), *spin(AS, FAR),
        as_bf16(right_y_table(1)),
    )[0]
    done = tuple(
        call(
            x_inverse_kernel,
            [
                jax.ShapeDtypeStruct(phase.shape, f32),
                jax.ShapeDtypeStruct(velocity.shape, f32),
            ],
            [pltpu.VMEM((4, *phase.shape), f32), pltpu.SemaphoreType.DMA((4,))],
            exchange(lines, BIG), x_back, out_space=pltpu.HBM,
        )
    )
    return tuple(untiled(v) for v in done)


def solution(mesh):
    finer = Mesh(
        mesh.devices.reshape(FAR, NEAR, COLS // 2, 2), ("far", "near", "z", "xl")
    )
    row, col = ("far", "near"), ("z", "xl")
    in_specs = (P(col, row, None), P(None, col, row, None))
    out_specs = (P(col, row, None), P(None, col, row, None))
    return jax.shard_map(
        on_device, mesh=finer, in_specs=in_specs, out_specs=out_specs, check_vma=False
    )
```

```python
import numpy as np

import jax
import jax.numpy as jnp
from jax import lax
from jax.experimental import pallas as pl
from jax.experimental.pallas import tpu as pltpu
from jax.sharding import Mesh
from jax.sharding import PartitionSpec as P

NX = 512
NY = 512
NZ = 32
KC = 192
KZ = 24
COLS = 32
FAR = 2
NEAR = 8
AS = KC // (FAR * COLS)
LO = 32 // NEAR
YL = NY // COLS
QS = 12
QP = 16
MODES = KZ * LO
LINES = 2 * KC
COST = 10_000_000_000

BIG = ("xl", "far", "z")

time_step = 0.001
epsilon = 0.01
mobility = 1.0
reynolds = 100.0
stabilizer = 2.0


def roots(numerator, period):
    angle = (numerator % period) * (2.0 * np.pi / period)
    return np.cos(angle), np.sin(angle)


def as_bf16(values):
    return jnp.asarray(np.asarray(values, np.float32)).astype(jnp.bfloat16)


def x_forward_table():
    c, s = roots(np.arange(KC)[:, None] * np.arange(NX)[None, :], NX)
    return np.stack([c, -s], axis=1).reshape(LINES, NX)


def x_inverse_table():
    c, s = roots(np.arange(KC)[:, None] * np.arange(NX)[None, :], NX)
    w = np.where(np.arange(KC) == 0, 1.0, 2.0)[:, None]
    return np.stack([w * c, -w * s], axis=1).reshape(LINES, NX)


def complex_rotation(c, s):
    return np.array([[c, -s], [s, c]])


def left_y_table(zr, direction):
    k32 = np.arange(32)
    c, s = roots(k32[:, None] * np.arange(COLS)[None, :], 32)
    same = np.einsum("ab,xw,zy->abxwzy", np.eye(AS), np.eye(FAR), np.eye(zr))
    rot = complex_rotation(c, direction * s).reshape(2, 2, NEAR, LO, COLS // 2, 2)
    n = LINES * zr
    if direction < 0:
        return np.einsum("pqrlcd,abxwzy->pralxzdwcbqy", rot, same).reshape(n, n)
    return np.einsum("pqrlcd,abxwzy->dxcapzqrblwy", rot, same).reshape(n, n)


def left_y_single_table():
    k32 = np.arange(32)
    c, s = roots(k32[:, None] * np.arange(COLS)[None, :], 32)
    same = np.einsum("xw,zy->xwzy", np.eye(FAR), np.eye(2))
    rot = complex_rotation(c, s).reshape(2, 2, NEAR, LO, COLS // 2, 2)
    return np.einsum("pqrlcd,xwzy->pzdxcqrlwy", rot, same).reshape(256, 256)


def twiddles(count, inner, lanes):
    k32 = np.arange(32).reshape(NEAR, 1, LO, 1, 1)
    full = (NEAR, count, LO, inner, 128)
    c, s = roots(np.broadcast_to(k32 * lanes.reshape(1, 1, 1, 1, 128), full), 512)
    return c.reshape(-1, 128), s.reshape(-1, 128)


def lanes_y():
    return np.broadcast_to(np.arange(YL)[None, :], (8, YL)).reshape(-1)


def short_rotation(direction):
    q = np.arange(QS) - QS // 2
    c, s = np.zeros((2, QP, YL))
    c[:QS], s[:QS] = roots(q[:, None] * np.arange(YL)[None, :], 16)
    return complex_rotation(c, direction * s)


def right_y_table(direction):
    form = "pkqy,fg->kfypgq" if direction < 0 else "pkqy,fg->kfqpgy"
    return np.einsum(form, short_rotation(direction), np.eye(8)).reshape(256, 256)


def right_merge_table():
    rot = short_rotation(-1)
    out = np.zeros((2, 16, YL, 2, 2, 8, QP))
    for z in range(2):
        for f in range(4):
            out[:, 4 * z + f, :, z, :, f, :] = np.einsum("pkqy->kypq", rot)
        out[:, 15 - z, :, z, :, 4, :] = np.einsum("pkqy->kypq", rot)
    return out.reshape(512, 512)


def left_z_table(direction, z_major):
    q = np.arange(KZ) - KZ // 2
    c, s = roots(q[:, None] * np.arange(NZ)[None, :], NZ)
    rot = complex_rotation(c, direction * s).reshape(2, 2, KZ, FAR, NEAR, 2)
    same = np.eye(LO)
    if direction < 0:
        form = "pkmxsz,ab->pmazsbxk" if z_major else "pkmxsz,ab->pmasbxzk"
        out = np.einsum(form, rot, same).reshape(2 * MODES, -1)
        return out / (NX * NY * NZ)
    form = "pkmxsz,ab->zsaxpkmb" if z_major else "pkmxsz,ab->saxzpkmb"
    return np.einsum(form, rot, same).reshape(-1, 2 * MODES)


def spread_table():
    low = [0, 0, 0, 0]
    high = [3, 1, 2, None]
    plain = [0, 1, 2, 3]
    other = [2, 3, 1, None]
    out = np.zeros((2, 4, QP, 2, 16, QP))
    for slot, f in enumerate(low + high + plain + other):
        if f is not None:
            for z in range(2):
                out[z, f, :, z, slot, :] = np.eye(QP)
    return out.reshape(128, 512)


def wave_table():
    lo = np.arange(LO).reshape(1, LO, 1, 1)
    m = np.arange(KZ).reshape(KZ, 1, 1, 1)
    q = np.arange(QP).reshape(1, 1, 1, QP)
    full = (KZ, LO, 8, QP)
    return np.stack(
        [
            np.broadcast_to(32 * (q - QS // 2) + lo, full),
            np.broadcast_to((m - KZ // 2) * (NX // NZ), full),
        ]
    ).reshape(2 * MODES, 128)


def dot(lhs, rhs):
    return lax.dot_general(
        lhs, rhs, (((1,), (0,)), ((), ())), preferred_element_type=jnp.float32
    )


def dot_tn(lhs, rhs):
    return lax.dot_general(
        lhs, rhs, (((0,), (0,)), ((), ())), preferred_element_type=jnp.float32
    )


def dot_nt(lhs, rhs):
    return lax.dot_general(
        lhs, rhs, (((1,), (1,)), ((), ())), preferred_element_type=jnp.float32
    )


def to_bf16(values):
    return values.astype(jnp.bfloat16)


TILES = NX // 128


def tiled(values):
    lead = values.shape[:-3]
    split = values.reshape(*lead, YL, 2, TILES, 128)
    return jnp.swapaxes(split, -3, -2).reshape(*lead, YL * TILES * 2, 128)


def untiled(values):
    lead = values.shape[:-2]
    split = values.reshape(*lead, YL, TILES, 2, 128)
    return jnp.swapaxes(split, -3, -2).reshape(*lead, YL, 2, NX)


def plane(ref, z, *lead):
    return jnp.concatenate(
        [ref[(*lead, pl.ds(2 * t + z, YL, stride=2 * TILES))] for t in range(TILES)], axis=1
    )


def put_plane(ref, z, values, *lead):
    for t in range(TILES):
        ref[(*lead, pl.ds(2 * t + z, YL, stride=2 * TILES))] = values[
            :, 128 * t : 128 * (t + 1)
        ]


def x_forward_kernel(
    phase_hbm, vel_hbm, table_hbm, out_ref, bulk_ref, phase_ref, vel_ref, table_ref,
    sems, wide,
):
    copies = [
        pltpu.make_async_copy(src, dst, sems.at[i])
        for i, (src, dst) in enumerate(
            [(phase_hbm, phase_ref), (vel_hbm, vel_ref), (table_hbm, table_ref)]
        )
    ]
    for i in (2, 1, 0):
        copies[i].start()
    copies[0].wait()
    phases = [plane(phase_ref, z) for z in range(2)]
    bulk = [p * p * p - p for p in phases]
    copies[1].wait()
    rows = []
    for z in range(2):
        rows += [phases[z]] + [plane(vel_ref, z, j) for j in range(3)]
    rows += [jnp.zeros((6 * YL, NX), jnp.float32), bulk[1], bulk[0]]
    x = jnp.concatenate([to_bf16(r) for r in rows], axis=0)
    copies[2].wait()
    lines = dot_nt(table_ref[...], x)
    out_ref[...] = to_bf16(lines[:, :128])
    wide[pl.ds(0, LINES, stride=2), :] = lines[:, 128:]
    wide[pl.ds(1, LINES, stride=2), :] = pltpu.roll(lines[:, 128:], YL, 1)
    bulk_ref[...] = to_bf16(wide[...])


def y_forward_kernel(in_ref, left_ref, cos_ref, sin_ref, right_ref, out_ref, wide):
    half = in_ref.shape[0] // 2
    sums = dot(left_ref[...], in_ref[...])
    re, im = sums[:half], sums[half:]
    c, s = cos_ref[...], sin_ref[...]
    lines = jnp.concatenate([to_bf16(re * c + im * s), to_bf16(im * c - re * s)], axis=1)
    modes = dot(lines, right_ref[...])
    for p in range(2):
        wide[pl.ds(p, half, stride=2), :] = modes[:, 128 * p : 128 * (p + 1)]
    out_ref[...] = to_bf16(wide[...])


def y_merge_kernel(in_ref, bulk_ref, left_ref, cos_ref, sin_ref, right_ref, out_ref, wide):
    half = in_ref.shape[0] // 2
    sums = dot(left_ref[...], jnp.concatenate([in_ref[...], bulk_ref[...]], axis=1))
    c, s = cos_ref[...], sin_ref[...]
    res, ims = [], []
    for t in range(2):
        re, im = (sums[p * half : (p + 1) * half, 128 * t : 128 * (t + 1)] for p in range(2))
        res.append(to_bf16(re * c + im * s))
        ims.append(to_bf16(im * c - re * s))
    modes = dot(jnp.concatenate(res + ims, axis=1), right_ref[...])
    for t in range(4):
        wide[pl.ds(t, half, stride=4), :] = modes[:, 128 * t : 128 * (t + 1)]
    out_ref[...] = to_bf16(wide[...])


def y_inverse_kernel(in_ref, left_ref, cos_ref, sin_ref, right_ref, out_ref, wide):
    half = in_ref.shape[0] // 2
    wide[...] = in_ref[...].astype(jnp.float32)
    modes = jnp.concatenate(
        [to_bf16(wide[pl.ds(p, half, stride=2), :]) for p in range(2)], axis=1
    )
    spun = unspun(dot(modes, right_ref[...]), cos_ref[...], sin_ref[...])
    out_ref[...] = to_bf16(dot(left_ref[...], spun))


def unspun(lines, c, s):
    re, im = lines[:, :128], lines[:, 128:]
    return jnp.concatenate([to_bf16(re * c - im * s), to_bf16(re * s + im * c)], axis=0)


def y_inverse_rider_kernel(
    in_ref, rider_ref, left_ref, cos_ref, sin_ref, right_ref, out_ref, wide, lines
):
    block = 2 * LINES // AS
    half = block // 2
    for a in range(AS):
        wide[pl.ds(a * block, block), :] = rows_of(in_ref, a).astype(jnp.float32)
    modes = jnp.concatenate(
        [to_bf16(wide[pl.ds(p, AS * half, stride=2), :]) for p in range(2)], axis=1
    )
    turned = dot(modes, right_ref[...])
    c, s = cos_ref[...], sin_ref[...]
    spun = [unspun(turned[a * half : (a + 1) * half], c, s) for a in range(AS)]
    every = dot(left_ref[...], jnp.concatenate(spun, axis=1))
    for a in range(AS):
        for j in range(4):
            lines[pl.ds(4 * a + j, 64, stride=4 * AS), :] = every[
                64 * j : 64 * (j + 1), 128 * a : 128 * (a + 1)
            ]
    lane = lax.broadcasted_iota(jnp.int32, (2 * LINES, 128), 1)
    out_ref[...] = to_bf16(
        jnp.where(lane < 7 * YL, lines[...], rider_ref[...].astype(jnp.float32))
    )


def first_wave():
    owner = (lax.axis_index("xl") * FAR + lax.axis_index("far")) * (COLS // 2)
    return ((owner + lax.axis_index("z")) * AS).astype(jnp.float32)


def cross_waves(wave_ref):
    ky = wave_ref[0:MODES] + (lax.axis_index("near") * LO).astype(jnp.float32)
    kz = wave_ref[MODES : 2 * MODES]
    slot = lax.broadcasted_iota(jnp.int32, (MODES, 128), 1) // QP
    return ky, kz, slot


def rows_of(ref, a):
    block = ref.shape[0] // NEAR
    part = block // AS
    return jnp.concatenate(
        [ref[pl.ds(r * block + a * part, part), :] for r in range(NEAR)], axis=0
    )


def put_rows(ref, a, values):
    block = ref.shape[0] // NEAR
    part = block // AS
    for r in range(NEAR):
        ref[pl.ds(r * block + a * part, part), :] = values[r * part : (r + 1) * part]


def derive_kernel(
    in_ref, spread_ref, left_ref, wave_ref, back_ref, out_ref, spectra_ref
):
    ky, kz, slot = cross_waves(wave_ref)
    across = ky * ky + kz * kz
    plain = slot == 3
    rows = jnp.concatenate([rows_of(in_ref, a) for a in range(AS)], axis=0)
    spreads = to_bf16(dot(rows, spread_ref[...]))
    part = rows.shape[0] // AS
    stacks = [
        jnp.concatenate([w[:, :256], w[:, 256:]], axis=0)
        for w in (spreads[part * a : part * (a + 1)] for a in range(AS))
    ]
    left = left_ref[...]
    many = [dot(left, stack) for stack in stacks]
    coeffs = []
    for a, modes in enumerate(many):
        spectra_ref[pl.ds(2 * MODES * a, 2 * MODES), :] = modes[:, 128:]
        kx = first_wave() + float(a)
        one = jnp.where(
            (slot == 0) | (slot == 6),
            kx,
            jnp.where(
                (slot == 1) | (slot == 4),
                ky,
                jnp.where(
                    (slot == 2) | (slot == 5),
                    kz,
                    jnp.where(plain, -(across + kx * kx), 0.0),
                ),
            ),
        )
        two = jnp.where(
            slot == 4, kz, jnp.where(slot == 5, kx, jnp.where(slot == 6, ky, 0.0))
        )
        re = modes[:MODES, :128] * one - modes[:MODES, 128:] * two
        im = modes[MODES:, :128] * one - modes[MODES:, 128:] * two
        coeffs.append(
            jnp.concatenate(
                [to_bf16(jnp.where(plain, re, -im)), to_bf16(jnp.where(plain, im, re))],
                axis=0,
            )
        )
    back = dot(back_ref[...], jnp.concatenate(coeffs, axis=1))
    for a in range(AS):
        put_rows(out_ref, a, to_bf16(back[:, 128 * a : 128 * (a + 1)]))


def solve_kernel(in_ref, spectra_ref, left_ref, wave_ref, back_ref, out_ref):
    ky, kz, slot = cross_waves(wave_ref)
    across = ky * ky + kz * kz
    scalar = slot == 0
    used = slot < 4
    many = dot(
        left_ref[...], jnp.concatenate([rows_of(in_ref, a) for a in range(AS)], axis=1)
    )
    coeffs = []
    for a in range(AS):
        modes = many[:, 128 * a : 128 * (a + 1)]
        kx = first_wave() + float(a)
        k2 = across + kx * kx
        stable = 1.0 / time_step + mobility * stabilizer * k2
        below = jnp.where(
            scalar,
            stable + mobility * epsilon * epsilon * k2 * k2,
            1.0 / time_step + k2 / reynolds,
        )
        inv = jnp.where(used, 1.0 / below, 0.0)
        keep = jnp.where(scalar, stable, 1.0 / time_step)
        mean = scalar & (k2 == 0.0)
        sign = jnp.where(mean, 0.0, jnp.where(scalar, -1.0, 1.0))
        bulk = jnp.where(scalar, mobility * k2, 0.0)
        wave = jnp.where(
            slot == 1, kx, jnp.where(slot == 2, ky, jnp.where(slot == 3, kz, 0.0))
        )
        shared = wave / jnp.maximum(k2, 1.0)
        parts = []
        for p in range(2):
            now = modes[p * MODES : (p + 1) * MODES]
            old = spectra_ref[pl.ds((2 * a + p) * MODES, MODES), :]
            fresh = (keep * old + sign * now - bulk * pltpu.roll(now, 64, 1)) * inv
            normal = wave * fresh
            for step in (16, 32, 64):
                normal = normal + pltpu.roll(normal, step, 1)
            parts.append(to_bf16(fresh - shared * normal))
        coeffs.append(jnp.concatenate(parts, axis=0))
    back = dot(back_ref[...], jnp.concatenate(coeffs, axis=1))
    half = back.shape[0] // 2
    for a in range(AS):
        both = back[:, 128 * a : 128 * (a + 1)]
        put_rows(out_ref, a, to_bf16(both[:half] + pltpu.roll(both[half:], 64, 1)))


def nonlinear_kernel(
    in_ref, phase_ref, vel_ref, back_ref, table_ref, out_ref, bulk_ref, wide
):
    wide[...] = in_ref[...].astype(jnp.float32)
    sides = [wide[pl.ds(z, LINES, stride=2), :] for z in range(2)]
    lane = lax.broadcasted_iota(jnp.int32, (LINES, 128), 1)
    bulk_ref[...] = to_bf16(
        jnp.where(lane < 7 * YL, pltpu.roll(sides[1], 7 * YL, 1), sides[0])
    )
    terms = []
    for z in range(2):
        values = dot_tn(to_bf16(sides[z]), back_ref[...])
        d = [values[YL * f : YL * (f + 1)] for f in range(7)]
        phase = plane(phase_ref, z)
        v = [plane(vel_ref, z, j) for j in range(3)]
        g, lap, w = d[0:3], d[3], d[4:7]
        potential = phase * phase * phase - phase - epsilon * epsilon * lap
        terms += [
            v[0] * g[0] + v[1] * g[1] + v[2] * g[2],
            v[1] * w[2] - v[2] * w[1] + potential * g[0],
            v[2] * w[0] - v[0] * w[2] + potential * g[1],
            v[0] * w[1] - v[1] * w[0] + potential * g[2],
        ]
    x = jnp.concatenate([to_bf16(t) for t in terms], axis=0)
    out_ref[...] = to_bf16(dot_nt(table_ref[...], x))


def x_inverse_kernel(in_ref, back_ref, phase_hbm, vel_hbm, fields, sems):
    values = dot_tn(in_ref[...], back_ref[...])
    copies = []
    for f in range(4):
        for z in range(2):
            row = YL * (4 * z + f)
            put_plane(fields, z, values[row : row + YL], f)
        target = phase_hbm if f == 0 else vel_hbm.at[f - 1]
        copies.append(pltpu.make_async_copy(fields.at[f], target, sems.at[f]))
        copies[-1].start()
    for c in copies:
        c.wait()


def call(kernel, outs, scratch, *args, space=pltpu.VMEM, out_space=pltpu.VMEM):
    specs = [pl.BlockSpec(memory_space=space)] * len(args)
    return pl.pallas_call(
        kernel,
        in_specs=specs,
        out_specs=[pl.BlockSpec(memory_space=out_space)] * len(outs),
        out_shape=outs,
        scratch_shapes=scratch,
        compiler_params=pltpu.CompilerParams(vmem_limit_bytes=16 * 1024 * 1024),
        cost_estimate=pl.CostEstimate(
            flops=COST, bytes_accessed=COST // 400, transcendentals=0
        ),
    )(*args)


def buffer(rows, dtype=jnp.bfloat16):
    return jax.ShapeDtypeStruct((rows, 128), dtype)


def exchange(values, axis):
    rows = values.shape[0]
    swapped = lax.all_to_all(
        values.reshape(rows // 2, 2, 128), axis, split_axis=0, concat_axis=0, tiled=True
    )
    return swapped.reshape(rows, 128)


def on_device(phase, velocity):
    phase, velocity = tiled(phase), tiled(velocity)
    f32 = jnp.float32
    x_table = as_bf16(x_forward_table())
    x_back = as_bf16(x_inverse_table())
    waves = jnp.asarray(wave_table(), f32)

    def spin(count, inner):
        return tuple(jnp.asarray(t, f32) for t in twiddles(count, inner, lanes_y()))

    def scratch(rows):
        return pltpu.VMEM((rows, 128), f32)

    lines, rider = call(
        x_forward_kernel, [buffer(LINES), buffer(2 * LINES)],
        [
            pltpu.VMEM(phase.shape, f32),
            pltpu.VMEM(velocity.shape, f32),
            pltpu.VMEM(x_table.shape, x_table.dtype),
            pltpu.SemaphoreType.DMA((3,)),
            scratch(2 * LINES),
        ],
        *(
            pltpu.with_memory_space_constraint(v, pltpu.HBM)
            for v in (phase, velocity, x_table)
        ),
        space=pltpu.HBM,
    )
    planes = call(
        y_forward_kernel, [buffer(LINES)], [scratch(LINES)],
        exchange(lines, BIG), as_bf16(left_y_table(1, -1)), *spin(AS, FAR),
        as_bf16(right_y_table(-1)),
    )[0]
    planes, spectra = call(
        derive_kernel, [buffer(2 * LINES), buffer(2 * MODES * AS, f32)], [],
        exchange(planes, "near"), as_bf16(spread_table()),
        as_bf16(left_z_table(-1, True)), waves, as_bf16(left_z_table(1, False)),
    )
    lines = call(
        y_inverse_rider_kernel, [buffer(2 * LINES)], [scratch(2 * LINES), scratch(2 * LINES)],
        exchange(planes, "near"), rider, as_bf16(left_y_single_table()), *spin(1, 2 * FAR),
        as_bf16(right_y_table(1)),
    )[0]
    lines, bulk = call(
        nonlinear_kernel, [buffer(LINES), buffer(LINES)], [scratch(2 * LINES)],
        exchange(lines, BIG), phase, velocity, x_back, x_table,
    )
    planes = call(
        y_merge_kernel, [buffer(2 * LINES)], [scratch(2 * LINES)],
        exchange(lines, BIG), bulk, as_bf16(left_y_table(1, -1)), *spin(AS, FAR),
        as_bf16(right_merge_table()),
    )[0]
    planes = call(
        solve_kernel, [buffer(LINES)], [],
        exchange(planes, "near"), spectra, as_bf16(left_z_table(-1, False)), waves,
        as_bf16(left_z_table(1, True)),
    )[0]
    lines = call(
        y_inverse_kernel, [buffer(LINES)], [scratch(LINES)],
        exchange(planes, "near"), as_bf16(left_y_table(1, 1)), *spin(AS, FAR),
        as_bf16(right_y_table(1)),
    )[0]
    done = tuple(
        call(
            x_inverse_kernel,
            [
                jax.ShapeDtypeStruct(phase.shape, f32),
                jax.ShapeDtypeStruct(velocity.shape, f32),
            ],
            [pltpu.VMEM((4, *phase.shape), f32), pltpu.SemaphoreType.DMA((4,))],
            exchange(lines, BIG), x_back, out_space=pltpu.HBM,
        )
    )
    return tuple(untiled(v) for v in done)


def solution(mesh):
    finer = Mesh(
        mesh.devices.reshape(FAR, NEAR, COLS // 2, 2), ("far", "near", "z", "xl")
    )
    row, col = ("far", "near"), ("z", "xl")
    in_specs = (P(col, row, None), P(None, col, row, None))
    out_specs = (P(col, row, None), P(None, col, row, None))
    return jax.shard_map(
        on_device, mesh=finer, in_specs=in_specs, out_specs=out_specs, check_vma=False
    )
```

```python
import numpy as np

import jax
import jax.numpy as jnp
from jax import lax
from jax.experimental import pallas as pl
from jax.experimental.pallas import tpu as pltpu
from jax.sharding import Mesh
from jax.sharding import PartitionSpec as P

NX = 512
NY = 512
NZ = 32
KC = 192
KZ = 24
COLS = 32
FAR = 2
NEAR = 8
AS = KC // (FAR * COLS)
LO = 32 // NEAR
YL = NY // COLS
QS = 12
QP = 16
MODES = KZ * LO
LINES = 2 * KC
COST = 10_000_000_000

BIG = ("xl", "far", "z")

time_step = 0.001
epsilon = 0.01
mobility = 1.0
reynolds = 100.0
stabilizer = 2.0


def roots(numerator, period):
    angle = (numerator % period) * (2.0 * np.pi / period)
    return np.cos(angle), np.sin(angle)


def as_bf16(values):
    return jnp.asarray(np.asarray(values, np.float32)).astype(jnp.bfloat16)


def x_forward_table():
    c, s = roots(np.arange(KC)[:, None] * np.arange(NX)[None, :], NX)
    return np.stack([c, -s], axis=1).reshape(LINES, NX)


def x_inverse_table():
    c, s = roots(np.arange(KC)[:, None] * np.arange(NX)[None, :], NX)
    w = np.where(np.arange(KC) == 0, 1.0, 2.0)[:, None]
    return np.stack([w * c, -w * s], axis=1).reshape(LINES, NX)


def complex_rotation(c, s):
    return np.array([[c, -s], [s, c]])


def left_y_table(zr, direction):
    k32 = np.arange(32)
    c, s = roots(k32[:, None] * np.arange(COLS)[None, :], 32)
    same = np.einsum("ab,xw,zy->abxwzy", np.eye(AS), np.eye(FAR), np.eye(zr))
    rot = complex_rotation(c, direction * s).reshape(2, 2, NEAR, LO, COLS // 2, 2)
    n = LINES * zr
    if direction < 0:
        return np.einsum("pqrlcd,abxwzy->pralxzdwcbqy", rot, same).reshape(n, n)
    return np.einsum("pqrlcd,abxwzy->dxcapzqrblwy", rot, same).reshape(n, n)


def left_y_single_table():
    k32 = np.arange(32)
    c, s = roots(k32[:, None] * np.arange(COLS)[None, :], 32)
    same = np.einsum("xw,zy->xwzy", np.eye(FAR), np.eye(2))
    rot = complex_rotation(c, s).reshape(2, 2, NEAR, LO, COLS // 2, 2)
    return np.einsum("pqrlcd,xwzy->pzdxcqrlwy", rot, same).reshape(256, 256)


def twiddles(count, inner, lanes):
    k32 = np.arange(32).reshape(NEAR, 1, LO, 1, 1)
    full = (NEAR, count, LO, inner, 128)
    c, s = roots(np.broadcast_to(k32 * lanes.reshape(1, 1, 1, 1, 128), full), 512)
    return c.reshape(-1, 128), s.reshape(-1, 128)


def lanes_y():
    return np.broadcast_to(np.arange(YL)[None, :], (8, YL)).reshape(-1)


def short_rotation(direction):
    q = np.arange(QS) - QS // 2
    c, s = np.zeros((2, QP, YL))
    c[:QS], s[:QS] = roots(q[:, None] * np.arange(YL)[None, :], 16)
    return complex_rotation(c, direction * s)


def right_y_table(direction):
    form = "pkqy,fg->kfypgq" if direction < 0 else "pkqy,fg->kfqpgy"
    return np.einsum(form, short_rotation(direction), np.eye(8)).reshape(256, 256)


def right_merge_table():
    rot = short_rotation(-1)
    out = np.zeros((2, 16, YL, 2, 2, 8, QP))
    for z in range(2):
        for f in range(4):
            out[:, 4 * z + f, :, z, :, f, :] = np.einsum("pkqy->kypq", rot)
        out[:, 15 - z, :, z, :, 4, :] = np.einsum("pkqy->kypq", rot)
    return out.reshape(512, 512)


def left_z_table(direction, z_major):
    q = np.arange(KZ) - KZ // 2
    c, s = roots(q[:, None] * np.arange(NZ)[None, :], NZ)
    rot = complex_rotation(c, direction * s).reshape(2, 2, KZ, FAR, NEAR, 2)
    same = np.eye(LO)
    if direction < 0:
        form = "pkmxsz,ab->pmazsbxk" if z_major else "pkmxsz,ab->pmasbxzk"
        out = np.einsum(form, rot, same).reshape(2 * MODES, -1)
        return out / (NX * NY * NZ)
    form = "pkmxsz,ab->zsaxpkmb" if z_major else "pkmxsz,ab->saxzpkmb"
    return np.einsum(form, rot, same).reshape(-1, 2 * MODES)


def spread_table():
    low = [0, 0, 0, 0]
    high = [3, 1, 2, None]
    plain = [0, 1, 2, 3]
    other = [2, 3, 1, None]
    out = np.zeros((2, 4, QP, 2, 16, QP))
    for slot, f in enumerate(low + high + plain + other):
        if f is not None:
            for z in range(2):
                out[z, f, :, z, slot, :] = np.eye(QP)
    return out.reshape(128, 512)


def wave_table():
    lo = np.arange(LO).reshape(1, LO, 1, 1)
    m = np.arange(KZ).reshape(KZ, 1, 1, 1)
    q = np.arange(QP).reshape(1, 1, 1, QP)
    full = (KZ, LO, 8, QP)
    return np.stack(
        [
            np.broadcast_to(32 * (q - QS // 2) + lo, full),
            np.broadcast_to((m - KZ // 2) * (NX // NZ), full),
        ]
    ).reshape(2 * MODES, 128)


def dot(lhs, rhs):
    return lax.dot_general(
        lhs, rhs, (((1,), (0,)), ((), ())), preferred_element_type=jnp.float32
    )


def dot_tn(lhs, rhs):
    return lax.dot_general(
        lhs, rhs, (((0,), (0,)), ((), ())), preferred_element_type=jnp.float32
    )


def dot_nt(lhs, rhs):
    return lax.dot_general(
        lhs, rhs, (((1,), (1,)), ((), ())), preferred_element_type=jnp.float32
    )


def to_bf16(values):
    return values.astype(jnp.bfloat16)


TILES = NX // 128


def tiled(values):
    lead = values.shape[:-3]
    split = values.reshape(*lead, YL, 2, TILES, 128)
    return jnp.swapaxes(split, -3, -2).reshape(*lead, YL * TILES * 2, 128)


def untiled(values):
    lead = values.shape[:-2]
    split = values.reshape(*lead, YL, TILES, 2, 128)
    return jnp.swapaxes(split, -3, -2).reshape(*lead, YL, 2, NX)


def plane(ref, z, *lead):
    return jnp.concatenate(
        [ref[(*lead, pl.ds(2 * t + z, YL, stride=2 * TILES))] for t in range(TILES)], axis=1
    )


def put_plane(ref, z, values, *lead):
    for t in range(TILES):
        ref[(*lead, pl.ds(2 * t + z, YL, stride=2 * TILES))] = values[
            :, 128 * t : 128 * (t + 1)
        ]


def x_forward_kernel(
    phase_hbm, vel_hbm, table_hbm, out_ref, bulk_ref, phase_ref, vel_ref, table_ref,
    sems, wide,
):
    copies = [
        pltpu.make_async_copy(src, dst, sems.at[i])
        for i, (src, dst) in enumerate(
            [
                (phase_hbm, phase_ref),
                (vel_hbm, vel_ref),
                (table_hbm.at[pl.ds(0, KC)], table_ref.at[pl.ds(0, KC)]),
                (table_hbm.at[pl.ds(KC, KC)], table_ref.at[pl.ds(KC, KC)]),
            ]
        )
    ]
    for i in (2, 3, 1, 0):
        copies[i].start()
    copies[0].wait()
    phases = [plane(phase_ref, z) for z in range(2)]
    bulk = [p * p * p - p for p in phases]
    copies[1].wait()
    rows = []
    for z in range(2):
        rows += [phases[z]] + [plane(vel_ref, z, j) for j in range(3)]
    rows += [jnp.zeros((6 * YL, NX), jnp.float32), bulk[1], bulk[0]]
    x = jnp.concatenate([to_bf16(r) for r in rows], axis=0)
    copies[2].wait()
    copies[3].wait()
    lines = dot_nt(table_ref[...], x)
    out_ref[...] = to_bf16(lines[:, :128])
    wide[pl.ds(0, LINES, stride=2), :] = lines[:, 128:]
    wide[pl.ds(1, LINES, stride=2), :] = pltpu.roll(lines[:, 128:], YL, 1)
    bulk_ref[...] = to_bf16(wide[...])


def y_forward_kernel(in_ref, left_ref, cos_ref, sin_ref, right_ref, out_ref, wide):
    half = in_ref.shape[0] // 2
    sums = dot(left_ref[...], in_ref[...])
    re, im = sums[:half], sums[half:]
    c, s = cos_ref[...], sin_ref[...]
    lines = jnp.concatenate([to_bf16(re * c + im * s), to_bf16(im * c - re * s)], axis=1)
    modes = dot(lines, right_ref[...])
    for p in range(2):
        wide[pl.ds(p, half, stride=2), :] = modes[:, 128 * p : 128 * (p + 1)]
    out_ref[...] = to_bf16(wide[...])


def y_merge_kernel(in_ref, bulk_ref, left_ref, cos_ref, sin_ref, right_ref, out_ref, wide):
    half = in_ref.shape[0] // 2
    sums = dot(left_ref[...], jnp.concatenate([in_ref[...], bulk_ref[...]], axis=1))
    c, s = cos_ref[...], sin_ref[...]
    res, ims = [], []
    for t in range(2):
        re, im = (sums[p * half : (p + 1) * half, 128 * t : 128 * (t + 1)] for p in range(2))
        res.append(to_bf16(re * c + im * s))
        ims.append(to_bf16(im * c - re * s))
    modes = dot(jnp.concatenate(res + ims, axis=1), right_ref[...])
    for t in range(4):
        wide[pl.ds(t, half, stride=4), :] = modes[:, 128 * t : 128 * (t + 1)]
    out_ref[...] = to_bf16(wide[...])


def y_inverse_kernel(in_ref, left_ref, cos_ref, sin_ref, right_ref, out_ref, wide):
    half = in_ref.shape[0] // 2
    wide[...] = in_ref[...].astype(jnp.float32)
    modes = jnp.concatenate(
        [to_bf16(wide[pl.ds(p, half, stride=2), :]) for p in range(2)], axis=1
    )
    spun = unspun(dot(modes, right_ref[...]), cos_ref[...], sin_ref[...])
    out_ref[...] = to_bf16(dot(left_ref[...], spun))


def unspun(lines, c, s):
    re, im = lines[:, :128], lines[:, 128:]
    return jnp.concatenate([to_bf16(re * c - im * s), to_bf16(re * s + im * c)], axis=0)


def y_inverse_rider_kernel(
    in_ref, rider_ref, left_ref, cos_ref, sin_ref, right_ref, out_ref, wide, lines
):
    block = 2 * LINES // AS
    half = block // 2
    for a in range(AS):
        wide[pl.ds(a * block, block), :] = rows_of(in_ref, a).astype(jnp.float32)
    modes = jnp.concatenate(
        [to_bf16(wide[pl.ds(p, AS * half, stride=2), :]) for p in range(2)], axis=1
    )
    turned = dot(modes, right_ref[...])
    c, s = cos_ref[...], sin_ref[...]
    spun = [unspun(turned[a * half : (a + 1) * half], c, s) for a in range(AS)]
    every = dot(left_ref[...], jnp.concatenate(spun, axis=1))
    for a in range(AS):
        for j in range(4):
            lines[pl.ds(4 * a + j, 64, stride=4 * AS), :] = every[
                64 * j : 64 * (j + 1), 128 * a : 128 * (a + 1)
            ]
    lane = lax.broadcasted_iota(jnp.int32, (2 * LINES, 128), 1)
    out_ref[...] = to_bf16(
        jnp.where(lane < 7 * YL, lines[...], rider_ref[...].astype(jnp.float32))
    )


def first_wave():
    owner = (lax.axis_index("xl") * FAR + lax.axis_index("far")) * (COLS // 2)
    return ((owner + lax.axis_index("z")) * AS).astype(jnp.float32)


def cross_waves(wave_ref):
    ky = wave_ref[0:MODES] + (lax.axis_index("near") * LO).astype(jnp.float32)
    kz = wave_ref[MODES : 2 * MODES]
    slot = lax.broadcasted_iota(jnp.int32, (MODES, 128), 1) // QP
    return ky, kz, slot


def rows_of(ref, a):
    block = ref.shape[0] // NEAR
    part = block // AS
    return jnp.concatenate(
        [ref[pl.ds(r * block + a * part, part), :] for r in range(NEAR)], axis=0
    )


def put_rows(ref, a, values):
    block = ref.shape[0] // NEAR
    part = block // AS
    for r in range(NEAR):
        ref[pl.ds(r * block + a * part, part), :] = values[r * part : (r + 1) * part]


def derive_kernel(
    in_ref, spread_ref, left_ref, wave_ref, back_ref, out_ref, spectra_ref
):
    ky, kz, slot = cross_waves(wave_ref)
    across = ky * ky + kz * kz
    plain = slot == 3
    rows = jnp.concatenate([rows_of(in_ref, a) for a in range(AS)], axis=0)
    spreads = to_bf16(dot(rows, spread_ref[...]))
    part = rows.shape[0] // AS
    stacks = [
        jnp.concatenate([w[:, :256], w[:, 256:]], axis=0)
        for w in (spreads[part * a : part * (a + 1)] for a in range(AS))
    ]
    left = left_ref[...]
    many = [dot(left, stack) for stack in stacks]
    coeffs = []
    for a, modes in enumerate(many):
        spectra_ref[pl.ds(2 * MODES * a, 2 * MODES), :] = modes[:, 128:]
        kx = first_wave() + float(a)
        one = jnp.where(
            (slot == 0) | (slot == 6),
            kx,
            jnp.where(
                (slot == 1) | (slot == 4),
                ky,
                jnp.where(
                    (slot == 2) | (slot == 5),
                    kz,
                    jnp.where(plain, -(across + kx * kx), 0.0),
                ),
            ),
        )
        two = jnp.where(
            slot == 4, kz, jnp.where(slot == 5, kx, jnp.where(slot == 6, ky, 0.0))
        )
        re = modes[:MODES, :128] * one - modes[:MODES, 128:] * two
        im = modes[MODES:, :128] * one - modes[MODES:, 128:] * two
        coeffs.append(
            jnp.concatenate(
                [to_bf16(jnp.where(plain, re, -im)), to_bf16(jnp.where(plain, im, re))],
                axis=0,
            )
        )
    back = dot(back_ref[...], jnp.concatenate(coeffs, axis=1))
    for a in range(AS):
        put_rows(out_ref, a, to_bf16(back[:, 128 * a : 128 * (a + 1)]))


def solve_kernel(in_ref, spectra_ref, left_ref, wave_ref, back_ref, out_ref):
    ky, kz, slot = cross_waves(wave_ref)
    across = ky * ky + kz * kz
    scalar = slot == 0
    used = slot < 4
    many = dot(
        left_ref[...], jnp.concatenate([rows_of(in_ref, a) for a in range(AS)], axis=1)
    )
    coeffs = []
    for a in range(AS):
        modes = many[:, 128 * a : 128 * (a + 1)]
        kx = first_wave() + float(a)
        k2 = across + kx * kx
        stable = 1.0 / time_step + mobility * stabilizer * k2
        below = jnp.where(
            scalar,
            stable + mobility * epsilon * epsilon * k2 * k2,
            1.0 / time_step + k2 / reynolds,
        )
        inv = jnp.where(used, 1.0 / below, 0.0)
        keep = jnp.where(scalar, stable, 1.0 / time_step)
        mean = scalar & (k2 == 0.0)
        sign = jnp.where(mean, 0.0, jnp.where(scalar, -1.0, 1.0))
        bulk = jnp.where(scalar, mobility * k2, 0.0)
        wave = jnp.where(
            slot == 1, kx, jnp.where(slot == 2, ky, jnp.where(slot == 3, kz, 0.0))
        )
        shared = wave / jnp.maximum(k2, 1.0)
        parts = []
        for p in range(2):
            now = modes[p * MODES : (p + 1) * MODES]
            old = spectra_ref[pl.ds((2 * a + p) * MODES, MODES), :]
            fresh = (keep * old + sign * now - bulk * pltpu.roll(now, 64, 1)) * inv
            normal = wave * fresh
            for step in (16, 32, 64):
                normal = normal + pltpu.roll(normal, step, 1)
            parts.append(to_bf16(fresh - shared * normal))
        coeffs.append(jnp.concatenate(parts, axis=0))
    back = dot(back_ref[...], jnp.concatenate(coeffs, axis=1))
    half = back.shape[0] // 2
    for a in range(AS):
        both = back[:, 128 * a : 128 * (a + 1)]
        put_rows(out_ref, a, to_bf16(both[:half] + pltpu.roll(both[half:], 64, 1)))


def nonlinear_kernel(
    in_ref, phase_ref, vel_ref, back_ref, table_ref, out_ref, bulk_ref, wide
):
    wide[...] = in_ref[...].astype(jnp.float32)
    sides = [wide[pl.ds(z, LINES, stride=2), :] for z in range(2)]
    lane = lax.broadcasted_iota(jnp.int32, (LINES, 128), 1)
    bulk_ref[...] = to_bf16(
        jnp.where(lane < 7 * YL, pltpu.roll(sides[1], 7 * YL, 1), sides[0])
    )
    terms = []
    for z in range(2):
        values = dot_tn(to_bf16(sides[z]), back_ref[...])
        d = [values[YL * f : YL * (f + 1)] for f in range(7)]
        phase = plane(phase_ref, z)
        v = [plane(vel_ref, z, j) for j in range(3)]
        g, lap, w = d[0:3], d[3], d[4:7]
        potential = phase * phase * phase - phase - epsilon * epsilon * lap
        terms += [
            v[0] * g[0] + v[1] * g[1] + v[2] * g[2],
            v[1] * w[2] - v[2] * w[1] + potential * g[0],
            v[2] * w[0] - v[0] * w[2] + potential * g[1],
            v[0] * w[1] - v[1] * w[0] + potential * g[2],
        ]
    x = jnp.concatenate([to_bf16(t) for t in terms], axis=0)
    out_ref[...] = to_bf16(dot_nt(table_ref[...], x))


def x_inverse_kernel(in_ref, back_ref, phase_hbm, vel_hbm, fields, sems):
    values = dot_tn(in_ref[...], back_ref[...])
    copies = []
    for f in range(4):
        for z in range(2):
            row = YL * (4 * z + f)
            put_plane(fields, z, values[row : row + YL], f)
        target = phase_hbm if f == 0 else vel_hbm.at[f - 1]
        copies.append(pltpu.make_async_copy(fields.at[f], target, sems.at[f]))
        copies[-1].start()
    for c in copies:
        c.wait()


def call(kernel, outs, scratch, *args, space=pltpu.VMEM, out_space=pltpu.VMEM):
    specs = [pl.BlockSpec(memory_space=space)] * len(args)
    return pl.pallas_call(
        kernel,
        in_specs=specs,
        out_specs=[pl.BlockSpec(memory_space=out_space)] * len(outs),
        out_shape=outs,
        scratch_shapes=scratch,
        compiler_params=pltpu.CompilerParams(vmem_limit_bytes=16 * 1024 * 1024),
        cost_estimate=pl.CostEstimate(
            flops=COST, bytes_accessed=COST // 400, transcendentals=0
        ),
    )(*args)


def buffer(rows, dtype=jnp.bfloat16):
    return jax.ShapeDtypeStruct((rows, 128), dtype)


def exchange(values, axis):
    rows = values.shape[0]
    swapped = lax.all_to_all(
        values.reshape(rows // 2, 2, 128), axis, split_axis=0, concat_axis=0, tiled=True
    )
    return swapped.reshape(rows, 128)


def on_device(phase, velocity):
    phase, velocity = tiled(phase), tiled(velocity)
    f32 = jnp.float32
    x_table = as_bf16(x_forward_table())
    x_back = as_bf16(x_inverse_table())
    waves = jnp.asarray(wave_table(), f32)

    def spin(count, inner):
        return tuple(jnp.asarray(t, f32) for t in twiddles(count, inner, lanes_y()))

    def scratch(rows):
        return pltpu.VMEM((rows, 128), f32)

    lines, rider = call(
        x_forward_kernel, [buffer(LINES), buffer(2 * LINES)],
        [
            pltpu.VMEM(phase.shape, f32),
            pltpu.VMEM(velocity.shape, f32),
            pltpu.VMEM(x_table.shape, x_table.dtype),
            pltpu.SemaphoreType.DMA((4,)),
            scratch(2 * LINES),
        ],
        *(
            pltpu.with_memory_space_constraint(v, pltpu.HBM)
            for v in (phase, velocity, x_table)
        ),
        space=pltpu.HBM,
    )
    planes = call(
        y_forward_kernel, [buffer(LINES)], [scratch(LINES)],
        exchange(lines, BIG), as_bf16(left_y_table(1, -1)), *spin(AS, FAR),
        as_bf16(right_y_table(-1)),
    )[0]
    planes, spectra = call(
        derive_kernel, [buffer(2 * LINES), buffer(2 * MODES * AS, f32)], [],
        exchange(planes, "near"), as_bf16(spread_table()),
        as_bf16(left_z_table(-1, True)), waves, as_bf16(left_z_table(1, False)),
    )
    lines = call(
        y_inverse_rider_kernel, [buffer(2 * LINES)], [scratch(2 * LINES), scratch(2 * LINES)],
        exchange(planes, "near"), rider, as_bf16(left_y_single_table()), *spin(1, 2 * FAR),
        as_bf16(right_y_table(1)),
    )[0]
    lines, bulk = call(
        nonlinear_kernel, [buffer(LINES), buffer(LINES)], [scratch(2 * LINES)],
        exchange(lines, BIG), phase, velocity, x_back, x_table,
    )
    planes = call(
        y_merge_kernel, [buffer(2 * LINES)], [scratch(2 * LINES)],
        exchange(lines, BIG), bulk, as_bf16(left_y_table(1, -1)), *spin(AS, FAR),
        as_bf16(right_merge_table()),
    )[0]
    planes = call(
        solve_kernel, [buffer(LINES)], [],
        exchange(planes, "near"), spectra, as_bf16(left_z_table(-1, False)), waves,
        as_bf16(left_z_table(1, True)),
    )[0]
    lines = call(
        y_inverse_kernel, [buffer(LINES)], [scratch(LINES)],
        exchange(planes, "near"), as_bf16(left_y_table(1, 1)), *spin(AS, FAR),
        as_bf16(right_y_table(1)),
    )[0]
    done = tuple(
        call(
            x_inverse_kernel,
            [
                jax.ShapeDtypeStruct(phase.shape, f32),
                jax.ShapeDtypeStruct(velocity.shape, f32),
            ],
            [pltpu.VMEM((4, *phase.shape), f32), pltpu.SemaphoreType.DMA((4,))],
            exchange(lines, BIG), x_back, out_space=pltpu.HBM,
        )
    )
    return tuple(untiled(v) for v in done)


def solution(mesh):
    finer = Mesh(
        mesh.devices.reshape(FAR, NEAR, COLS // 2, 2), ("far", "near", "z", "xl")
    )
    row, col = ("far", "near"), ("z", "xl")
    in_specs = (P(col, row, None), P(None, col, row, None))
    out_specs = (P(col, row, None), P(None, col, row, None))
    return jax.shard_map(
        on_device, mesh=finer, in_specs=in_specs, out_specs=out_specs, check_vma=False
    )
```
